256 devices in a mesh: section: 8 (over z), dp: 32 (over x, y, core).
Axes of the slice: x: 4, y: 4, z: 8, core: 2. Of those that a mesh axis runs over, the one named last changes fastest.
Arguments:
- entry: bfloat16 [6144, 3584], P('dp'), may hold values from -6 to 6
- norm_gain: float32 [8, 3584], P('section'), may hold values from 0.5 to 1.5
- w_qkv: bfloat16 [8, 3584, 1152], P('section', 'dp'), may hold values from -0.09375 to 0.09375
- w_out: bfloat16 [8, 896, 3584], P('section', 'dp'), may hold values from -0.1875 to 0.1875
- final_gain: float32 [3584], replicated, may hold values from 0.5 to 1.5
- lengths: int32 [128], P('dp'), may hold values from 24 to 48
- positive: int32 [64], P('dp'), may hold values from 0 to 63, each once
Outputs:
- section_grads: bfloat16 [8, 6144, 3584], P('section', 'dp')
The draws below stay inside these ranges and needn't reach their ends.
Inputs may be any that keep to these rules, and one draw needn't show every extreme that they name: lengths[j] is the count of tokens of sequence j; its last token is pooled. Each document index is the positive of exactly one query.
All inputs are finite; a program needn't handle non-finite values.
Results may differ from the reference program's by a relative error of at most 0.022.
Values may be sent and summed in bfloat16 or wider, within the bound.
No kernel may reach another device: no remote copies, remote signals or barrier semaphores. Data moves between devices by JAX's collectives and lax.ppermute only.
A program may use at most 192 MiB of HBM per device.

```python
import jax
import jax.numpy as jnp
from jax import lax

D = 3584
HEAD_DIM = 64
GROUP_HEADS = 7
KV_GROUPS = 2
LEN = 48
QW = 896
QUERIES = 64
SEQS = 128
TOKENS = 6144
N_SECTION = 8


def place_ends(values, rng, smallest, high):
    index_at = [jax.random.randint(jax.random.fold_in(rng, axis), (), 0, length) for axis, length in enumerate(values.shape)]
    main_axis = values.shape.index(max(values.shape))
    next_to = index_at[:main_axis] + [(index_at[main_axis] + 1) % values.shape[main_axis]] + index_at[main_axis + 1:]
    return values.at[tuple(index_at)].set(smallest).at[tuple(next_to)].set(high)


def shard_levels(rng, dims, shards, smallest, high):
    def one(axis_at, shards_of):
        steps = jax.random.uniform(jax.random.fold_in(jax.random.fold_in(rng, 6), axis_at), (shards_of,), jnp.float32, smallest / len(shards), high / len(shards))
        return jnp.repeat(jnp.exp(steps), dims[axis_at] // shards_of).reshape((-1,) + (1,) * (len(dims) - axis_at - 1))

    level = one(*shards[0])
    for cut in shards[1:]:
        level = level * one(*cut)
    return level


def noise(rng, dims, deviation, reach, shards=(), kind=jnp.bfloat16):
    drawn = jax.random.normal(rng, dims, jnp.float32) * deviation
    if len(shards) > 0:
        drawn = shard_levels(rng, dims, shards, -0.22, 0.18) * drawn
    return jnp.clip(drawn, min=-reach, max=reach).astype(kind)


def setup_inputs(seed: int = 0) -> dict:
    arg_keys = jax.random.split(jax.random.key(seed), 8)
    return {
        "entry": noise(arg_keys[0], (TOKENS, D), 1.0, 6.0, ((0, 32),)),
        "norm_gain": jnp.clip(1.0 + 0.1 * jax.random.normal(arg_keys[1], (N_SECTION, D), jnp.float32), 0.5, 1.5),
        "w_qkv": noise(arg_keys[2], (N_SECTION, D, QW + 2 * KV_GROUPS * HEAD_DIM), D ** -0.5, 0.09375, ((0, 8), (1, 32))),
        "w_out": noise(arg_keys[3], (N_SECTION, QW, D), QW ** -0.5, 0.1875, ((0, 8), (1, 32))),
        "final_gain": jnp.clip(1.0 + 0.1 * jax.random.normal(arg_keys[4], (D,), jnp.float32), 0.5, 1.5),
        "lengths": place_ends(jax.random.randint(arg_keys[5], (SEQS,), LEN // 2, LEN + 1), jax.random.fold_in(arg_keys[5], 1), LEN // 2, LEN).astype(jnp.int32),
        "positive": jax.random.permutation(arg_keys[6], QUERIES).astype(jnp.int32),
    }


rope_base = 1000000.0
norm_eps = 1e-06
sharpness_divisor = 0.05
objective_coefficient = 256.0

def rotary(values, positions):
    half_dim = values.shape[-1] // 2
    frequency = rope_base ** (-jnp.arange(half_dim, dtype=jnp.float32) * (2.0 / values.shape[-1]))
    angles = positions.astype(jnp.float32)[:, None] * frequency[None, :]
    cosine = jnp.cos(angles)[:, None, :]
    sine_part = jnp.sin(angles)[:, None, :]
    first_half = values[..., :half_dim]
    second_half = values[..., half_dim:]
    return jnp.concatenate([first_half * cosine - second_half * sine_part, second_half * cosine + first_half * sine_part], axis=-1)

def rms_scale(values, gain_row):
    return values * lax.rsqrt(lax.optimization_barrier(jnp.mean(values * values, axis=-1, keepdims=True)) + norm_eps) * gain_row

def attention_layer(hidden, seq_lengths, gain_row, weight_qkv, weight_out):
    row_count, row_width = hidden.shape
    seq_count = seq_lengths.shape[0]
    length = row_count // seq_count
    q_width = weight_out.shape[0]
    kv_width = KV_GROUPS * HEAD_DIM
    wide_in = hidden.astype(jnp.float32)
    normed = rms_scale(wide_in, gain_row).astype(jnp.bfloat16)
    projected = jnp.dot(normed, weight_qkv, preferred_element_type=jnp.float32)
    positions = jnp.arange(length, dtype=jnp.int32)
    query_rot = rotary(projected[:, :q_width].reshape(seq_count, length, KV_GROUPS * GROUP_HEADS, HEAD_DIM), positions).astype(jnp.bfloat16)
    key_rot = rotary(projected[:, q_width:q_width + kv_width].reshape(seq_count, length, KV_GROUPS, HEAD_DIM), positions).astype(jnp.bfloat16)
    value_rows = projected[:, q_width + kv_width:].reshape(seq_count, length, KV_GROUPS, HEAD_DIM).astype(jnp.bfloat16)
    query_grid = query_rot.reshape(seq_count, length, KV_GROUPS, GROUP_HEADS, HEAD_DIM)
    scores = jnp.einsum('sqgzd,skgd->sgzqk', query_grid.astype(jnp.float32), key_rot.astype(jnp.float32)) * HEAD_DIM ** (-0.5)
    key_live = positions[None, :] < seq_lengths[:, None]
    weights = jnp.where(key_live[:, None, None, None, :], jnp.exp(scores), 0.0)
    prob_low = (weights / lax.optimization_barrier(jnp.sum(weights, axis=-1, keepdims=True))).astype(jnp.bfloat16)
    context = jnp.einsum('sgzqk,skgd->sqgzd', prob_low.astype(jnp.float32), value_rows.astype(jnp.float32)).astype(jnp.bfloat16)
    branch = jnp.dot(context.reshape(row_count, q_width), weight_out, preferred_element_type=jnp.float32)
    return (wide_in + branch).astype(jnp.bfloat16)

def embed_rows(rows_in, final_gain):
    pooled = rms_scale(rows_in.astype(jnp.float32), final_gain)
    return pooled * lax.rsqrt(lax.optimization_barrier(jnp.sum(pooled * pooled, axis=-1, keepdims=True)))

def pair_terms(question_representation, passage_representation, positive):
    match_raw_scores = jnp.dot(question_representation, passage_representation.T, preferred_element_type=jnp.float32) * (1.0 / sharpness_divisor)
    weights = jnp.exp(match_raw_scores)
    normalized_exponential_odds = weights / lax.optimization_barrier(jnp.sum(weights, axis=-1, keepdims=True))
    correct_target_column = (positive[:, None] == jnp.arange(passage_representation.shape[0], dtype=jnp.int32)[None, :]).astype(jnp.float32)
    return (normalized_exponential_odds - correct_target_column) * (objective_coefficient / sharpness_divisor)

def reference(entry, norm_gain, w_qkv, w_out, final_gain, lengths, positive):
    section_count = norm_gain.shape[0]
    seq_count = lengths.shape[0]
    length = entry.shape[0] // seq_count
    row_width = entry.shape[1]
    hidden = entry
    inputs = []
    for layer_id in range(section_count):
        inputs.append(hidden)
        hidden = attention_layer(hidden, lengths, norm_gain[layer_id], w_qkv[layer_id], w_out[layer_id])
    seq_grid = hidden.reshape(seq_count, length, row_width)
    last_rows = jnp.take_along_axis(seq_grid, (lengths - 1)[:, None, None], axis=1)[:, 0]
    embedding, back_embed = jax.vjp(lambda rows_in: embed_rows(rows_in, final_gain), last_rows)
    emb_low = embedding.astype(jnp.bfloat16)
    question_representation = emb_low[0::2]
    passage_representation = emb_low[1::2]
    pair_coef = pair_terms(question_representation, passage_representation, positive)
    grad_query = jnp.dot(pair_coef, passage_representation.astype(jnp.float32), precision=lax.Precision.HIGHEST)
    grad_doc = jnp.dot(pair_coef.T, question_representation.astype(jnp.float32), precision=lax.Precision.HIGHEST)
    grad_emb = jnp.stack([grad_query, grad_doc], axis=1).reshape(seq_count, row_width)
    grad_last = back_embed(grad_emb)[0]
    slot_hit = jnp.arange(length, dtype=jnp.int32)[None, :] == (lengths - 1)[:, None]
    seed_grad = jnp.where(slot_hit[:, :, None], grad_last[:, None, :], 0).astype(jnp.bfloat16).reshape(-1, row_width)
    cotangent = seed_grad
    collected = []
    for layer_id in reversed(range(section_count)):
        _, pull_back = jax.vjp(lambda values: attention_layer(values, lengths, norm_gain[layer_id], w_qkv[layer_id], w_out[layer_id]), inputs[layer_id])
        cotangent = pull_back(cotangent)[0]
        collected.append(cotangent)
    return jnp.stack(collected[::-1])
```

```python
import functools

import jax
import jax.numpy as jnp
from jax import lax
from jax.experimental import pallas as pl
from jax.experimental.pallas import tpu as pltpu
from jax.sharding import Mesh
from jax.sharding import PartitionSpec as P

HEAD_DIM = 64
LEN = 48
D = 3584
QW = 896
KV = 128
XW = QW + 2 * KV
PACK = XW + QW
PAIRS = QW // 128
DP = ("dp_0", "dp_1", "dp_2")
ROPE_BASE = 1000000.0
EPS = 1e-06
SHARP = 20.0
COEF = 256.0
CHUNK = 512
CHUNKS = D // CHUNK
F32 = jnp.float32
BF16 = jnp.bfloat16


def dot_nn(a, b):
    return lax.dot_general(a, b, (((1,), (0,)), ((), ())), preferred_element_type=F32)


def dot_nt(a, b):
    return lax.dot_general(a, b, (((1,), (1,)), ((), ())), preferred_element_type=F32)


def dot_tn(a, b):
    return lax.dot_general(a, b, (((0,), (0,)), ((), ())), preferred_element_type=F32)


def lanes(rows):
    return lax.broadcasted_iota(jnp.int32, (rows, 128), 1)


def partner(x):
    low = lax.rem(lanes(x.shape[0]), 64) < 32
    return jnp.where(low, pltpu.roll(x, 96, 1), pltpu.roll(x, 32, 1))


def paired(z):
    left = lanes(LEN) < 64
    rolled = pltpu.roll(z, 64, 1)
    pad = jnp.zeros((16, 128), BF16)
    a_left = jnp.where(left, z, 0.0).astype(BF16)
    b_right = jnp.where(left, 0.0, z).astype(BF16)
    b_left = jnp.where(left, rolled, 0.0).astype(BF16)
    a_right = jnp.where(left, 0.0, rolled).astype(BF16)
    return (
        jnp.concatenate([a_left, pad, a_right, pad], axis=0),
        jnp.concatenate([a_left, pad, b_right, pad], axis=0),
        jnp.concatenate([b_left, pad, b_right, pad], axis=0),
    )


SPANS = ((0, 3 * LEN), (3 * LEN, 4 * LEN), (4 * LEN, 7 * LEN))


def by_pair(dot, rows, blocks):
    return jnp.concatenate(
        [dot(rows[lo:hi], block) for (lo, hi), block in zip(SPANS, blocks)], axis=0
    )


def unpaired(rows, other):
    left = lanes(LEN) < 64
    s00, s01, s11 = (dot_tn(rows[lo:hi], other[lo:hi]) for lo, hi in SPANS)
    first = jnp.where(left, s00[:LEN] + s01[:LEN], 0.0)
    first += pltpu.roll(jnp.where(left, 0.0, s00[64 : 64 + LEN]), 64, 1)
    second = jnp.where(left, 0.0, s01[64 : 64 + LEN] + s11[64 : 64 + LEN])
    second += pltpu.roll(jnp.where(left, s11[:LEN], 0.0), 64, 1)
    return first + second


def half_sums(x):
    left = lanes(x.shape[0]) < 64
    low = jnp.sum(jnp.where(left, x, 0.0), axis=1, keepdims=True)
    high = jnp.sum(jnp.where(left, 0.0, x), axis=1, keepdims=True)
    return low, high, left


def probabilities(q_rows, k_blocks, length):
    scores = by_pair(dot_nt, q_rows, k_blocks) * HEAD_DIM ** (-0.5)
    live = lax.rem(lanes(scores.shape[0]), 64) < length
    weights = jnp.where(live, jnp.exp(scores), 0.0)
    low, high, left = half_sums(weights)
    return weights * jnp.where(left, 1.0 / low, 1.0 / high)


def rows_of(x_ref):
    return jnp.concatenate([x_ref[:, 128 * i : 128 * i + 128] for i in range(PAIRS)], axis=0)


def inv_rms(wide):
    return lax.rsqrt(jnp.sum(wide * wide, axis=1, keepdims=True) * (1.0 / D) + EPS)


def forward_kernel(
    tick,
    last_stage,
    micro,
    meta,
    inbox,
    entry,
    gain,
    table,
    packed,
    w_out,
    stash_h_in,
    stash_x_in,
    last_in,
    out,
    stash_h,
    stash_x,
    last,
    wq_v,
    wo_v,
    h_v,
    n_v,
    acc_v,
    x_v,
    ctx_v,
    last_v,
    wq_sem,
    wo_sem,
    sems,
):
    del stash_h_in, stash_x_in, last_in
    stage = meta[0]
    slot = tick - stage

    @pl.when(jnp.logical_and(slot >= 0, slot < micro))
    def _():
        length = meta[1 + slot]
        row0 = pl.multiple_of(slot * LEN, LEN)

        def wq_copy(i):
            rows = pl.ds(pl.multiple_of(i * CHUNK, CHUNK), CHUNK)
            return pltpu.make_async_copy(
                packed.at[rows, pl.ds(0, XW)], wq_v.at[rows, :], wq_sem.at[i]
            )

        def wo_copy(i):
            cols = pl.ds(pl.multiple_of(i * CHUNK, CHUNK), CHUNK)
            return pltpu.make_async_copy(w_out.at[:, cols], wo_v.at[:, cols], wo_sem.at[i])

        first = pltpu.make_async_copy(entry.at[pl.ds(row0, LEN), :], h_v, sems.at[0])
        later = pltpu.make_async_copy(inbox, h_v, sems.at[0])

        @pl.when(stage == 0)
        def _():
            first.start()

        @pl.when(stage != 0)
        def _():
            later.start()

        for i in range(CHUNKS):
            wq_copy(i).start()
        for i in range(CHUNKS):
            wo_copy(i).start()
        later.wait()
        keep_h = pltpu.make_async_copy(h_v, stash_h.at[pl.ds(row0, LEN), :], sems.at[1])
        keep_h.start()
        wide = h_v[...].astype(F32)
        n_v[...] = (wide * inv_rms(wide) * gain[...]).astype(BF16)
        acc_v[...] = jnp.zeros_like(acc_v)

        @pl.loop(0, CHUNKS)
        def _(i):
            wq_copy(i).wait()
            cols = pl.ds(pl.multiple_of(i * CHUNK, CHUNK), CHUNK)
            acc_v[...] += dot_nn(n_v[:, cols], wq_v[cols, :])

        cosine, sine = table[0], table[1]
        for i in range(PAIRS + 1):
            part = acc_v[:, 128 * i : 128 * i + 128]
            x_v[:, 128 * i : 128 * i + 128] = (part * cosine + partner(part) * sine).astype(BF16)
        x_v[:, QW + KV :] = acc_v[:, QW + KV :].astype(BF16)
        keep_x = pltpu.make_async_copy(x_v, stash_x.at[pl.ds(row0, LEN), :], sems.at[2])
        keep_x.start()
        k_blocks = paired(x_v[:, QW : QW + KV].astype(F32))
        v_blocks = paired(x_v[:, QW + KV :].astype(F32))
        probs = probabilities(rows_of(x_v), k_blocks, length).astype(BF16)
        context = by_pair(dot_nn, probs, v_blocks).astype(BF16)
        for i in range(PAIRS):
            ctx_v[:, 128 * i : 128 * i + 128] = context[LEN * i : LEN * i + LEN]

        @pl.loop(0, CHUNKS)
        def _(i):
            wo_copy(i).wait()
            cols = pl.ds(pl.multiple_of(i * CHUNK, CHUNK), CHUNK)
            branch = dot_nn(ctx_v[...], wo_v[:, cols])
            out[:, cols] = (h_v[:, cols].astype(F32) + branch).astype(BF16)

        @pl.when(stage == last_stage)
        def _():
            hit = lax.broadcasted_iota(jnp.int32, (LEN, D), 0) == length - 1
            row = jnp.sum(jnp.where(hit, out[...].astype(F32), 0.0), axis=0, keepdims=True)
            last_v[...] = jnp.broadcast_to(row, (8, D))
            put = pltpu.make_async_copy(last_v, last.at[slot], sems.at[3])
            put.start()
            put.wait()

        keep_h.wait()
        keep_x.wait()


def backward_kernel(
    tick,
    last_stage,
    micro,
    meta,
    inbox,
    seed,
    gain,
    table,
    packed,
    w_out,
    stash_h,
    stash_x,
    grads_in,
    out,
    grads,
    wq_v,
    wo_v,
    h_v,
    g_v,
    x_v,
    dctx_v,
    dx_v,
    dn_v,
    wq_sem,
    wo_sem,
    sems,
):
    del grads_in
    stage = meta[0]
    slot = tick - (last_stage - stage)

    @pl.when(jnp.logical_and(slot >= 0, slot < micro))
    def _():
        length = meta[1 + slot]
        row0 = pl.multiple_of(slot * LEN, LEN)

        def wq_copy(i):
            rows = pl.ds(pl.multiple_of(i * CHUNK, CHUNK), CHUNK)
            return pltpu.make_async_copy(
                packed.at[rows, pl.ds(0, XW)], wq_v.at[rows, :], wq_sem.at[i]
            )

        def wo_copy(i):
            cols = pl.ds(pl.multiple_of(i * CHUNK, CHUNK), CHUNK)
            return pltpu.make_async_copy(w_out.at[:, cols], wo_v.at[:, cols], wo_sem.at[i])

        for i in range(CHUNKS):
            wo_copy(i).start()
        get_x = pltpu.make_async_copy(stash_x.at[pl.ds(row0, LEN), :], x_v, sems.at[0])
        get_h = pltpu.make_async_copy(stash_h.at[pl.ds(row0, LEN), :], h_v, sems.at[1])
        get_x.start()
        get_h.start()
        for i in range(CHUNKS):
            wq_copy(i).start()

        @pl.when(stage == last_stage)
        def _():
            hit = lax.broadcasted_iota(jnp.int32, (LEN, D), 0) == length - 1
            row = jnp.where(lax.broadcasted_iota(jnp.int32, (8, D), 0) == slot, seed[...], 0.0)
            row = jnp.sum(row, axis=0, keepdims=True)
            g_v[...] = jnp.where(hit, jnp.broadcast_to(row, (LEN, D)), 0.0).astype(BF16)

        @pl.when(stage != last_stage)
        def _():
            g_v[...] = inbox[...]

        dctx_v[...] = jnp.zeros_like(dctx_v)

        @pl.loop(0, CHUNKS)
        def _(i):
            wo_copy(i).wait()
            cols = pl.ds(pl.multiple_of(i * CHUNK, CHUNK), CHUNK)
            dctx_v[...] += dot_nt(g_v[:, cols], wo_v[:, cols])

        get_x.wait()
        q_rows = rows_of(x_v)
        k_blocks = paired(x_v[:, QW : QW + KV].astype(F32))
        v_blocks = paired(x_v[:, QW + KV :].astype(F32))
        probs = probabilities(q_rows, k_blocks, length)
        dctx = rows_of(dctx_v).astype(BF16)
        dvalue = unpaired(probs.astype(BF16), dctx)
        dprobs = by_pair(dot_nt, dctx, v_blocks).astype(BF16).astype(F32)
        low, high, left = half_sums(dprobs * probs)
        dscores = probs * (dprobs - jnp.where(left, low, high)) * HEAD_DIM ** (-0.5)
        dscores = dscores.astype(BF16)
        dquery = by_pair(dot_nn, dscores, k_blocks).astype(BF16).astype(F32)
        dkey = unpaired(dscores, q_rows).astype(BF16).astype(F32)
        cosine, sine = table[0], table[1]
        for i in range(PAIRS):
            part = dquery[LEN * i : LEN * i + LEN]
            dx_v[:, 128 * i : 128 * i + 128] = (part * cosine - partner(part) * sine).astype(BF16)
        dx_v[:, QW : QW + KV] = (dkey * cosine - partner(dkey) * sine).astype(BF16)
        dx_v[:, QW + KV :] = dvalue.astype(BF16)

        @pl.loop(0, CHUNKS)
        def _(i):
            wq_copy(i).wait()
            rows = pl.ds(pl.multiple_of(i * CHUNK, CHUNK), CHUNK)
            dn_v[:, rows] = dot_nt(dx_v[...], wq_v[rows, :]).astype(BF16)

        get_h.wait()
        wide = h_v[...].astype(F32)
        scale = inv_rms(wide)
        scaled = dn_v[...].astype(F32) * gain[...]
        inner = jnp.sum(scaled * wide, axis=1, keepdims=True)
        out[...] = (
            g_v[...].astype(F32)
            + scale * scaled
            - wide * (scale * scale * scale * inner * (1.0 / D))
        ).astype(BF16)
        put = pltpu.make_async_copy(out, grads.at[pl.ds(row0, LEN), :], sems.at[2])
        put.start()
        put.wait()


ANY = pl.BlockSpec(memory_space=pl.ANY)
VMEM = pl.BlockSpec(memory_space=pltpu.VMEM)
SMEM = pl.BlockSpec(memory_space=pltpu.SMEM)
LAYER_COST = pl.CostEstimate(
    flops=2 * LEN * D * (XW + QW), bytes_accessed=2 * D * (XW + QW), transcendentals=0
)
LIMIT = 40 * 1024 * 1024


def forward_layer(tick, last_stage, micro, meta, inbox, entry, gain, table, packed, w_out, state):
    return pl.pallas_call(
        functools.partial(forward_kernel, tick, last_stage, micro),
        out_shape=(
            jax.ShapeDtypeStruct((LEN, D), BF16),
            *(jax.ShapeDtypeStruct(a.shape, a.dtype) for a in state),
        ),
        in_specs=[SMEM, ANY, ANY, VMEM, VMEM, ANY, ANY, ANY, ANY, ANY],
        out_specs=(VMEM, ANY, ANY, ANY),
        input_output_aliases={7: 1, 8: 2, 9: 3},
        scratch_shapes=[
            pltpu.VMEM((D, XW), BF16),
            pltpu.VMEM((QW, D), BF16),
            pltpu.VMEM((LEN, D), BF16),
            pltpu.VMEM((LEN, D), BF16),
            pltpu.VMEM((LEN, XW), F32),
            pltpu.VMEM((LEN, XW), BF16),
            pltpu.VMEM((LEN, QW), BF16),
            pltpu.VMEM((8, D), F32),
            pltpu.SemaphoreType.DMA((CHUNKS,)),
            pltpu.SemaphoreType.DMA((CHUNKS,)),
            pltpu.SemaphoreType.DMA((4,)),
        ],
        compiler_params=pltpu.CompilerParams(vmem_limit_bytes=LIMIT),
        cost_estimate=LAYER_COST,
        name="forward_layer",
    )(meta, inbox, entry, gain, table, packed, w_out, *state)


def backward_layer(
    tick, last_stage, micro, meta, inbox, seed, gain, table, packed, w_out, stash, grads
):
    return pl.pallas_call(
        functools.partial(backward_kernel, tick, last_stage, micro),
        out_shape=(
            jax.ShapeDtypeStruct((LEN, D), BF16),
            jax.ShapeDtypeStruct(grads.shape, grads.dtype),
        ),
        in_specs=[SMEM, VMEM, VMEM, VMEM, VMEM, ANY, ANY, ANY, ANY, ANY],
        out_specs=(VMEM, ANY),
        input_output_aliases={9: 1},
        scratch_shapes=[
            pltpu.VMEM((D, XW), BF16),
            pltpu.VMEM((QW, D), BF16),
            pltpu.VMEM((LEN, D), BF16),
            pltpu.VMEM((LEN, D), BF16),
            pltpu.VMEM((LEN, XW), BF16),
            pltpu.VMEM((LEN, QW), F32),
            pltpu.VMEM((LEN, XW), BF16),
            pltpu.VMEM((LEN, D), BF16),
            pltpu.SemaphoreType.DMA((CHUNKS,)),
            pltpu.SemaphoreType.DMA((CHUNKS,)),
            pltpu.SemaphoreType.DMA((3,)),
        ],
        compiler_params=pltpu.CompilerParams(vmem_limit_bytes=LIMIT),
        cost_estimate=LAYER_COST,
        name="backward_layer",
    )(meta, inbox, seed, gain, table, packed, w_out, *stash, grads)


def embed_kernel(last, final_gain, labels, out):
    rows = jnp.concatenate([last[j, 0:1, :] for j in (0, 2, 1, 3)] + [jnp.zeros((4, D), F32)], axis=0)
    pooled = rows * inv_rms(rows) * final_gain[...]
    size = jnp.sum(pooled * pooled, axis=1, keepdims=True)
    row = lax.broadcasted_iota(jnp.int32, (8, D), 0)
    unit = jnp.where(row < 4, pooled * lax.rsqrt(jnp.where(size > 0.0, size, 1.0)), 0.0)
    which = lax.broadcasted_iota(jnp.int32, (8, 128), 0)
    label = jnp.where(which == 0, labels[0], jnp.where(which == 1, labels[1], 0)).astype(F32)
    out[:, :D] = unit.astype(BF16)
    out[:, D:] = label.astype(BF16)


def embed(last, final_gain, labels):
    return pl.pallas_call(
        embed_kernel,
        out_shape=jax.ShapeDtypeStruct((8, D + 128), BF16),
        in_specs=[VMEM, VMEM, SMEM],
        out_specs=VMEM,
        name="embed",
    )(last, final_gain, labels)


def loss_kernel(me, last, final_gain, everyone, seed):
    count = everyone.shape[0]
    emb = everyone[:, :D]
    label = everyone[:, D:].astype(F32)[:, 0:1].astype(jnp.int32)
    scores = dot_nt(emb, emb) * SHARP
    row = lax.broadcasted_iota(jnp.int32, (count, count), 0)
    col = lax.broadcasted_iota(jnp.int32, (count, count), 1)
    valid = jnp.logical_and(lax.rem(row, 4) < 2, lax.rem(col, 4) >= 2)
    weights = jnp.where(valid, jnp.exp(scores), 0.0)
    total = jnp.sum(weights, axis=1, keepdims=True)
    prob = weights / jnp.where(total > 0.0, total, 1.0)
    target = lax.div(label, 2) * 4 + 2 + lax.rem(label, 2)
    hit = jnp.logical_and(valid, col == target)
    coef = (prob - hit.astype(F32)) * (COEF * SHARP)
    coef = jnp.where(valid, coef, 0.0)
    both = coef + coef.T
    mine = lax.broadcasted_iota(jnp.int32, (8, count), 0)
    pick = lax.broadcasted_iota(jnp.int32, (8, count), 1) == me[0] * 4 + mine
    pick = jnp.logical_and(pick, mine < 4).astype(F32)
    own = lax.dot_general(
        pick, both, (((1,), (0,)), ((), ())), precision=lax.Precision.HIGHEST,
        preferred_element_type=F32,
    )
    top = own.astype(BF16)
    rest = own - top.astype(F32)
    mid = rest.astype(BF16)
    low = (rest - mid.astype(F32)).astype(BF16)
    grad = dot_nn(top, emb) + (dot_nn(mid, emb) + dot_nn(low, emb))
    rows = jnp.concatenate([last[j, 0:1, :] for j in (0, 2, 1, 3)] + [jnp.zeros((4, D), F32)], axis=0)
    gain = final_gain[...]
    scale = inv_rms(rows)
    pooled = rows * scale * gain
    size = jnp.sum(pooled * pooled, axis=1, keepdims=True)
    norm = lax.rsqrt(jnp.where(size > 0.0, size, 1.0))
    unit = pooled * norm
    dpooled = norm * (grad - unit * jnp.sum(grad * unit, axis=1, keepdims=True))
    scaled = dpooled * gain
    inner = jnp.sum(scaled * rows, axis=1, keepdims=True)
    drow = scale * scaled - rows * (scale * scale * scale * inner * (1.0 / D))
    drow = drow.astype(BF16).astype(F32)
    seed[...] = jnp.concatenate(
        [drow[0:1], drow[2:3], drow[1:2], drow[3:4], jnp.zeros((4, D), F32)], axis=0
    )


def loss_seed(me, last, final_gain, everyone):
    return pl.pallas_call(
        loss_kernel,
        out_shape=jax.ShapeDtypeStruct((8, D), F32),
        in_specs=[SMEM, VMEM, VMEM, VMEM],
        out_specs=VMEM,
        name="loss_seed",
    )(me, last, final_gain, everyone)


def rotary_table():
    lane = jnp.arange(128, dtype=jnp.int32)
    frequency = ROPE_BASE ** (-(lane % 32).astype(F32) * (2.0 / HEAD_DIM))
    angles = jnp.arange(LEN, dtype=F32)[:, None] * frequency[None, :]
    sign = jnp.where(lane % 64 < 32, -1.0, 1.0)
    return jnp.stack([jnp.cos(angles), jnp.sin(angles) * sign])


def per_device(entry, norm_gain, w_qkv, w_out, final_gain, lengths, positive):
    stage = lax.axis_index("section")
    stages = lax.axis_size("section")
    replica = lax.axis_index(DP)
    micro = lengths.shape[0]
    shard = jnp.concatenate([w_qkv[0], w_out[0].reshape(-1, QW)], axis=1)
    packed = lax.all_gather(shard, DP, axis=0, tiled=True)
    full_out = packed[:, XW:].reshape(QW, D)
    meta = jnp.concatenate([stage.reshape(1), lengths]).astype(jnp.int32)
    table = rotary_table()
    gain = norm_gain
    ticks = micro + stages - 1
    rows = micro * LEN
    state = (
        jnp.zeros((rows, D), BF16),
        jnp.zeros((rows, XW), BF16),
        jnp.zeros((micro, 8, D), F32),
    )
    inbox = entry[:LEN]
    for tick in range(ticks):
        out, *state = forward_layer(
            tick, stages - 1, micro, meta, inbox, entry, gain, table, packed, full_out, state
        )
        if tick < ticks - 1:
            pairs = [(s, s + 1) for s in range(stages - 1) if 0 <= tick - s < micro]
            inbox = lax.ppermute(out, "section", pairs)
    stash_h, stash_x, last = state
    final_row = final_gain[None, :]
    mine = embed(last, final_row, positive)[:4]
    count = lax.axis_size(DP)
    copies = jnp.broadcast_to(mine, (count, *mine.shape))
    everyone = lax.all_to_all(copies, DP, split_axis=0, concat_axis=0, tiled=True)
    everyone = everyone.reshape(count * 4, D + 128)
    seed = loss_seed(replica.reshape(1), last, final_row, everyone)
    grads = jnp.zeros((rows, D), BF16)
    for tick in range(ticks):
        out, grads = backward_layer(
            tick, stages - 1, micro, meta, inbox, seed, gain, table, packed, full_out,
            (stash_h, stash_x), grads,
        )
        if tick < ticks - 1:
            pairs = [
                (stages - 1 - s, stages - 2 - s)
                for s in range(stages - 1)
                if 0 <= tick - s < micro
            ]
            inbox = lax.ppermute(out, "section", pairs)
    return grads[None]


def solution(mesh):
    finer = Mesh(
        mesh.devices.reshape(mesh.shape["section"], 4, 4, 2), ("section", "dp_0", "dp_1", "dp_2")
    )
    in_specs = (
        P(DP, None),
        P("section", None),
        P("section", DP, None),
        P("section", DP, None),
        P(),
        P(DP),
        P(DP),
    )
    return jax.shard_map(
        per_device,
        mesh=finer,
        in_specs=in_specs,
        out_specs=P("section", DP, None),
        check_vma=False,
    )
```

```python
import functools

import jax
import jax.numpy as jnp
from jax import lax
from jax.experimental import pallas as pl
from jax.experimental.pallas import tpu as pltpu
from jax.sharding import Mesh
from jax.sharding import PartitionSpec as P

HEAD_DIM = 64
LEN = 48
D = 3584
QW = 896
KV = 128
XW = QW + 2 * KV
PACK = XW + QW
PAIRS = QW // 128
DP = ("dp_0", "dp_1", "dp_2")
ROPE_BASE = 1000000.0
EPS = 1e-06
SHARP = 20.0
COEF = 256.0
CHUNK = 512
CHUNKS = D // CHUNK
STAGGER = 4200
F32 = jnp.float32
BF16 = jnp.bfloat16


def dot_nn(a, b):
    return lax.dot_general(a, b, (((1,), (0,)), ((), ())), preferred_element_type=F32)


def dot_nt(a, b):
    return lax.dot_general(a, b, (((1,), (1,)), ((), ())), preferred_element_type=F32)


def dot_tn(a, b):
    return lax.dot_general(a, b, (((0,), (0,)), ((), ())), preferred_element_type=F32)


def lanes(rows):
    return lax.broadcasted_iota(jnp.int32, (rows, 128), 1)


def partner(x):
    low = lax.rem(lanes(x.shape[0]), 64) < 32
    return jnp.where(low, pltpu.roll(x, 96, 1), pltpu.roll(x, 32, 1))


def paired(z):
    left = lanes(LEN) < 64
    rolled = pltpu.roll(z, 64, 1)
    pad = jnp.zeros((16, 128), BF16)
    a_left = jnp.where(left, z, 0.0).astype(BF16)
    b_right = jnp.where(left, 0.0, z).astype(BF16)
    b_left = jnp.where(left, rolled, 0.0).astype(BF16)
    a_right = jnp.where(left, 0.0, rolled).astype(BF16)
    return (
        jnp.concatenate([a_left, pad, a_right, pad], axis=0),
        jnp.concatenate([a_left, pad, b_right, pad], axis=0),
        jnp.concatenate([b_left, pad, b_right, pad], axis=0),
    )


SPANS = ((0, 3 * LEN), (3 * LEN, 4 * LEN), (4 * LEN, 7 * LEN))


def by_pair(dot, rows, blocks):
    return jnp.concatenate(
        [dot(rows[lo:hi], block) for (lo, hi), block in zip(SPANS, blocks)], axis=0
    )


def unpaired(rows, other):
    left = lanes(LEN) < 64
    s00, s01, s11 = (dot_tn(rows[lo:hi], other[lo:hi]) for lo, hi in SPANS)
    first = jnp.where(left, s00[:LEN] + s01[:LEN], 0.0)
    first += pltpu.roll(jnp.where(left, 0.0, s00[64 : 64 + LEN]), 64, 1)
    second = jnp.where(left, 0.0, s01[64 : 64 + LEN] + s11[64 : 64 + LEN])
    second += pltpu.roll(jnp.where(left, s11[:LEN], 0.0), 64, 1)
    return first + second


def half_sums(x):
    left = lanes(x.shape[0]) < 64
    low = jnp.sum(jnp.where(left, x, 0.0), axis=1, keepdims=True)
    high = jnp.sum(jnp.where(left, 0.0, x), axis=1, keepdims=True)
    return low, high, left


def probabilities(q_rows, k_blocks, length):
    scores = by_pair(dot_nt, q_rows, k_blocks) * HEAD_DIM ** (-0.5)
    live = lax.rem(lanes(scores.shape[0]), 64) < length
    weights = jnp.where(live, jnp.exp(scores), 0.0)
    low, high, left = half_sums(weights)
    return weights * jnp.where(left, 1.0 / low, 1.0 / high)


def rows_of(x_ref):
    return jnp.concatenate([x_ref[:, 128 * i : 128 * i + 128] for i in range(PAIRS)], axis=0)


def inv_rms(wide):
    return lax.rsqrt(jnp.sum(wide * wide, axis=1, keepdims=True) * (1.0 / D) + EPS)


def forward_kernel(
    tick,
    last_stage,
    micro,
    meta,
    inbox,
    entry,
    gain,
    table,
    wq,
    wo,
    stash_h_in,
    stash_x_in,
    last_in,
    out,
    stash_h,
    stash_x,
    last,
    h_v,
    n_v,
    acc_v,
    x_v,
    ctx_v,
    last_v,
    sems,
):
    del stash_h_in, stash_x_in, last_in
    stage = meta[0]
    slot = tick - stage

    @pl.when(jnp.logical_and(slot >= 0, slot < micro))
    def _():
        length = meta[1 + slot]
        row0 = pl.multiple_of(slot * LEN, LEN)

        first = pltpu.make_async_copy(entry.at[pl.ds(row0, LEN), :], h_v, sems.at[0])
        later = pltpu.make_async_copy(inbox, h_v, sems.at[0])

        @pl.when(stage == 0)
        def _():
            first.start()

        @pl.when(stage != 0)
        def _():
            later.start()

        if tick == 0:

            @pl.when(meta[1 + micro] == 1)
            def _():
                pl.delay(STAGGER)

        later.wait()
        keep_h = pltpu.make_async_copy(h_v, stash_h.at[pl.ds(row0, LEN), :], sems.at[1])
        keep_h.start()
        wide = h_v[...].astype(F32)
        n_v[...] = (wide * inv_rms(wide) * gain[...]).astype(BF16)
        acc_v[...] = jnp.zeros_like(acc_v)

        @pl.loop(0, CHUNKS)
        def _(i):
            cols = pl.ds(pl.multiple_of(i * CHUNK, CHUNK), CHUNK)
            acc_v[...] += dot_nn(n_v[:, cols], wq[cols, :])

        cosine, sine = table[0], table[1]
        for i in range(PAIRS + 1):
            part = acc_v[:, 128 * i : 128 * i + 128]
            x_v[:, 128 * i : 128 * i + 128] = (part * cosine + partner(part) * sine).astype(BF16)
        x_v[:, QW + KV :] = acc_v[:, QW + KV :].astype(BF16)
        keep_x = pltpu.make_async_copy(x_v, stash_x.at[pl.ds(row0, LEN), :], sems.at[2])
        keep_x.start()
        k_blocks = paired(x_v[:, QW : QW + KV].astype(F32))
        v_blocks = paired(x_v[:, QW + KV :].astype(F32))
        probs = probabilities(rows_of(x_v), k_blocks, length).astype(BF16)
        context = by_pair(dot_nn, probs, v_blocks).astype(BF16)
        for i in range(PAIRS):
            ctx_v[:, 128 * i : 128 * i + 128] = context[LEN * i : LEN * i + LEN]

        @pl.loop(0, CHUNKS)
        def _(i):
            cols = pl.ds(pl.multiple_of(i * CHUNK, CHUNK), CHUNK)
            branch = dot_nn(ctx_v[...], wo[:, cols])
            out[:, cols] = (h_v[:, cols].astype(F32) + branch).astype(BF16)

        @pl.when(stage == last_stage)
        def _():
            hit = lax.broadcasted_iota(jnp.int32, (LEN, D), 0) == length - 1
            row = jnp.sum(jnp.where(hit, out[...].astype(F32), 0.0), axis=0, keepdims=True)
            last_v[...] = jnp.broadcast_to(row, (8, D))
            put = pltpu.make_async_copy(last_v, last.at[slot], sems.at[3])
            put.start()
            put.wait()

        keep_h.wait()
        keep_x.wait()


def backward_kernel(
    tick,
    last_stage,
    micro,
    meta,
    inbox,
    seed,
    gain,
    table,
    wq,
    wo,
    stash_h,
    stash_x,
    grads_in,
    out,
    grads,
    h_v,
    g_v,
    x_v,
    dctx_v,
    dx_v,
    dn_v,
    sems,
):
    del grads_in
    stage = meta[0]
    slot = tick - (last_stage - stage)

    @pl.when(jnp.logical_and(slot >= 0, slot < micro))
    def _():
        length = meta[1 + slot]
        row0 = pl.multiple_of(slot * LEN, LEN)

        get_x = pltpu.make_async_copy(stash_x.at[pl.ds(row0, LEN), :], x_v, sems.at[0])
        get_h = pltpu.make_async_copy(stash_h.at[pl.ds(row0, LEN), :], h_v, sems.at[1])
        get_x.start()
        get_h.start()
        if tick == 0:

            @pl.when(meta[1 + micro] == 1)
            def _():
                pl.delay(STAGGER)


        @pl.when(stage == last_stage)
        def _():
            hit = lax.broadcasted_iota(jnp.int32, (LEN, D), 0) == length - 1
            row = jnp.where(lax.broadcasted_iota(jnp.int32, (8, D), 0) == slot, seed[...], 0.0)
            row = jnp.sum(row, axis=0, keepdims=True)
            g_v[...] = jnp.where(hit, jnp.broadcast_to(row, (LEN, D)), 0.0).astype(BF16)

        @pl.when(stage != last_stage)
        def _():
            g_v[...] = inbox[...]

        dctx_v[...] = jnp.zeros_like(dctx_v)

        @pl.loop(0, CHUNKS)
        def _(i):
            cols = pl.ds(pl.multiple_of(i * CHUNK, CHUNK), CHUNK)
            dctx_v[...] += dot_nt(g_v[:, cols], wo[:, cols])

        get_x.wait()
        q_rows = rows_of(x_v)
        k_blocks = paired(x_v[:, QW : QW + KV].astype(F32))
        v_blocks = paired(x_v[:, QW + KV :].astype(F32))
        probs = probabilities(q_rows, k_blocks, length)
        dctx = rows_of(dctx_v).astype(BF16)
        dvalue = unpaired(probs.astype(BF16), dctx)
        dprobs = by_pair(dot_nt, dctx, v_blocks).astype(BF16).astype(F32)
        low, high, left = half_sums(dprobs * probs)
        dscores = probs * (dprobs - jnp.where(left, low, high)) * HEAD_DIM ** (-0.5)
        dscores = dscores.astype(BF16)
        dquery = by_pair(dot_nn, dscores, k_blocks).astype(BF16).astype(F32)
        dkey = unpaired(dscores, q_rows).astype(BF16).astype(F32)
        cosine, sine = table[0], table[1]
        for i in range(PAIRS):
            part = dquery[LEN * i : LEN * i + LEN]
            dx_v[:, 128 * i : 128 * i + 128] = (part * cosine - partner(part) * sine).astype(BF16)
        dx_v[:, QW : QW + KV] = (dkey * cosine - partner(dkey) * sine).astype(BF16)
        dx_v[:, QW + KV :] = dvalue.astype(BF16)

        @pl.loop(0, CHUNKS)
        def _(i):
            rows = pl.ds(pl.multiple_of(i * CHUNK, CHUNK), CHUNK)
            dn_v[:, rows] = dot_nt(dx_v[...], wq[rows, :]).astype(BF16)

        get_h.wait()
        wide = h_v[...].astype(F32)
        scale = inv_rms(wide)
        scaled = dn_v[...].astype(F32) * gain[...]
        inner = jnp.sum(scaled * wide, axis=1, keepdims=True)
        out[...] = (
            g_v[...].astype(F32)
            + scale * scaled
            - wide * (scale * scale * scale * inner * (1.0 / D))
        ).astype(BF16)
        put = pltpu.make_async_copy(out, grads.at[pl.ds(row0, LEN), :], sems.at[2])
        put.start()
        put.wait()


ANY = pl.BlockSpec(memory_space=pl.ANY)
VMEM = pl.BlockSpec(memory_space=pltpu.VMEM)
SMEM = pl.BlockSpec(memory_space=pltpu.SMEM)
LAYER_COST = pl.CostEstimate(
    flops=2 * LEN * D * (XW + QW), bytes_accessed=2 * D * (XW + QW), transcendentals=0
)
LIMIT = 24 * 1024 * 1024
SMALL = 8 * 1024 * 1024


def forward_layer(tick, last_stage, micro, meta, inbox, entry, gain, table, wq, wo, state):
    return pl.pallas_call(
        functools.partial(forward_kernel, tick, last_stage, micro),
        out_shape=(
            jax.ShapeDtypeStruct((LEN, D), BF16),
            *(jax.ShapeDtypeStruct(a.shape, a.dtype) for a in state),
        ),
        in_specs=[SMEM, ANY, ANY, VMEM, VMEM, VMEM, VMEM, ANY, ANY, ANY],
        out_specs=(VMEM, ANY, ANY, ANY),
        input_output_aliases={7: 1, 8: 2, 9: 3},
        scratch_shapes=[
            pltpu.VMEM((LEN, D), BF16),
            pltpu.VMEM((LEN, D), BF16),
            pltpu.VMEM((LEN, XW), F32),
            pltpu.VMEM((LEN, XW), BF16),
            pltpu.VMEM((LEN, QW), BF16),
            pltpu.VMEM((8, D), F32),
            pltpu.SemaphoreType.DMA((4,)),
        ],
        compiler_params=pltpu.CompilerParams(vmem_limit_bytes=LIMIT),
        cost_estimate=LAYER_COST,
        name="forward_layer",
    )(meta, inbox, entry, gain, table, wq, wo, *state)


def backward_layer(
    tick, last_stage, micro, meta, inbox, seed, gain, table, wq, wo, stash, grads
):
    return pl.pallas_call(
        functools.partial(backward_kernel, tick, last_stage, micro),
        out_shape=(
            jax.ShapeDtypeStruct((LEN, D), BF16),
            jax.ShapeDtypeStruct(grads.shape, grads.dtype),
        ),
        in_specs=[SMEM, VMEM, VMEM, VMEM, VMEM, VMEM, VMEM, ANY, ANY, ANY],
        out_specs=(VMEM, ANY),
        input_output_aliases={9: 1},
        scratch_shapes=[
            pltpu.VMEM((LEN, D), BF16),
            pltpu.VMEM((LEN, D), BF16),
            pltpu.VMEM((LEN, XW), BF16),
            pltpu.VMEM((LEN, QW), F32),
            pltpu.VMEM((LEN, XW), BF16),
            pltpu.VMEM((LEN, D), BF16),
            pltpu.SemaphoreType.DMA((3,)),
        ],
        compiler_params=pltpu.CompilerParams(vmem_limit_bytes=LIMIT),
        cost_estimate=LAYER_COST,
        name="backward_layer",
    )(meta, inbox, seed, gain, table, wq, wo, *stash, grads)


def pack_kernel(w_qkv, w_out, shard):
    shard[:, :XW] = w_qkv[...]
    pieces = [w_out[:, QW * j : QW * j + QW].astype(F32) for j in range(D // QW)]
    shard[:, XW:] = jnp.concatenate(pieces, axis=0).astype(BF16)


def pack(w_qkv, w_out):
    return pl.pallas_call(
        pack_kernel,
        out_shape=jax.ShapeDtypeStruct((w_qkv.shape[0], PACK), BF16),
        in_specs=[VMEM, VMEM],
        out_specs=VMEM,
        compiler_params=pltpu.CompilerParams(vmem_limit_bytes=SMALL),
        name="pack",
    )(w_qkv, w_out)


def unpack_kernel(packed, wq, wo, part_v, sems):
    parts = D // QW
    groups = 8
    rows = D // groups
    short = rows // (4 * parts)
    whole = pltpu.make_async_copy(packed.at[:, pl.ds(0, XW)], wq, sems.at[groups])

    def piece(i):
        at = pl.ds(pl.multiple_of(i * rows, rows), rows)
        return pltpu.make_async_copy(packed.at[at, pl.ds(XW, QW)], part_v.at[at, :], sems.at[i])

    for i in range(groups):
        piece(i).start()
    whole.start()

    @pl.loop(0, groups)
    def _(i):
        piece(i).wait()
        blocks = []
        for r in range(4):
            at = pl.ds(pl.multiple_of(i * rows + r * (rows // 4), 16), rows // 4)
            blocks.append(part_v[at, :].astype(F32))
        to = pl.ds(pl.multiple_of(i * (rows // 4), 16), rows // 4)
        for j in range(parts):
            cut = [block[short * j : short * j + short] for block in blocks]
            wo[to, QW * j : QW * j + QW] = jnp.concatenate(cut, axis=0).astype(BF16)

    whole.wait()


def unpack(packed):
    return pl.pallas_call(
        unpack_kernel,
        out_shape=(jax.ShapeDtypeStruct((D, XW), BF16), jax.ShapeDtypeStruct((QW, D), BF16)),
        in_specs=[ANY],
        out_specs=(VMEM, VMEM),
        scratch_shapes=[pltpu.VMEM((D, QW), BF16), pltpu.SemaphoreType.DMA((9,))],
        compiler_params=pltpu.CompilerParams(vmem_limit_bytes=LIMIT),
        name="unpack",
    )(packed)


HALF = D // 2
WIDE = HALF + 128


def pooled_rows(last):
    return jnp.concatenate([last[j, 0:1, :] for j in (0, 2, 1, 3)], axis=0)


def embed_kernel(last, final_gain, labels, out):
    rows = pooled_rows(last)
    pooled = rows * inv_rms(rows) * final_gain[...]
    unit = pooled * lax.rsqrt(jnp.sum(pooled * pooled, axis=1, keepdims=True))
    halves = jnp.concatenate([unit[:, :HALF], unit[:, HALF:]], axis=0).astype(BF16)
    which = lax.broadcasted_iota(jnp.int32, (8, 128), 0)
    label = jnp.where(which == 0, labels[0], jnp.where(which == 1, labels[1], 0))
    label = label.astype(F32).astype(BF16)
    for i in range(out.shape[0]):
        out[i, :, :HALF] = halves
        out[i, :, HALF:] = label


def embed(count, last, final_gain, labels):
    return pl.pallas_call(
        functools.partial(embed_kernel),
        out_shape=jax.ShapeDtypeStruct((count, 8, WIDE), BF16),
        in_specs=[VMEM, VMEM, SMEM],
        out_specs=VMEM,
        compiler_params=pltpu.CompilerParams(vmem_limit_bytes=SMALL),
        name="embed",
    )(last, final_gain, labels)


def loss_kernel(me, last, final_gain, everyone, seed):
    count = everyone.shape[0]
    emb = everyone[:, :HALF]
    label = everyone[:, HALF:].astype(F32)[:, 0:1].astype(jnp.int32)
    scores = dot_nt(emb, emb)
    scores = scores + pltpu.roll(pltpu.roll(scores, count - 4, 0), count - 4, 1)
    row = lax.rem(lax.broadcasted_iota(jnp.int32, (count, count), 0), 8)
    col = lax.broadcasted_iota(jnp.int32, (count, count), 1)
    doc = jnp.logical_and(lax.rem(col, 8) >= 2, lax.rem(col, 8) < 4)
    valid = jnp.logical_and(row < 2, doc)
    weights = jnp.where(valid, jnp.exp(scores * SHARP), 0.0)
    total = jnp.sum(weights, axis=1, keepdims=True)
    prob = weights / jnp.where(row[:, :1] < 2, total, 1.0)
    target = lax.div(label, 2) * 8 + 2 + lax.rem(label, 2)
    coef = jnp.where(valid, (prob - (col == target).astype(F32)) * (COEF * SHARP), 0.0)
    both = coef + coef.T
    mine = lax.broadcasted_iota(jnp.int32, (8, count), 0)
    pick = lax.broadcasted_iota(jnp.int32, (8, count), 1) == me[0] * 8 + mine
    own = lax.dot_general(
        pick.astype(F32),
        both,
        (((1,), (0,)), ((), ())),
        precision=lax.Precision.HIGHEST,
        preferred_element_type=F32,
    )[:4]
    own = jnp.concatenate([own, pltpu.roll(own, 4, 1)], axis=0)
    top = own.astype(BF16)
    rest = own - top.astype(F32)
    mid = rest.astype(BF16)
    low = (rest - mid.astype(F32)).astype(BF16)
    grad = dot_nn(top, emb) + (dot_nn(mid, emb) + dot_nn(low, emb))
    grad = jnp.concatenate([grad[:4], grad[4:]], axis=1)
    rows = pooled_rows(last)
    gain = final_gain[...]
    scale = inv_rms(rows)
    pooled = rows * scale * gain
    norm = lax.rsqrt(jnp.sum(pooled * pooled, axis=1, keepdims=True))
    unit = pooled * norm
    dpooled = norm * (grad - unit * jnp.sum(grad * unit, axis=1, keepdims=True))
    scaled = dpooled * gain
    inner = jnp.sum(scaled * rows, axis=1, keepdims=True)
    drow = scale * scaled - rows * (scale * scale * scale * inner * (1.0 / D))
    drow = drow.astype(BF16).astype(F32)
    seed[...] = jnp.concatenate(
        [drow[0:1], drow[2:3], drow[1:2], drow[3:4], jnp.zeros((4, D), F32)], axis=0
    )


def loss_seed(me, last, final_gain, everyone):
    return pl.pallas_call(
        loss_kernel,
        out_shape=jax.ShapeDtypeStruct((8, D), F32),
        in_specs=[SMEM, VMEM, VMEM, VMEM],
        out_specs=VMEM,
        compiler_params=pltpu.CompilerParams(vmem_limit_bytes=SMALL),
        name="loss_seed",
    )(me, last, final_gain, everyone)


def rotary_table():
    lane = jnp.arange(128, dtype=jnp.int32)
    frequency = ROPE_BASE ** (-(lane % 32).astype(F32) * (2.0 / HEAD_DIM))
    angles = jnp.arange(LEN, dtype=F32)[:, None] * frequency[None, :]
    sign = jnp.where(lane % 64 < 32, -1.0, 1.0)
    return jnp.stack([jnp.cos(angles), jnp.sin(angles) * sign])


def per_device(entry, norm_gain, w_qkv, w_out, final_gain, lengths, positive):
    stage = lax.axis_index("section")
    stages = lax.axis_size("section")
    replica = lax.axis_index(DP)
    micro = lengths.shape[0]
    core = lax.axis_index("dp_2")
    wq, wo = unpack(lax.all_gather(pack(w_qkv[0], w_out[0]), DP, axis=0, tiled=True))
    meta = jnp.concatenate([stage.reshape(1), lengths, core.reshape(1)]).astype(jnp.int32)
    table = rotary_table()
    gain = norm_gain
    ticks = micro + stages - 1
    rows = micro * LEN
    state = (
        jnp.zeros((rows, D), BF16),
        jnp.zeros((rows, XW), BF16),
        jnp.zeros((micro, 8, D), F32),
    )
    inbox = entry[:LEN]
    for tick in range(ticks):
        out, *state = forward_layer(
            tick, stages - 1, micro, meta, inbox, entry, gain, table, wq, wo, state
        )
        if tick < ticks - 1:
            pairs = [(s, s + 1) for s in range(stages - 1) if 0 <= tick - s < micro]
            inbox = lax.ppermute(out, "section", pairs)
    stash_h, stash_x, last = state
    final_row = final_gain[None, :]
    count = lax.axis_size(DP)
    copies = embed(count, last, final_row, positive)
    everyone = lax.all_to_all(copies, DP, split_axis=0, concat_axis=0, tiled=True)
    everyone = everyone.reshape(count * 8, WIDE)
    seed = loss_seed(replica.reshape(1), last, final_row, everyone)
    grads = jnp.zeros((rows, D), BF16)
    for tick in range(ticks):
        out, grads = backward_layer(
            tick, stages - 1, micro, meta, inbox, seed, gain, table, wq, wo,
            (stash_h, stash_x), grads,
        )
        if tick < ticks - 1:
            pairs = [
                (stages - 1 - s, stages - 2 - s)
                for s in range(stages - 1)
                if 0 <= tick - s < micro
            ]
            inbox = lax.ppermute(out, "section", pairs)
    return grads[None]


def solution(mesh):
    finer = Mesh(
        mesh.devices.reshape(mesh.shape["section"], 4, 4, 2), ("section", "dp_0", "dp_1", "dp_2")
    )
    in_specs = (
        P(DP, None),
        P("section", None),
        P("section", DP, None),
        P("section", DP, None),
        P(),
        P(DP),
        P(DP),
    )
    return jax.shard_map(
        per_device,
        mesh=finer,
        in_specs=in_specs,
        out_specs=P("section", DP, None),
        check_vma=False,
    )
```

```python
import functools

import jax
import jax.numpy as jnp
from jax import lax
from jax.experimental import pallas as pl
from jax.experimental.pallas import tpu as pltpu
from jax.sharding import Mesh
from jax.sharding import PartitionSpec as P

HEAD_DIM = 64
LEN = 48
D = 3584
QW = 896
KV = 128
XW = QW + 2 * KV
PACK = XW + QW
PAIRS = QW // 128
DP = ("dp_0", "dp_1", "dp_2")
ROPE_BASE = 1000000.0
EPS = 1e-06
SHARP = 20.0
COEF = 256.0
HALVES = 2
HALF = D // HALVES
STAGGER = 6500
F32 = jnp.float32
BF16 = jnp.bfloat16


def dot_nn(a, b):
    return lax.dot_general(a, b, (((1,), (0,)), ((), ())), preferred_element_type=F32)


def dot_nt(a, b):
    return lax.dot_general(a, b, (((1,), (1,)), ((), ())), preferred_element_type=F32)


def dot_tn(a, b):
    return lax.dot_general(a, b, (((0,), (0,)), ((), ())), preferred_element_type=F32)


def lanes(rows):
    return lax.broadcasted_iota(jnp.int32, (rows, 128), 1)


def partner(x):
    low = lax.rem(lanes(x.shape[0]), 64) < 32
    return jnp.where(low, pltpu.roll(x, 96, 1), pltpu.roll(x, 32, 1))


def paired(z):
    left = lanes(LEN) < 64
    rolled = pltpu.roll(z, 64, 1)
    pad = jnp.zeros((16, 128), BF16)
    a_left = jnp.where(left, z, 0.0).astype(BF16)
    b_right = jnp.where(left, 0.0, z).astype(BF16)
    b_left = jnp.where(left, rolled, 0.0).astype(BF16)
    a_right = jnp.where(left, 0.0, rolled).astype(BF16)
    return (
        jnp.concatenate([a_left, pad, a_right, pad], axis=0),
        jnp.concatenate([a_left, pad, b_right, pad], axis=0),
        jnp.concatenate([b_left, pad, b_right, pad], axis=0),
    )


SPANS = ((0, 3 * LEN), (3 * LEN, 4 * LEN), (4 * LEN, 7 * LEN))


def by_pair(dot, rows, blocks):
    return jnp.concatenate(
        [dot(rows[lo:hi], block) for (lo, hi), block in zip(SPANS, blocks)], axis=0
    )


def unpaired(rows, other):
    left = lanes(LEN) < 64
    s00, s01, s11 = (dot_tn(rows[lo:hi], other[lo:hi]) for lo, hi in SPANS)
    first = jnp.where(left, s00[:LEN] + s01[:LEN], 0.0)
    first += pltpu.roll(jnp.where(left, 0.0, s00[64 : 64 + LEN]), 64, 1)
    second = jnp.where(left, 0.0, s01[64 : 64 + LEN] + s11[64 : 64 + LEN])
    second += pltpu.roll(jnp.where(left, s11[:LEN], 0.0), 64, 1)
    return first + second


def half_sums(x):
    left = lanes(x.shape[0]) < 64
    low = jnp.sum(jnp.where(left, x, 0.0), axis=1, keepdims=True)
    high = jnp.sum(jnp.where(left, 0.0, x), axis=1, keepdims=True)
    return low, high, left


def probabilities(q_rows, k_blocks, length):
    scores = by_pair(dot_nt, q_rows, k_blocks) * HEAD_DIM ** (-0.5)
    live = lax.rem(lanes(scores.shape[0]), 64) < length
    weights = jnp.where(live, jnp.exp(scores), 0.0)
    low, high, left = half_sums(weights)
    return weights * jnp.where(left, 1.0 / low, 1.0 / high)


def rows_of(x_ref):
    return jnp.concatenate([x_ref[:, 128 * i : 128 * i + 128] for i in range(PAIRS)], axis=0)


def inv_rms(wide):
    return lax.rsqrt(jnp.sum(wide * wide, axis=1, keepdims=True) * (1.0 / D) + EPS)


def forward_kernel(
    tick,
    last_stage,
    micro,
    meta,
    inbox,
    entry,
    gain,
    table,
    wq,
    wo,
    stash_h_in,
    stash_x_in,
    last_in,
    out,
    stash_h,
    stash_x,
    last,
    h_v,
    n_v,
    acc_v,
    x_v,
    ctx_v,
    last_v,
    sems,
):
    del stash_h_in, stash_x_in, last_in
    stage = meta[0]
    slot = tick - stage

    @pl.when(jnp.logical_and(slot >= 0, slot < micro))
    def _():
        length = meta[1 + slot]
        row0 = pl.multiple_of(slot * LEN, LEN)

        first = pltpu.make_async_copy(entry.at[pl.ds(row0, LEN), :], h_v, sems.at[0])
        later = pltpu.make_async_copy(inbox, h_v, sems.at[0])

        @pl.when(stage == 0)
        def _():
            first.start()

        @pl.when(stage != 0)
        def _():
            later.start()

        if tick == 0:

            @pl.when(meta[5] == 1)
            def _():
                pl.delay(STAGGER)

        later.wait()
        keep_h = pltpu.make_async_copy(h_v, stash_h.at[pl.ds(row0, LEN), :], sems.at[1])
        keep_h.start()
        wide = h_v[...].astype(F32)
        n_v[...] = (wide * inv_rms(wide) * gain[...]).astype(BF16)
        acc_v[...] = dot_nn(n_v[...], wq[...])
        cosine, sine = table[0], table[1]
        for i in range(PAIRS + 1):
            part = acc_v[:, 128 * i : 128 * i + 128]
            x_v[:, 128 * i : 128 * i + 128] = (part * cosine + partner(part) * sine).astype(BF16)
        x_v[:, QW + KV :] = acc_v[:, QW + KV :].astype(BF16)
        keep_x = pltpu.make_async_copy(x_v, stash_x.at[pl.ds(row0, LEN), :], sems.at[2])
        keep_x.start()
        k_blocks = paired(x_v[:, QW : QW + KV].astype(F32))
        v_blocks = paired(x_v[:, QW + KV :].astype(F32))
        probs = probabilities(rows_of(x_v), k_blocks, length).astype(BF16)
        context = by_pair(dot_nn, probs, v_blocks).astype(BF16)
        for i in range(PAIRS):
            ctx_v[:, 128 * i : 128 * i + 128] = context[LEN * i : LEN * i + LEN]

        @pl.loop(0, HALVES)
        def _(i):
            cols = pl.ds(pl.multiple_of(i * HALF, HALF), HALF)
            branch = dot_nn(ctx_v[...], wo[:, cols])
            out[:, cols] = (h_v[:, cols].astype(F32) + branch).astype(BF16)

        @pl.when(stage == last_stage)
        def _():
            hit = lax.broadcasted_iota(jnp.int32, (LEN, D), 0) == length - 1
            row = jnp.sum(jnp.where(hit, out[...].astype(F32), 0.0), axis=0, keepdims=True)
            last_v[...] = jnp.broadcast_to(row, (8, D))
            put = pltpu.make_async_copy(last_v, last.at[slot], sems.at[3])
            put.start()
            put.wait()

        keep_h.wait()
        keep_x.wait()


def backward_kernel(
    tick,
    last_stage,
    micro,
    meta,
    inbox,
    seed,
    gain,
    table,
    wq,
    wo,
    stash_h,
    stash_x,
    grads_in,
    out,
    grads,
    h_v,
    g_v,
    x_v,
    dctx_v,
    dx_v,
    dn_v,
    sems,
):
    del grads_in
    stage = meta[0]
    slot = tick - (last_stage - stage)

    @pl.when(jnp.logical_and(slot >= 0, slot < micro))
    def _():
        length = meta[1 + slot]
        row0 = pl.multiple_of(slot * LEN, LEN)

        get_x = pltpu.make_async_copy(stash_x.at[pl.ds(row0, LEN), :], x_v, sems.at[0])
        get_h = pltpu.make_async_copy(stash_h.at[pl.ds(row0, LEN), :], h_v, sems.at[1])
        get_x.start()
        get_h.start()
        if tick == 0:

            @pl.when(meta[5] == 1)
            def _():
                pl.delay(STAGGER)


        @pl.when(stage == last_stage)
        def _():
            hit = lax.broadcasted_iota(jnp.int32, (LEN, D), 0) == length - 1
            row = jnp.where(lax.broadcasted_iota(jnp.int32, (8, D), 0) == slot, seed[...], 0.0)
            row = jnp.sum(row, axis=0, keepdims=True)
            g_v[...] = jnp.where(hit, jnp.broadcast_to(row, (LEN, D)), 0.0).astype(BF16)

        @pl.when(stage != last_stage)
        def _():
            g_v[...] = inbox[...]

        dctx_v[...] = dot_nt(g_v[...], wo[...])
        get_x.wait()
        q_rows = rows_of(x_v)
        k_blocks = paired(x_v[:, QW : QW + KV].astype(F32))
        v_blocks = paired(x_v[:, QW + KV :].astype(F32))
        probs = probabilities(q_rows, k_blocks, length)
        dctx = rows_of(dctx_v).astype(BF16)
        dvalue = unpaired(probs.astype(BF16), dctx)
        dprobs = by_pair(dot_nt, dctx, v_blocks).astype(BF16).astype(F32)
        low, high, left = half_sums(dprobs * probs)
        dscores = probs * (dprobs - jnp.where(left, low, high)) * HEAD_DIM ** (-0.5)
        dscores = dscores.astype(BF16)
        dquery = by_pair(dot_nn, dscores, k_blocks).astype(BF16).astype(F32)
        dkey = unpaired(dscores, q_rows).astype(BF16).astype(F32)
        cosine, sine = table[0], table[1]
        for i in range(PAIRS):
            part = dquery[LEN * i : LEN * i + LEN]
            dx_v[:, 128 * i : 128 * i + 128] = (part * cosine - partner(part) * sine).astype(BF16)
        dx_v[:, QW : QW + KV] = (dkey * cosine - partner(dkey) * sine).astype(BF16)
        dx_v[:, QW + KV :] = dvalue.astype(BF16)

        @pl.loop(0, HALVES)
        def _(i):
            rows = pl.ds(pl.multiple_of(i * HALF, HALF), HALF)
            dn_v[:, rows] = dot_nt(dx_v[...], wq[rows, :]).astype(BF16)

        get_h.wait()
        wide = h_v[...].astype(F32)
        scale = inv_rms(wide)
        scaled = dn_v[...].astype(F32) * gain[...]
        inner = jnp.sum(scaled * wide, axis=1, keepdims=True)
        out[...] = (
            g_v[...].astype(F32)
            + scale * scaled
            - wide * (scale * scale * scale * inner * (1.0 / D))
        ).astype(BF16)
        put = pltpu.make_async_copy(out, grads.at[pl.ds(row0, LEN), :], sems.at[2])
        put.start()
        put.wait()


ANY = pl.BlockSpec(memory_space=pl.ANY)
VMEM = pl.BlockSpec(memory_space=pltpu.VMEM)
SMEM = pl.BlockSpec(memory_space=pltpu.SMEM)
LAYER_COST = pl.CostEstimate(
    flops=2 * LEN * D * (XW + QW), bytes_accessed=2 * D * (XW + QW), transcendentals=0
)
LIMIT = 24 * 1024 * 1024
SMALL = 8 * 1024 * 1024


def forward_layer(tick, last_stage, micro, meta, inbox, entry, gain, table, wq, wo, state):
    return pl.pallas_call(
        functools.partial(forward_kernel, tick, last_stage, micro),
        out_shape=(
            jax.ShapeDtypeStruct((LEN, D), BF16),
            *(jax.ShapeDtypeStruct(a.shape, a.dtype) for a in state),
        ),
        in_specs=[SMEM, ANY, ANY, VMEM, VMEM, VMEM, VMEM, ANY, ANY, ANY],
        out_specs=(VMEM, ANY, ANY, ANY),
        input_output_aliases={7: 1, 8: 2, 9: 3},
        scratch_shapes=[
            pltpu.VMEM((LEN, D), BF16),
            pltpu.VMEM((LEN, D), BF16),
            pltpu.VMEM((LEN, XW), F32),
            pltpu.VMEM((LEN, XW), BF16),
            pltpu.VMEM((LEN, QW), BF16),
            pltpu.VMEM((8, D), F32),
            pltpu.SemaphoreType.DMA((4,)),
        ],
        compiler_params=pltpu.CompilerParams(vmem_limit_bytes=LIMIT),
        cost_estimate=LAYER_COST,
        name="forward_layer",
    )(meta, inbox, entry, gain, table, wq, wo, *state)


def backward_layer(
    tick, last_stage, micro, meta, inbox, seed, gain, table, wq, wo, stash, grads
):
    return pl.pallas_call(
        functools.partial(backward_kernel, tick, last_stage, micro),
        out_shape=(
            jax.ShapeDtypeStruct((LEN, D), BF16),
            jax.ShapeDtypeStruct(grads.shape, grads.dtype),
        ),
        in_specs=[SMEM, VMEM, VMEM, VMEM, VMEM, VMEM, VMEM, ANY, ANY, ANY],
        out_specs=(VMEM, ANY),
        input_output_aliases={9: 1},
        scratch_shapes=[
            pltpu.VMEM((LEN, D), BF16),
            pltpu.VMEM((LEN, D), BF16),
            pltpu.VMEM((LEN, XW), BF16),
            pltpu.VMEM((LEN, QW), F32),
            pltpu.VMEM((LEN, XW), BF16),
            pltpu.VMEM((LEN, D), BF16),
            pltpu.SemaphoreType.DMA((3,)),
        ],
        compiler_params=pltpu.CompilerParams(vmem_limit_bytes=LIMIT),
        cost_estimate=LAYER_COST,
        name="backward_layer",
    )(meta, inbox, seed, gain, table, wq, wo, *stash, grads)


def pack_kernel(w_qkv, w_out, shard):
    shard[:, :XW] = w_qkv[...]
    pieces = [w_out[:, QW * j : QW * j + QW].astype(F32) for j in range(D // QW)]
    shard[:, XW:] = jnp.concatenate(pieces, axis=0).astype(BF16)


def pack(w_qkv, w_out):
    return pl.pallas_call(
        pack_kernel,
        out_shape=jax.ShapeDtypeStruct((w_qkv.shape[0], PACK), BF16),
        in_specs=[VMEM, VMEM],
        out_specs=VMEM,
        compiler_params=pltpu.CompilerParams(vmem_limit_bytes=SMALL),
        name="pack",
    )(w_qkv, w_out)


def unpack_kernel(packed, wq, wo, part_v, sems):
    parts = D // QW
    groups = 8
    rows = D // groups
    short = rows // (4 * parts)
    whole = pltpu.make_async_copy(packed.at[:, pl.ds(0, XW)], wq, sems.at[groups])

    def piece(i):
        at = pl.ds(pl.multiple_of(i * rows, rows), rows)
        return pltpu.make_async_copy(packed.at[at, pl.ds(XW, QW)], part_v.at[at, :], sems.at[i])

    for i in range(groups):
        piece(i).start()
    whole.start()

    @pl.loop(0, groups)
    def _(i):
        piece(i).wait()
        blocks = []
        for r in range(4):
            at = pl.ds(pl.multiple_of(i * rows + r * (rows // 4), 16), rows // 4)
            blocks.append(part_v[at, :].astype(F32))
        to = pl.ds(pl.multiple_of(i * (rows // 4), 16), rows // 4)
        for j in range(parts):
            cut = [block[short * j : short * j + short] for block in blocks]
            wo[to, QW * j : QW * j + QW] = jnp.concatenate(cut, axis=0).astype(BF16)

    whole.wait()


def unpack(packed):
    return pl.pallas_call(
        unpack_kernel,
        out_shape=(jax.ShapeDtypeStruct((D, XW), BF16), jax.ShapeDtypeStruct((QW, D), BF16)),
        in_specs=[ANY],
        out_specs=(VMEM, VMEM),
        scratch_shapes=[pltpu.VMEM((D, QW), BF16), pltpu.SemaphoreType.DMA((9,))],
        compiler_params=pltpu.CompilerParams(vmem_limit_bytes=LIMIT),
        name="unpack",
    )(packed)


WIDE = HALF + 128


def pooled_rows(last):
    return jnp.concatenate([last[j, 0:1, :] for j in (0, 2, 1, 3)], axis=0)


def embed_kernel(last, final_gain, labels, wq, wo, out):
    del wq, wo
    rows = pooled_rows(last)
    pooled = rows * inv_rms(rows) * final_gain[...]
    unit = pooled * lax.rsqrt(jnp.sum(pooled * pooled, axis=1, keepdims=True))
    halves = jnp.concatenate([unit[:, :HALF], unit[:, HALF:]], axis=0).astype(BF16)
    which = lax.broadcasted_iota(jnp.int32, (8, 128), 0)
    label = jnp.where(which == 0, labels[0], jnp.where(which == 1, labels[1], 0))
    label = label.astype(F32).astype(BF16)
    for i in range(out.shape[0]):
        out[i, :, :HALF] = halves
        out[i, :, HALF:] = label


def embed(count, last, final_gain, labels, wq, wo):
    return pl.pallas_call(
        functools.partial(embed_kernel),
        out_shape=jax.ShapeDtypeStruct((count, 8, WIDE), BF16),
        in_specs=[VMEM, VMEM, SMEM, VMEM, VMEM],
        out_specs=VMEM,
        compiler_params=pltpu.CompilerParams(vmem_limit_bytes=LIMIT),
        name="embed",
    )(last, final_gain, labels, wq, wo)


def loss_kernel(me, last, final_gain, everyone, wq, wo, seed):
    del wq, wo
    count = everyone.shape[0]
    emb = everyone[:, :HALF]
    label = everyone[:, HALF:].astype(F32)[:, 0:1].astype(jnp.int32)
    scores = dot_nt(emb, emb)
    scores = scores + pltpu.roll(pltpu.roll(scores, count - 4, 0), count - 4, 1)
    row = lax.rem(lax.broadcasted_iota(jnp.int32, (count, count), 0), 8)
    col = lax.broadcasted_iota(jnp.int32, (count, count), 1)
    doc = jnp.logical_and(lax.rem(col, 8) >= 2, lax.rem(col, 8) < 4)
    valid = jnp.logical_and(row < 2, doc)
    weights = jnp.where(valid, jnp.exp(scores * SHARP), 0.0)
    total = jnp.sum(weights, axis=1, keepdims=True)
    prob = weights / jnp.where(row[:, :1] < 2, total, 1.0)
    target = lax.div(label, 2) * 8 + 2 + lax.rem(label, 2)
    coef = jnp.where(valid, (prob - (col == target).astype(F32)) * (COEF * SHARP), 0.0)
    both = coef + coef.T
    mine = lax.broadcasted_iota(jnp.int32, (8, count), 0)
    pick = lax.broadcasted_iota(jnp.int32, (8, count), 1) == me[6] * 8 + mine
    own = lax.dot_general(
        pick.astype(F32),
        both,
        (((1,), (0,)), ((), ())),
        precision=lax.Precision.HIGHEST,
        preferred_element_type=F32,
    )[:4]
    own = jnp.concatenate([own, pltpu.roll(own, 4, 1)], axis=0)
    top = own.astype(BF16)
    rest = own - top.astype(F32)
    mid = rest.astype(BF16)
    low = (rest - mid.astype(F32)).astype(BF16)
    grad = dot_nn(top, emb) + (dot_nn(mid, emb) + dot_nn(low, emb))
    grad = jnp.concatenate([grad[:4], grad[4:]], axis=1)
    rows = pooled_rows(last)
    gain = final_gain[...]
    scale = inv_rms(rows)
    pooled = rows * scale * gain
    norm = lax.rsqrt(jnp.sum(pooled * pooled, axis=1, keepdims=True))
    unit = pooled * norm
    dpooled = norm * (grad - unit * jnp.sum(grad * unit, axis=1, keepdims=True))
    scaled = dpooled * gain
    inner = jnp.sum(scaled * rows, axis=1, keepdims=True)
    drow = scale * scaled - rows * (scale * scale * scale * inner * (1.0 / D))
    drow = drow.astype(BF16).astype(F32)
    seed[...] = jnp.concatenate(
        [drow[0:1], drow[2:3], drow[1:2], drow[3:4], jnp.zeros((4, D), F32)], axis=0
    )


def loss_seed(me, last, final_gain, everyone, wq, wo):
    return pl.pallas_call(
        loss_kernel,
        out_shape=jax.ShapeDtypeStruct((8, D), F32),
        in_specs=[SMEM, VMEM, VMEM, VMEM, VMEM, VMEM],
        out_specs=VMEM,
        compiler_params=pltpu.CompilerParams(vmem_limit_bytes=LIMIT),
        name="loss_seed",
    )(me, last, final_gain, everyone, wq, wo)


def rotary_table():
    lane = jnp.arange(128, dtype=jnp.int32)
    frequency = ROPE_BASE ** (-(lane % 32).astype(F32) * (2.0 / HEAD_DIM))
    angles = jnp.arange(LEN, dtype=F32)[:, None] * frequency[None, :]
    sign = jnp.where(lane % 64 < 32, -1.0, 1.0)
    return jnp.stack([jnp.cos(angles), jnp.sin(angles) * sign])


def per_device(entry, norm_gain, w_qkv, w_out, final_gain, lengths, positive):
    stage = lax.axis_index("section")
    stages = lax.axis_size("section")
    replica = lax.axis_index(DP)
    micro = lengths.shape[0]
    core = lax.axis_index("dp_2")
    meta = jnp.concatenate([stage[None], lengths, core[None], replica[None]])
    shard, final_row, meta = lax.optimization_barrier(
        (pack(w_qkv[0], w_out[0]), final_gain[None, :], meta)
    )
    wq, wo = unpack(lax.all_gather(shard, DP, axis=0, tiled=True))
    table = rotary_table()
    gain = norm_gain
    ticks = micro + stages - 1
    rows = micro * LEN
    state = (
        jnp.zeros((rows, D), BF16),
        jnp.zeros((rows, XW), BF16),
        jnp.zeros((micro, 8, D), F32),
    )
    inbox = entry[:LEN]
    for tick in range(ticks):
        out, *state = forward_layer(
            tick, stages - 1, micro, meta, inbox, entry, gain, table, wq, wo, state
        )
        if tick < ticks - 1:
            pairs = [(s, s + 1) for s in range(stages - 1) if 0 <= tick - s < micro]
            inbox = lax.ppermute(out, "section", pairs)
    stash_h, stash_x, last = state
    count = lax.axis_size(DP)
    copies = embed(count, last, final_row, positive, wq, wo)
    everyone = lax.all_to_all(copies, DP, split_axis=0, concat_axis=0, tiled=True)
    everyone = everyone.reshape(count * 8, WIDE)
    seed = loss_seed(meta, last, final_row, everyone, wq, wo)
    grads = jnp.zeros((rows, D), BF16)
    for tick in range(ticks):
        out, grads = backward_layer(
            tick, stages - 1, micro, meta, inbox, seed, gain, table, wq, wo,
            (stash_h, stash_x), grads,
        )
        if tick < ticks - 1:
            pairs = [
                (stages - 1 - s, stages - 2 - s)
                for s in range(stages - 1)
                if 0 <= tick - s < micro
            ]
            inbox = lax.ppermute(out, "section", pairs)
    return grads[None]


def solution(mesh):
    finer = Mesh(
        mesh.devices.reshape(mesh.shape["section"], 4, 4, 2), ("section", "dp_0", "dp_1", "dp_2")
    )
    in_specs = (
        P(DP, None),
        P("section", None),
        P("section", DP, None),
        P("section", DP, None),
        P(),
        P(DP),
        P(DP),
    )
    return jax.shard_map(
        per_device,
        mesh=finer,
        in_specs=in_specs,
        out_specs=P("section", DP, None),
        check_vma=False,
    )
```

```python
import functools

import jax
import jax.numpy as jnp
from jax import lax
from jax.experimental import pallas as pl
from jax.experimental.pallas import tpu as pltpu
from jax.sharding import Mesh
from jax.sharding import PartitionSpec as P

HEAD_DIM = 64
LEN = 48
D = 3584
QW = 896
KV = 128
XW = QW + 2 * KV
PACK = XW + QW
PAIRS = QW // 128
DP = ("dp_0", "dp_1", "dp_2")
ROPE_BASE = 1000000.0
EPS = 1e-06
SHARP = 20.0
COEF = 256.0
HALVES = 2
HALF = D // HALVES
STAGGER = 5000
EVEN = 800
F32 = jnp.float32
BF16 = jnp.bfloat16


def dot_nn(a, b):
    return lax.dot_general(a, b, (((1,), (0,)), ((), ())), preferred_element_type=F32)


def dot_nt(a, b):
    return lax.dot_general(a, b, (((1,), (1,)), ((), ())), preferred_element_type=F32)


def dot_tn(a, b):
    return lax.dot_general(a, b, (((0,), (0,)), ((), ())), preferred_element_type=F32)


def lanes(rows):
    return lax.broadcasted_iota(jnp.int32, (rows, 128), 1)


def partner(x):
    low = lax.rem(lanes(x.shape[0]), 64) < 32
    return jnp.where(low, pltpu.roll(x, 96, 1), pltpu.roll(x, 32, 1))


def paired(z):
    left = lanes(LEN) < 64
    rolled = pltpu.roll(z, 64, 1)
    pad = jnp.zeros((16, 128), BF16)
    a_left = jnp.where(left, z, 0.0).astype(BF16)
    b_right = jnp.where(left, 0.0, z).astype(BF16)
    b_left = jnp.where(left, rolled, 0.0).astype(BF16)
    a_right = jnp.where(left, 0.0, rolled).astype(BF16)
    return (
        jnp.concatenate([a_left, pad, a_right, pad], axis=0),
        jnp.concatenate([a_left, pad, b_right, pad], axis=0),
        jnp.concatenate([b_left, pad, b_right, pad], axis=0),
    )


SPANS = ((0, 3 * LEN), (3 * LEN, 4 * LEN), (4 * LEN, 7 * LEN))


def by_pair(dot, rows, blocks):
    return jnp.concatenate(
        [dot(rows[lo:hi], block) for (lo, hi), block in zip(SPANS, blocks)], axis=0
    )


def unpaired(rows, other):
    left = lanes(LEN) < 64
    s00, s01, s11 = (dot_tn(rows[lo:hi], other[lo:hi]) for lo, hi in SPANS)
    first = jnp.where(left, s00[:LEN] + s01[:LEN], 0.0)
    first += pltpu.roll(jnp.where(left, 0.0, s00[64 : 64 + LEN]), 64, 1)
    second = jnp.where(left, 0.0, s01[64 : 64 + LEN] + s11[64 : 64 + LEN])
    second += pltpu.roll(jnp.where(left, s11[:LEN], 0.0), 64, 1)
    return first + second


def half_sums(x):
    left = lanes(x.shape[0]) < 64
    low = jnp.sum(jnp.where(left, x, 0.0), axis=1, keepdims=True)
    high = jnp.sum(jnp.where(left, 0.0, x), axis=1, keepdims=True)
    return low, high, left


def probabilities(q_rows, k_blocks, length):
    scores = by_pair(dot_nt, q_rows, k_blocks) * HEAD_DIM ** (-0.5)
    live = lax.rem(lanes(scores.shape[0]), 64) < length
    weights = jnp.where(live, jnp.exp(scores), 0.0)
    low, high, left = half_sums(weights)
    return weights * jnp.where(left, 1.0 / low, 1.0 / high)


def rows_of(x_ref):
    return jnp.concatenate([x_ref[:, 128 * i : 128 * i + 128] for i in range(PAIRS)], axis=0)


def inv_rms(wide):
    return lax.rsqrt(jnp.sum(wide * wide, axis=1, keepdims=True) * (1.0 / D) + EPS)


def forward_kernel(
    tick,
    last_stage,
    micro,
    meta,
    inbox,
    entry,
    gain,
    table,
    wq,
    wo,
    *refs,
):
    out, stash_h, stash_x, last, h_v, n_v, acc_v, x_v, ctx_v, last_v, sems = refs[-11:]
    stage = meta[0]
    slot = tick - stage

    @pl.when(jnp.logical_and(slot >= 0, slot < micro))
    def _():
        length = meta[1 + slot]
        row0 = pl.multiple_of(slot * LEN, LEN)

        first = pltpu.make_async_copy(entry.at[pl.ds(row0, LEN), :], h_v, sems.at[0])
        later = pltpu.make_async_copy(inbox, h_v, sems.at[0])

        @pl.when(stage == 0)
        def _():
            first.start()

        @pl.when(stage != 0)
        def _():
            later.start()

        @pl.when(meta[5] == 1)
        def _():
            pl.delay(STAGGER if tick == 0 else EVEN)

        later.wait()
        keep_h = pltpu.make_async_copy(h_v, stash_h.at[pl.ds(row0, LEN), :], sems.at[1])
        keep_h.start()
        wide = h_v[...].astype(F32)
        n_v[...] = (wide * inv_rms(wide) * gain[...]).astype(BF16)
        acc_v[...] = dot_nn(n_v[...], wq[...])
        cosine, sine = table[0], table[1]
        for i in range(PAIRS + 1):
            part = acc_v[:, 128 * i : 128 * i + 128]
            x_v[:, 128 * i : 128 * i + 128] = (part * cosine + partner(part) * sine).astype(BF16)
        x_v[:, QW + KV :] = acc_v[:, QW + KV :].astype(BF16)
        keep_x = pltpu.make_async_copy(x_v, stash_x.at[pl.ds(row0, LEN), :], sems.at[2])
        keep_x.start()
        k_blocks = paired(x_v[:, QW : QW + KV].astype(F32))
        v_blocks = paired(x_v[:, QW + KV :].astype(F32))
        probs = probabilities(rows_of(x_v), k_blocks, length).astype(BF16)
        context = by_pair(dot_nn, probs, v_blocks).astype(BF16)
        for i in range(PAIRS):
            ctx_v[:, 128 * i : 128 * i + 128] = context[LEN * i : LEN * i + LEN]

        @pl.loop(0, HALVES)
        def _(i):
            cols = pl.ds(pl.multiple_of(i * HALF, HALF), HALF)
            branch = dot_nn(ctx_v[...], wo[:, cols])
            out[:, cols] = (h_v[:, cols].astype(F32) + branch).astype(BF16)

        @pl.when(stage == last_stage)
        def _():
            hit = lax.broadcasted_iota(jnp.int32, (LEN, D), 0) == length - 1
            row = jnp.sum(jnp.where(hit, out[...].astype(F32), 0.0), axis=0, keepdims=True)
            last_v[...] = jnp.broadcast_to(row, (8, D))
            put = pltpu.make_async_copy(last_v, last.at[slot], sems.at[3])
            put.start()
            put.wait()

        keep_h.wait()
        keep_x.wait()


def backward_kernel(
    tick,
    last_stage,
    micro,
    meta,
    inbox,
    seed,
    gain,
    table,
    wq,
    wo,
    stash_h,
    stash_x,
    *refs,
):
    out, grads, h_v, g_v, x_v, dctx_v, dx_v, dn_v, sems = refs[-9:]
    stage = meta[0]
    slot = tick - (last_stage - stage)

    @pl.when(jnp.logical_and(slot >= 0, slot < micro))
    def _():
        length = meta[1 + slot]
        row0 = pl.multiple_of(slot * LEN, LEN)

        get_x = pltpu.make_async_copy(stash_x.at[pl.ds(row0, LEN), :], x_v, sems.at[0])
        get_h = pltpu.make_async_copy(stash_h.at[pl.ds(row0, LEN), :], h_v, sems.at[1])
        get_x.start()
        get_h.start()
        @pl.when(meta[5] == 1)
        def _():
            pl.delay(STAGGER if tick == 0 else EVEN)


        @pl.when(stage == last_stage)
        def _():
            hit = lax.broadcasted_iota(jnp.int32, (LEN, D), 0) == length - 1
            row = jnp.where(lax.broadcasted_iota(jnp.int32, (8, D), 0) == slot, seed[...], 0.0)
            row = jnp.sum(row, axis=0, keepdims=True)
            g_v[...] = jnp.where(hit, jnp.broadcast_to(row, (LEN, D)), 0.0).astype(BF16)

        @pl.when(stage != last_stage)
        def _():
            g_v[...] = inbox[...]

        dctx_v[...] = dot_nn(g_v[...], wo[...])
        get_x.wait()
        q_rows = rows_of(x_v)
        k_blocks = paired(x_v[:, QW : QW + KV].astype(F32))
        v_blocks = paired(x_v[:, QW + KV :].astype(F32))
        probs = probabilities(q_rows, k_blocks, length)
        dctx = rows_of(dctx_v).astype(BF16)
        dvalue = unpaired(probs.astype(BF16), dctx)
        dprobs = by_pair(dot_nt, dctx, v_blocks).astype(BF16).astype(F32)
        low, high, left = half_sums(dprobs * probs)
        dscores = probs * (dprobs - jnp.where(left, low, high)) * HEAD_DIM ** (-0.5)
        dscores = dscores.astype(BF16)
        dquery = by_pair(dot_nn, dscores, k_blocks).astype(BF16).astype(F32)
        dkey = unpaired(dscores, q_rows).astype(BF16).astype(F32)
        cosine, sine = table[0], table[1]
        for i in range(PAIRS):
            part = dquery[LEN * i : LEN * i + LEN]
            dx_v[:, 128 * i : 128 * i + 128] = (part * cosine - partner(part) * sine).astype(BF16)
        dx_v[:, QW : QW + KV] = (dkey * cosine - partner(dkey) * sine).astype(BF16)
        dx_v[:, QW + KV :] = dvalue.astype(BF16)

        @pl.loop(0, HALVES)
        def _(i):
            cols = pl.ds(pl.multiple_of(i * HALF, HALF), HALF)
            dn_v[:, cols] = dot_nn(dx_v[...], wq[:, cols]).astype(BF16)

        get_h.wait()
        wide = h_v[...].astype(F32)
        scale = inv_rms(wide)
        scaled = dn_v[...].astype(F32) * gain[...]
        inner = jnp.sum(scaled * wide, axis=1, keepdims=True)
        out[...] = (
            g_v[...].astype(F32)
            + scale * scaled
            - wide * (scale * scale * scale * inner * (1.0 / D))
        ).astype(BF16)
        put = pltpu.make_async_copy(out, grads.at[pl.ds(row0, LEN), :], sems.at[2])
        put.start()
        put.wait()


ANY = pl.BlockSpec(memory_space=pl.ANY)
VMEM = pl.BlockSpec(memory_space=pltpu.VMEM)
SMEM = pl.BlockSpec(memory_space=pltpu.SMEM)
HBM = pl.BlockSpec(memory_space=pltpu.HBM)
LAYER_COST = pl.CostEstimate(
    flops=2 * LEN * D * (XW + QW), bytes_accessed=2 * D * (XW + QW), transcendentals=0
)
LIMIT = 8 * 1024 * 1024
LARGE = 14 * 1024 * 1024
SMALL = 8 * 1024 * 1024


def forward_layer(
    tick, last_stage, micro, meta, inbox, entry, gain, table, wq, wo, before, state
):
    rows = micro * LEN
    kept = (((rows, D), BF16), ((rows, XW), BF16), ((micro, 8, D), F32))
    return pl.pallas_call(
        functools.partial(forward_kernel, tick, last_stage, micro),
        out_shape=tuple(jax.ShapeDtypeStruct(*a) for a in (((LEN, D), BF16), *kept)),
        in_specs=[SMEM, ANY, ANY, VMEM, VMEM, VMEM, VMEM, *[ANY] * len((*before, *state))],
        out_specs=(VMEM, ANY, ANY, ANY),
        input_output_aliases={7 + len(before) + i: 1 + i for i in range(len(state))},
        scratch_shapes=[
            pltpu.VMEM((LEN, D), BF16),
            pltpu.VMEM((LEN, D), BF16),
            pltpu.VMEM((LEN, XW), F32),
            pltpu.VMEM((LEN, XW), BF16),
            pltpu.VMEM((LEN, QW), BF16),
            pltpu.VMEM((8, D), F32),
            pltpu.SemaphoreType.DMA((4,)),
        ],
        compiler_params=pltpu.CompilerParams(vmem_limit_bytes=LIMIT),
        cost_estimate=LAYER_COST,
        name="forward_layer",
    )(meta, inbox, entry, gain, table, wq, wo, *before, *state)


def backward_layer(
    tick, last_stage, micro, meta, inbox, seed, gain, table, wq_t, wo_t, stash, grads
):
    return pl.pallas_call(
        functools.partial(backward_kernel, tick, last_stage, micro),
        out_shape=(
            jax.ShapeDtypeStruct((LEN, D), BF16),
            jax.ShapeDtypeStruct((micro * LEN, D), BF16),
        ),
        in_specs=[SMEM, VMEM, VMEM, VMEM, VMEM, VMEM, VMEM, ANY, ANY, *[ANY] * len(grads)],
        out_specs=(VMEM, ANY),
        input_output_aliases={9 + i: 1 + i for i in range(len(grads))},
        scratch_shapes=[
            pltpu.VMEM((LEN, D), BF16),
            pltpu.VMEM((LEN, D), BF16),
            pltpu.VMEM((LEN, XW), BF16),
            pltpu.VMEM((LEN, QW), F32),
            pltpu.VMEM((LEN, XW), BF16),
            pltpu.VMEM((LEN, D), BF16),
            pltpu.SemaphoreType.DMA((3,)),
        ],
        compiler_params=pltpu.CompilerParams(vmem_limit_bytes=LIMIT),
        cost_estimate=LAYER_COST,
        name="backward_layer",
    )(meta, inbox, seed, gain, table, wq_t, wo_t, *stash, *grads)


TURN = 256


def turn_kernel(early, meta, after, wq, wo, *refs):
    del after
    wq_t, wo_t, wq_v, wo_v, sems = refs[-5:]
    half = lax.div(meta[7], 2)
    due = meta[0] >= half if early else meta[0] < half

    @pl.when(due)
    def _():
        def copies(i, slot):
            at = pl.ds(pl.multiple_of(i * TURN, TURN), TURN)
            return (
                pltpu.make_async_copy(wq_v.at[slot], wq_t.at[:, at], sems.at[0, slot]),
                pltpu.make_async_copy(wo_v.at[slot], wo_t.at[at, :], sems.at[1, slot]),
            )

        @pl.loop(0, D // TURN)
        def _(i):
            slot = lax.rem(i, 2)
            at = pl.ds(pl.multiple_of(i * TURN, TURN), TURN)

            @pl.when(i >= 2)
            def _():
                for copy in copies(i - 2, slot):
                    copy.wait()

            wq_v[slot] = wq[at, :].T
            wo_v[slot] = wo[:, at].T
            for copy in copies(i, slot):
                copy.start()

        for i in (D // TURN - 2, D // TURN - 1):
            for copy in copies(i, i % 2):
                copy.wait()


def turn(early, meta, after, wq, wo, turned):
    return pl.pallas_call(
        functools.partial(turn_kernel, early),
        out_shape=(jax.ShapeDtypeStruct((XW, D), BF16), jax.ShapeDtypeStruct((D, QW), BF16)),
        in_specs=[SMEM, ANY, VMEM, VMEM, *[ANY] * len(turned)],
        out_specs=(ANY, ANY),
        input_output_aliases={4 + i: i for i in range(len(turned))},
        scratch_shapes=[
            pltpu.VMEM((2, XW, TURN), BF16),
            pltpu.VMEM((2, TURN, QW), BF16),
            pltpu.SemaphoreType.DMA((2, 2)),
        ],
        compiler_params=pltpu.CompilerParams(vmem_limit_bytes=LIMIT),
        cost_estimate=pl.CostEstimate(flops=0, bytes_accessed=4 * D * (XW + QW), transcendentals=0),
        name="turn",
    )(meta, after, wq, wo, *turned)


def pack_kernel(w_qkv, w_out, shard, w_v, sems):
    first = pltpu.make_async_copy(w_out, w_v, sems.at[0])
    second = pltpu.make_async_copy(w_qkv, shard.at[:, pl.ds(0, XW)], sems.at[1])
    first.start()
    second.start()
    first.wait()
    pieces = [w_v[:, QW * j : QW * j + QW].astype(F32) for j in range(D // QW)]
    shard[:, XW:] = jnp.concatenate(pieces, axis=0).astype(BF16)
    second.wait()


def pack(w_qkv, w_out):
    return pl.pallas_call(
        pack_kernel,
        out_shape=jax.ShapeDtypeStruct((w_qkv.shape[0], PACK), BF16),
        in_specs=[HBM, HBM],
        out_specs=VMEM,
        scratch_shapes=[pltpu.VMEM(w_out.shape, BF16), pltpu.SemaphoreType.DMA((2,))],
        compiler_params=pltpu.CompilerParams(vmem_limit_bytes=SMALL),
        name="pack",
    )(w_qkv, w_out)


def unpack_kernel(packed, early, wq, wo, part_v, sems):
    del early
    parts = D // QW
    groups = 8
    rows = D // groups
    short = rows // (4 * parts)
    whole = pltpu.make_async_copy(packed.at[:, pl.ds(0, XW)], wq, sems.at[groups])

    def piece(i):
        at = pl.ds(pl.multiple_of(i * rows, rows), rows)
        return pltpu.make_async_copy(packed.at[at, pl.ds(XW, QW)], part_v.at[at, :], sems.at[i])

    for i in range(groups):
        piece(i).start()
    whole.start()

    @pl.loop(0, groups)
    def _(i):
        piece(i).wait()
        blocks = []
        for r in range(4):
            at = pl.ds(pl.multiple_of(i * rows + r * (rows // 4), 16), rows // 4)
            blocks.append(part_v[at, :].astype(F32))
        to = pl.ds(pl.multiple_of(i * (rows // 4), 16), rows // 4)
        for j in range(parts):
            cut = [block[short * j : short * j + short] for block in blocks]
            wo[to, QW * j : QW * j + QW] = jnp.concatenate(cut, axis=0).astype(BF16)

    whole.wait()


def unpack(packed, early):
    return pl.pallas_call(
        unpack_kernel,
        out_shape=(jax.ShapeDtypeStruct((D, XW), BF16), jax.ShapeDtypeStruct((QW, D), BF16)),
        in_specs=[HBM, VMEM],
        out_specs=(VMEM, VMEM),
        scratch_shapes=[pltpu.VMEM((D, QW), BF16), pltpu.SemaphoreType.DMA((9,))],
        compiler_params=pltpu.CompilerParams(vmem_limit_bytes=LARGE),
        name="unpack",
    )(packed, early)


WIDE = HALF + 128


def pooled_rows(last):
    return jnp.concatenate([last[j, 0:1, :] for j in (0, 2, 1, 3)], axis=0)


def embed_kernel(last, final_gain, labels, out):
    rows = pooled_rows(last)
    pooled = rows * inv_rms(rows) * final_gain[...]
    unit = pooled * lax.rsqrt(jnp.sum(pooled * pooled, axis=1, keepdims=True))
    halves = jnp.concatenate([unit[:, :HALF], unit[:, HALF:]], axis=0).astype(BF16)
    which = lax.broadcasted_iota(jnp.int32, (8, 128), 0)
    label = jnp.where(which == 0, labels[0], jnp.where(which == 1, labels[1], 0))
    label = label.astype(F32).astype(BF16)
    for i in range(out.shape[0]):
        out[i, :, :HALF] = halves
        out[i, :, HALF:] = label


def embed(count, last, final_gain, labels):
    return pl.pallas_call(
        embed_kernel,
        out_shape=jax.ShapeDtypeStruct((count, 8, WIDE), BF16),
        in_specs=[VMEM, VMEM, SMEM],
        out_specs=VMEM,
        compiler_params=pltpu.CompilerParams(vmem_limit_bytes=LIMIT),
        name="embed",
    )(last, final_gain, labels)


def loss_kernel(meta, last, final_gain, here, there, seed):
    everyone = jnp.concatenate([here[...], there[...]], axis=0)
    count = everyone.shape[0]
    emb = everyone[:, :HALF]
    label = everyone[:, HALF:].astype(F32)[:, 0:1].astype(jnp.int32)
    scores = dot_nt(emb, emb)
    scores = scores + pltpu.roll(pltpu.roll(scores, count - 4, 0), count - 4, 1)
    row = lax.rem(lax.broadcasted_iota(jnp.int32, (count, count), 0), 8)
    col = lax.broadcasted_iota(jnp.int32, (count, count), 1)
    doc = jnp.logical_and(lax.rem(col, 8) >= 2, lax.rem(col, 8) < 4)
    valid = jnp.logical_and(row < 2, doc)
    weights = jnp.where(valid, jnp.exp(scores * SHARP), 0.0)
    total = jnp.sum(weights, axis=1, keepdims=True)
    prob = weights / jnp.where(row[:, :1] < 2, total, 1.0)
    owner = lax.div(label, 2)
    away = (lax.rem(owner, 2) != meta[5]).astype(jnp.int32)
    target = away * (count // 2) + lax.div(owner, 2) * 8 + 2 + lax.rem(label, 2)
    coef = jnp.where(valid, (prob - (col == target).astype(F32)) * (COEF * SHARP), 0.0)
    both = coef + coef.T
    mine = lax.broadcasted_iota(jnp.int32, (8, count), 0)
    pick = lax.broadcasted_iota(jnp.int32, (8, count), 1) == lax.div(meta[6], 2) * 8 + mine
    own = lax.dot_general(
        pick.astype(F32),
        both,
        (((1,), (0,)), ((), ())),
        precision=lax.Precision.HIGHEST,
        preferred_element_type=F32,
    )[:4]
    own = jnp.concatenate([own, pltpu.roll(own, 4, 1)], axis=0)
    top = own.astype(BF16)
    rest = own - top.astype(F32)
    mid = rest.astype(BF16)
    low = (rest - mid.astype(F32)).astype(BF16)
    grad = dot_nn(top, emb) + (dot_nn(mid, emb) + dot_nn(low, emb))
    grad = jnp.concatenate([grad[:4], grad[4:]], axis=1)
    rows = pooled_rows(last)
    gain = final_gain[...]
    scale = inv_rms(rows)
    pooled = rows * scale * gain
    norm = lax.rsqrt(jnp.sum(pooled * pooled, axis=1, keepdims=True))
    unit = pooled * norm
    dpooled = norm * (grad - unit * jnp.sum(grad * unit, axis=1, keepdims=True))
    scaled = dpooled * gain
    inner = jnp.sum(scaled * rows, axis=1, keepdims=True)
    drow = scale * scaled - rows * (scale * scale * scale * inner * (1.0 / D))
    drow = drow.astype(BF16).astype(F32)
    seed[...] = jnp.concatenate(
        [drow[0:1], drow[2:3], drow[1:2], drow[3:4], jnp.zeros((4, D), F32)], axis=0
    )


def loss_seed(meta, last, final_gain, here, there):
    return pl.pallas_call(
        loss_kernel,
        out_shape=jax.ShapeDtypeStruct((8, D), F32),
        in_specs=[SMEM, VMEM, VMEM, VMEM, VMEM],
        out_specs=VMEM,
        compiler_params=pltpu.CompilerParams(vmem_limit_bytes=LIMIT),
        name="loss_seed",
    )(meta, last, final_gain, here, there)


def rotary_table():
    lane = jnp.arange(128, dtype=jnp.int32)
    frequency = ROPE_BASE ** (-(lane % 32).astype(F32) * (2.0 / HEAD_DIM))
    angles = jnp.arange(LEN, dtype=F32)[:, None] * frequency[None, :]
    sign = jnp.where(lane % 64 < 32, -1.0, 1.0)
    return jnp.stack([jnp.cos(angles), jnp.sin(angles) * sign])


def per_device(entry, norm_gain, w_qkv, w_out, final_gain, lengths, positive):
    stage = lax.axis_index("section")
    stages = lax.axis_size("section")
    replica = lax.axis_index(DP)
    core = lax.axis_index("dp_2")
    micro = lengths.shape[0]
    gain = norm_gain
    final_row = final_gain[None, :]
    packed = lax.all_gather(pack(w_qkv[0], w_out[0]), DP, axis=0, tiled=True)
    wq, wo = unpack(packed, final_row)
    numbers = jnp.array([stages], jnp.int32)
    meta = jnp.concatenate([stage[None], lengths, core[None], replica[None], numbers])
    table = rotary_table()
    ticks = micro + stages - 1
    half = stages // 2
    state, turned = (), ()
    inbox = entry[:LEN]
    for tick in range(ticks):
        before = turned if tick in (1, half + micro) else ()
        out, *state = forward_layer(
            tick, stages - 1, micro, meta, inbox, entry, gain, table, wq, wo, before, state
        )
        if tick == 0:
            turned = turn(True, meta, out, wq, wo, turned)
        if tick == half + micro - 1:
            turned = turn(False, meta, out, wq, wo, turned)
        if tick < ticks - 1:
            pairs = [(s, s + 1) for s in range(stages - 1) if 0 <= tick - s < micro]
            inbox = lax.ppermute(out, "section", pairs)
    *stash, last = state
    count = lax.axis_size(DP[:2])
    copies = embed(count, last, final_row, positive)
    here = lax.all_to_all(copies, DP[:2], split_axis=0, concat_axis=0, tiled=True)
    here = here.reshape(count * 8, WIDE)
    there = lax.ppermute(here, "dp_2", [(0, 1), (1, 0)])
    seed = loss_seed(meta, last, final_row, here, there)
    grads = ()
    for tick in range(ticks):
        out, *grads = backward_layer(
            tick, stages - 1, micro, meta, inbox, seed, gain, table, *turned, stash, grads
        )
        if tick < ticks - 1:
            pairs = [
                (stages - 1 - s, stages - 2 - s)
                for s in range(stages - 1)
                if 0 <= tick - s < micro
            ]
            inbox = lax.ppermute(out, "section", pairs)
    return grads[0][None]


def solution(mesh):
    finer = Mesh(
        mesh.devices.reshape(mesh.shape["section"], 4, 4, 2), ("section", "dp_0", "dp_1", "dp_2")
    )
    in_specs = (
        P(DP, None),
        P("section", None),
        P("section", DP, None),
        P("section", DP, None),
        P(),
        P(DP),
        P(DP),
    )
    return jax.shard_map(
        per_device,
        mesh=finer,
        in_specs=in_specs,
        out_specs=P("section", DP, None),
        check_vma=False,
    )
```

```python
import functools

import jax
import jax.numpy as jnp
from jax import lax
from jax.experimental import pallas as pl
from jax.experimental.pallas import tpu as pltpu
from jax.sharding import Mesh
from jax.sharding import PartitionSpec as P

HEAD_DIM = 64
LEN = 48
D = 3584
QW = 896
KV = 128
XW = QW + 2 * KV
PACK = XW + QW
PAIRS = QW // 128
DP = ("dp_0", "dp_1", "dp_2")
ROPE_BASE = 1000000.0
EPS = 1e-06
SHARP = 20.0
COEF = 256.0
HALVES = 2
HALF = D // HALVES
STAGGER = 6000
EVEN = 1050
F32 = jnp.float32
BF16 = jnp.bfloat16


def dot_nn(a, b):
    return lax.dot_general(a, b, (((1,), (0,)), ((), ())), preferred_element_type=F32)


def dot_nt(a, b):
    return lax.dot_general(a, b, (((1,), (1,)), ((), ())), preferred_element_type=F32)


def dot_tn(a, b):
    return lax.dot_general(a, b, (((0,), (0,)), ((), ())), preferred_element_type=F32)


def lanes(rows):
    return lax.broadcasted_iota(jnp.int32, (rows, 128), 1)


def partner(x):
    low = lax.rem(lanes(x.shape[0]), 64) < 32
    return jnp.where(low, pltpu.roll(x, 96, 1), pltpu.roll(x, 32, 1))


def paired(z):
    left = lanes(LEN) < 64
    rolled = pltpu.roll(z, 64, 1)
    pad = jnp.zeros((16, 128), BF16)
    a_left = jnp.where(left, z, 0.0).astype(BF16)
    b_right = jnp.where(left, 0.0, z).astype(BF16)
    b_left = jnp.where(left, rolled, 0.0).astype(BF16)
    a_right = jnp.where(left, 0.0, rolled).astype(BF16)
    return (
        jnp.concatenate([a_left, pad, a_right, pad], axis=0),
        jnp.concatenate([a_left, pad, b_right, pad], axis=0),
        jnp.concatenate([b_left, pad, b_right, pad], axis=0),
    )


SPANS = ((0, 3 * LEN), (3 * LEN, 4 * LEN), (4 * LEN, 7 * LEN))


def by_pair(dot, rows, blocks):
    return jnp.concatenate(
        [dot(rows[lo:hi], block) for (lo, hi), block in zip(SPANS, blocks)], axis=0
    )


def unpaired(rows, other):
    left = lanes(LEN) < 64
    s00, s01, s11 = (dot_tn(rows[lo:hi], other[lo:hi]) for lo, hi in SPANS)
    first = jnp.where(left, s00[:LEN] + s01[:LEN], 0.0)
    first += pltpu.roll(jnp.where(left, 0.0, s00[64 : 64 + LEN]), 64, 1)
    second = jnp.where(left, 0.0, s01[64 : 64 + LEN] + s11[64 : 64 + LEN])
    second += pltpu.roll(jnp.where(left, s11[:LEN], 0.0), 64, 1)
    return first + second


def half_sums(x):
    left = lanes(x.shape[0]) < 64
    low = jnp.sum(jnp.where(left, x, 0.0), axis=1, keepdims=True)
    high = jnp.sum(jnp.where(left, 0.0, x), axis=1, keepdims=True)
    return low, high, left


def probabilities(q_rows, k_blocks, length):
    scores = by_pair(dot_nt, q_rows, k_blocks) * HEAD_DIM ** (-0.5)
    live = lax.rem(lanes(scores.shape[0]), 64) < length
    weights = jnp.where(live, jnp.exp(scores), 0.0)
    low, high, left = half_sums(weights)
    return weights * jnp.where(left, 1.0 / low, 1.0 / high)


def rows_of(x_ref):
    return jnp.concatenate([x_ref[:, 128 * i : 128 * i + 128] for i in range(PAIRS)], axis=0)


def inv_rms(wide):
    return lax.rsqrt(jnp.sum(wide * wide, axis=1, keepdims=True) * (1.0 / D) + EPS)


def forward_kernel(
    tick,
    last_stage,
    micro,
    meta,
    inbox,
    entry,
    gain,
    table,
    wq,
    wo,
    *refs,
):
    out, stash_h, stash_x, last, h_v, n_v, acc_v, x_v, ctx_v, last_v, sems = refs[-11:]
    stage = meta[0]
    slot = tick - stage

    @pl.when(jnp.logical_and(slot >= 0, slot < micro))
    def _():
        length = meta[1 + slot]
        row0 = pl.multiple_of(slot * LEN, LEN)

        first = pltpu.make_async_copy(entry.at[pl.ds(row0, LEN), :], h_v, sems.at[0])
        later = pltpu.make_async_copy(inbox, h_v, sems.at[0])

        @pl.when(stage == 0)
        def _():
            first.start()

        @pl.when(stage != 0)
        def _():
            later.start()

        @pl.when(meta[5] == 1)
        def _():
            pl.delay(STAGGER if tick == 0 else EVEN)

        later.wait()
        keep_h = pltpu.make_async_copy(h_v, stash_h.at[pl.ds(row0, LEN), :], sems.at[1])
        keep_h.start()
        wide = h_v[...].astype(F32)
        n_v[...] = (wide * inv_rms(wide) * gain[...]).astype(BF16)
        acc_v[...] = dot_nn(n_v[...], wq[...])
        cosine, sine = table[0], table[1]
        for i in range(PAIRS + 1):
            part = acc_v[:, 128 * i : 128 * i + 128]
            x_v[:, 128 * i : 128 * i + 128] = (part * cosine + partner(part) * sine).astype(BF16)
        x_v[:, QW + KV :] = acc_v[:, QW + KV :].astype(BF16)
        keep_x = pltpu.make_async_copy(x_v, stash_x.at[pl.ds(row0, LEN), :], sems.at[2])
        keep_x.start()
        k_blocks = paired(x_v[:, QW : QW + KV].astype(F32))
        v_blocks = paired(x_v[:, QW + KV :].astype(F32))
        probs = probabilities(rows_of(x_v), k_blocks, length).astype(BF16)
        context = by_pair(dot_nn, probs, v_blocks).astype(BF16)
        for i in range(PAIRS):
            ctx_v[:, 128 * i : 128 * i + 128] = context[LEN * i : LEN * i + LEN]

        @pl.loop(0, HALVES)
        def _(i):
            cols = pl.ds(pl.multiple_of(i * HALF, HALF), HALF)
            branch = dot_nn(ctx_v[...], wo[:, cols])
            out[:, cols] = (h_v[:, cols].astype(F32) + branch).astype(BF16)

        @pl.when(stage == last_stage)
        def _():
            hit = lax.broadcasted_iota(jnp.int32, (LEN, D), 0) == length - 1
            row = jnp.sum(jnp.where(hit, out[...].astype(F32), 0.0), axis=0, keepdims=True)
            last_v[...] = jnp.broadcast_to(row, (8, D))
            put = pltpu.make_async_copy(last_v, last.at[slot], sems.at[3])
            put.start()
            put.wait()

        keep_h.wait()
        keep_x.wait()


def backward_kernel(
    tick,
    last_stage,
    micro,
    meta,
    inbox,
    seed,
    gain,
    table,
    wq,
    wo,
    stash_h,
    stash_x,
    *refs,
):
    out, grads, h_v, g_v, x_v, dctx_v, dx_v, dn_v, sems = refs[-9:]
    stage = meta[0]
    slot = tick - (last_stage - stage)

    @pl.when(jnp.logical_and(slot >= 0, slot < micro))
    def _():
        length = meta[1 + slot]
        row0 = pl.multiple_of(slot * LEN, LEN)

        get_x = pltpu.make_async_copy(stash_x.at[pl.ds(row0, LEN), :], x_v, sems.at[0])
        get_h = pltpu.make_async_copy(stash_h.at[pl.ds(row0, LEN), :], h_v, sems.at[1])
        get_x.start()
        get_h.start()
        @pl.when(meta[5] == 1)
        def _():
            pl.delay(STAGGER if tick == 0 else EVEN)


        @pl.when(stage == last_stage)
        def _():
            hit = lax.broadcasted_iota(jnp.int32, (LEN, D), 0) == length - 1
            row = jnp.where(lax.broadcasted_iota(jnp.int32, (8, D), 0) == slot, seed[...], 0.0)
            row = jnp.sum(row, axis=0, keepdims=True)
            g_v[...] = jnp.where(hit, jnp.broadcast_to(row, (LEN, D)), 0.0).astype(BF16)

        @pl.when(stage != last_stage)
        def _():
            g_v[...] = inbox[...]

        dctx_v[...] = dot_nn(g_v[...], wo[...])
        get_x.wait()
        q_rows = rows_of(x_v)
        k_blocks = paired(x_v[:, QW : QW + KV].astype(F32))
        v_blocks = paired(x_v[:, QW + KV :].astype(F32))
        probs = probabilities(q_rows, k_blocks, length)
        dctx = rows_of(dctx_v).astype(BF16)
        dvalue = unpaired(probs.astype(BF16), dctx)
        dprobs = by_pair(dot_nt, dctx, v_blocks).astype(BF16).astype(F32)
        low, high, left = half_sums(dprobs * probs)
        dscores = probs * (dprobs - jnp.where(left, low, high)) * HEAD_DIM ** (-0.5)
        dscores = dscores.astype(BF16)
        dquery = by_pair(dot_nn, dscores, k_blocks).astype(BF16).astype(F32)
        dkey = unpaired(dscores, q_rows).astype(BF16).astype(F32)
        cosine, sine = table[0], table[1]
        for i in range(PAIRS):
            part = dquery[LEN * i : LEN * i + LEN]
            dx_v[:, 128 * i : 128 * i + 128] = (part * cosine - partner(part) * sine).astype(BF16)
        dx_v[:, QW : QW + KV] = (dkey * cosine - partner(dkey) * sine).astype(BF16)
        dx_v[:, QW + KV :] = dvalue.astype(BF16)

        @pl.loop(0, HALVES)
        def _(i):
            cols = pl.ds(pl.multiple_of(i * HALF, HALF), HALF)
            dn_v[:, cols] = dot_nn(dx_v[...], wq[:, cols]).astype(BF16)

        get_h.wait()
        wide = h_v[...].astype(F32)
        scale = inv_rms(wide)
        scaled = dn_v[...].astype(F32) * gain[...]
        inner = jnp.sum(scaled * wide, axis=1, keepdims=True)
        out[...] = (
            g_v[...].astype(F32)
            + scale * scaled
            - wide * (scale * scale * scale * inner * (1.0 / D))
        ).astype(BF16)
        put = pltpu.make_async_copy(out, grads.at[pl.ds(row0, LEN), :], sems.at[2])
        put.start()
        put.wait()


ANY = pl.BlockSpec(memory_space=pl.ANY)
VMEM = pl.BlockSpec(memory_space=pltpu.VMEM)
SMEM = pl.BlockSpec(memory_space=pltpu.SMEM)
HBM = pl.BlockSpec(memory_space=pltpu.HBM)
LAYER_COST = pl.CostEstimate(
    flops=2 * LEN * D * (XW + QW), bytes_accessed=2 * D * (XW + QW), transcendentals=0
)
LIMIT = 8 * 1024 * 1024
LARGE = 14 * 1024 * 1024
WHOLE = 60 * 1024 * 1024
SMALL = 8 * 1024 * 1024


def forward_layer(
    tick, last_stage, micro, meta, inbox, entry, gain, table, wq, wo, before, state
):
    rows = micro * LEN
    kept = (((rows, D), BF16), ((rows, XW), BF16), ((micro, 8, D), F32))
    return pl.pallas_call(
        functools.partial(forward_kernel, tick, last_stage, micro),
        out_shape=tuple(jax.ShapeDtypeStruct(*a) for a in (((LEN, D), BF16), *kept)),
        in_specs=[SMEM, ANY, ANY, VMEM, VMEM, VMEM, VMEM, *[ANY] * len((*before, *state))],
        out_specs=(VMEM, ANY, ANY, ANY),
        input_output_aliases={7 + len(before) + i: 1 + i for i in range(len(state))},
        scratch_shapes=[
            pltpu.VMEM((LEN, D), BF16),
            pltpu.VMEM((LEN, D), BF16),
            pltpu.VMEM((LEN, XW), F32),
            pltpu.VMEM((LEN, XW), BF16),
            pltpu.VMEM((LEN, QW), BF16),
            pltpu.VMEM((8, D), F32),
            pltpu.SemaphoreType.DMA((4,)),
        ],
        compiler_params=pltpu.CompilerParams(vmem_limit_bytes=LIMIT),
        cost_estimate=LAYER_COST,
        name="forward_layer",
    )(meta, inbox, entry, gain, table, wq, wo, *before, *state)


def backward_layer(
    tick, last_stage, micro, meta, inbox, seed, gain, table, wq_t, wo_t, stash, grads
):
    return pl.pallas_call(
        functools.partial(backward_kernel, tick, last_stage, micro),
        out_shape=(
            jax.ShapeDtypeStruct((LEN, D), BF16),
            jax.ShapeDtypeStruct((micro * LEN, D), BF16),
        ),
        in_specs=[SMEM, VMEM, VMEM, VMEM, VMEM, VMEM, VMEM, ANY, ANY, *[ANY] * len(grads)],
        out_specs=(VMEM, ANY),
        input_output_aliases={9 + i: 1 + i for i in range(len(grads))},
        scratch_shapes=[
            pltpu.VMEM((LEN, D), BF16),
            pltpu.VMEM((LEN, D), BF16),
            pltpu.VMEM((LEN, XW), BF16),
            pltpu.VMEM((LEN, QW), F32),
            pltpu.VMEM((LEN, XW), BF16),
            pltpu.VMEM((LEN, D), BF16),
            pltpu.SemaphoreType.DMA((3,)),
        ],
        compiler_params=pltpu.CompilerParams(vmem_limit_bytes=LIMIT),
        cost_estimate=LAYER_COST,
        name="backward_layer",
    )(meta, inbox, seed, gain, table, wq_t, wo_t, *stash, *grads)


TURN = 256


def turn_kernel(early, meta, after, wq, wo, *refs):
    del after
    wq_t, wo_t, wq_v, wo_v, sems = refs[-5:]
    half = lax.div(meta[7], 2)
    due = meta[0] >= half if early else meta[0] < half

    @pl.when(due)
    def _():
        def copies(i, slot):
            at = pl.ds(pl.multiple_of(i * TURN, TURN), TURN)
            return (
                pltpu.make_async_copy(wq_v.at[slot], wq_t.at[:, at], sems.at[0, slot]),
                pltpu.make_async_copy(wo_v.at[slot], wo_t.at[at, :], sems.at[1, slot]),
            )

        @pl.loop(0, D // TURN)
        def _(i):
            slot = lax.rem(i, 2)
            at = pl.ds(pl.multiple_of(i * TURN, TURN), TURN)

            @pl.when(i >= 2)
            def _():
                for copy in copies(i - 2, slot):
                    copy.wait()

            wq_v[slot] = wq[at, :].T
            wo_v[slot] = wo[:, at].T
            for copy in copies(i, slot):
                copy.start()

        for i in (D // TURN - 2, D // TURN - 1):
            for copy in copies(i, i % 2):
                copy.wait()


def turn(early, meta, after, wq, wo, turned):
    return pl.pallas_call(
        functools.partial(turn_kernel, early),
        out_shape=(jax.ShapeDtypeStruct((XW, D), BF16), jax.ShapeDtypeStruct((D, QW), BF16)),
        in_specs=[SMEM, ANY, VMEM, VMEM, *[ANY] * len(turned)],
        out_specs=(ANY, ANY),
        input_output_aliases={4 + i: i for i in range(len(turned))},
        scratch_shapes=[
            pltpu.VMEM((2, XW, TURN), BF16),
            pltpu.VMEM((2, TURN, QW), BF16),
            pltpu.SemaphoreType.DMA((2, 2)),
        ],
        compiler_params=pltpu.CompilerParams(vmem_limit_bytes=LIMIT),
        cost_estimate=pl.CostEstimate(flops=0, bytes_accessed=4 * D * (XW + QW), transcendentals=0),
        name="turn",
    )(meta, after, wq, wo, *turned)


def pack_kernel(w_qkv, w_out, shard, w_v, sems):
    first = pltpu.make_async_copy(w_out, w_v, sems.at[0])
    second = pltpu.make_async_copy(w_qkv, shard.at[:, pl.ds(0, XW)], sems.at[1])
    first.start()
    second.start()
    first.wait()
    pieces = [w_v[:, QW * j : QW * j + QW].astype(F32) for j in range(D // QW)]
    shard[:, XW:] = jnp.concatenate(pieces, axis=0).astype(BF16)
    second.wait()


def pack(w_qkv, w_out):
    return pl.pallas_call(
        pack_kernel,
        out_shape=jax.ShapeDtypeStruct((w_qkv.shape[0], PACK), BF16),
        in_specs=[HBM, HBM],
        out_specs=VMEM,
        scratch_shapes=[pltpu.VMEM(w_out.shape, BF16), pltpu.SemaphoreType.DMA((2,))],
        compiler_params=pltpu.CompilerParams(vmem_limit_bytes=WHOLE),
        name="pack",
    )(w_qkv, w_out)


def unpack_kernel(packed, early, wq, wo, part_v, sems):
    del early
    parts = D // QW
    groups = 8
    rows = D // groups
    short = rows // (4 * parts)
    whole = pltpu.make_async_copy(packed.at[:, pl.ds(0, XW)], wq, sems.at[groups])

    def piece(i):
        at = pl.ds(pl.multiple_of(i * rows, rows), rows)
        return pltpu.make_async_copy(packed.at[at, pl.ds(XW, QW)], part_v.at[at, :], sems.at[i])

    for i in range(groups):
        piece(i).start()
    whole.start()

    @pl.loop(0, groups)
    def _(i):
        piece(i).wait()
        blocks = []
        for r in range(4):
            at = pl.ds(pl.multiple_of(i * rows + r * (rows // 4), 16), rows // 4)
            blocks.append(part_v[at, :].astype(F32))
        to = pl.ds(pl.multiple_of(i * (rows // 4), 16), rows // 4)
        for j in range(parts):
            cut = [block[short * j : short * j + short] for block in blocks]
            wo[to, QW * j : QW * j + QW] = jnp.concatenate(cut, axis=0).astype(BF16)

    whole.wait()


def unpack(packed, early):
    return pl.pallas_call(
        unpack_kernel,
        out_shape=(jax.ShapeDtypeStruct((D, XW), BF16), jax.ShapeDtypeStruct((QW, D), BF16)),
        in_specs=[HBM, VMEM],
        out_specs=(VMEM, VMEM),
        scratch_shapes=[pltpu.VMEM((D, QW), BF16), pltpu.SemaphoreType.DMA((9,))],
        compiler_params=pltpu.CompilerParams(vmem_limit_bytes=LARGE),
        name="unpack",
    )(packed, early)


WIDE = HALF + 128


def pooled_rows(last):
    return jnp.concatenate([last[j, 0:1, :] for j in (0, 2, 1, 3)], axis=0)


def embed_kernel(last, final_gain, labels, out):
    rows = pooled_rows(last)
    pooled = rows * inv_rms(rows) * final_gain[...]
    unit = pooled * lax.rsqrt(jnp.sum(pooled * pooled, axis=1, keepdims=True))
    halves = jnp.concatenate([unit[:, :HALF], unit[:, HALF:]], axis=0).astype(BF16)
    which = lax.broadcasted_iota(jnp.int32, (8, 128), 0)
    label = jnp.where(which == 0, labels[0], jnp.where(which == 1, labels[1], 0))
    label = label.astype(F32).astype(BF16)
    for i in range(out.shape[0]):
        out[i, :, :HALF] = halves
        out[i, :, HALF:] = label


def embed(count, last, final_gain, labels):
    return pl.pallas_call(
        embed_kernel,
        out_shape=jax.ShapeDtypeStruct((count, 8, WIDE), BF16),
        in_specs=[VMEM, VMEM, SMEM],
        out_specs=VMEM,
        compiler_params=pltpu.CompilerParams(vmem_limit_bytes=LIMIT),
        name="embed",
    )(last, final_gain, labels)


def loss_kernel(meta, last, final_gain, here, there, seed):
    everyone = jnp.concatenate([here[...], there[...]], axis=0)
    count = everyone.shape[0]
    emb = everyone[:, :HALF]
    label = everyone[:, HALF:].astype(F32)[:, 0:1].astype(jnp.int32)
    scores = dot_nt(emb, emb)
    scores = scores + pltpu.roll(pltpu.roll(scores, count - 4, 0), count - 4, 1)
    row = lax.rem(lax.broadcasted_iota(jnp.int32, (count, count), 0), 8)
    col = lax.broadcasted_iota(jnp.int32, (count, count), 1)
    doc = jnp.logical_and(lax.rem(col, 8) >= 2, lax.rem(col, 8) < 4)
    valid = jnp.logical_and(row < 2, doc)
    weights = jnp.where(valid, jnp.exp(scores * SHARP), 0.0)
    total = jnp.sum(weights, axis=1, keepdims=True)
    prob = weights / jnp.where(row[:, :1] < 2, total, 1.0)
    owner = lax.div(label, 2)
    away = (lax.rem(owner, 2) != meta[5]).astype(jnp.int32)
    target = away * (count // 2) + lax.div(owner, 2) * 8 + 2 + lax.rem(label, 2)
    coef = jnp.where(valid, (prob - (col == target).astype(F32)) * (COEF * SHARP), 0.0)
    both = coef + coef.T
    mine = lax.broadcasted_iota(jnp.int32, (8, count), 0)
    pick = lax.broadcasted_iota(jnp.int32, (8, count), 1) == lax.div(meta[6], 2) * 8 + mine
    own = lax.dot_general(
        pick.astype(F32),
        both,
        (((1,), (0,)), ((), ())),
        precision=lax.Precision.HIGHEST,
        preferred_element_type=F32,
    )[:4]
    own = jnp.concatenate([own, pltpu.roll(own, 4, 1)], axis=0)
    top = own.astype(BF16)
    rest = own - top.astype(F32)
    mid = rest.astype(BF16)
    low = (rest - mid.astype(F32)).astype(BF16)
    grad = dot_nn(top, emb) + (dot_nn(mid, emb) + dot_nn(low, emb))
    grad = jnp.concatenate([grad[:4], grad[4:]], axis=1)
    rows = pooled_rows(last)
    gain = final_gain[...]
    scale = inv_rms(rows)
    pooled = rows * scale * gain
    norm = lax.rsqrt(jnp.sum(pooled * pooled, axis=1, keepdims=True))
    unit = pooled * norm
    dpooled = norm * (grad - unit * jnp.sum(grad * unit, axis=1, keepdims=True))
    scaled = dpooled * gain
    inner = jnp.sum(scaled * rows, axis=1, keepdims=True)
    drow = scale * scaled - rows * (scale * scale * scale * inner * (1.0 / D))
    drow = drow.astype(BF16).astype(F32)
    seed[...] = jnp.concatenate(
        [drow[0:1], drow[2:3], drow[1:2], drow[3:4], jnp.zeros((4, D), F32)], axis=0
    )


def loss_seed(meta, last, final_gain, here, there):
    return pl.pallas_call(
        loss_kernel,
        out_shape=jax.ShapeDtypeStruct((8, D), F32),
        in_specs=[SMEM, VMEM, VMEM, VMEM, VMEM],
        out_specs=VMEM,
        compiler_params=pltpu.CompilerParams(vmem_limit_bytes=LIMIT),
        name="loss_seed",
    )(meta, last, final_gain, here, there)


def rotary_table():
    lane = jnp.arange(128, dtype=jnp.int32)
    frequency = ROPE_BASE ** (-(lane % 32).astype(F32) * (2.0 / HEAD_DIM))
    angles = jnp.arange(LEN, dtype=F32)[:, None] * frequency[None, :]
    sign = jnp.where(lane % 64 < 32, -1.0, 1.0)
    return jnp.stack([jnp.cos(angles), jnp.sin(angles) * sign])


def per_device(entry, norm_gain, w_qkv, w_out, final_gain, lengths, positive):
    stage = lax.axis_index("section")
    stages = lax.axis_size("section")
    replica = lax.axis_index(DP)
    core = lax.axis_index("dp_2")
    micro = lengths.shape[0]
    gain = norm_gain
    final_row = final_gain[None, :]
    packed = lax.all_gather(pack(w_qkv[0], w_out[0]), DP, axis=0, tiled=True)
    wq, wo = unpack(packed, final_row)
    numbers = jnp.array([stages], jnp.int32)
    meta = jnp.concatenate([stage[None], lengths, core[None], replica[None], numbers])
    table = rotary_table()
    ticks = micro + stages - 1
    half = stages // 2
    state, turned = (), ()
    inbox = entry[:LEN]
    for tick in range(ticks):
        before = turned if tick in (1, half + micro) else ()
        out, *state = forward_layer(
            tick, stages - 1, micro, meta, inbox, entry, gain, table, wq, wo, before, state
        )
        if tick == 0:
            turned = turn(True, meta, out, wq, wo, turned)
        if tick == half + micro - 1:
            turned = turn(False, meta, out, wq, wo, turned)
        if tick < ticks - 1:
            pairs = [(s, s + 1) for s in range(stages - 1) if 0 <= tick - s < micro]
            inbox = lax.ppermute(out, "section", pairs)
    *stash, last = state
    count = lax.axis_size(DP[:2])
    copies = embed(count, last, final_row, positive)
    here = lax.all_to_all(copies, DP[:2], split_axis=0, concat_axis=0, tiled=True)
    here = here.reshape(count * 8, WIDE)
    there = lax.ppermute(here, "dp_2", [(0, 1), (1, 0)])
    seed = loss_seed(meta, last, final_row, here, there)
    grads = ()
    for tick in range(ticks):
        out, *grads = backward_layer(
            tick, stages - 1, micro, meta, inbox, seed, gain, table, *turned, stash, grads
        )
        if tick < ticks - 1:
            pairs = [
                (stages - 1 - s, stages - 2 - s)
                for s in range(stages - 1)
                if 0 <= tick - s < micro
            ]
            inbox = lax.ppermute(out, "section", pairs)
    return grads[0][None]


def solution(mesh):
    finer = Mesh(
        mesh.devices.reshape(mesh.shape["section"], 4, 4, 2), ("section", "dp_0", "dp_1", "dp_2")
    )
    in_specs = (
        P(DP, None),
        P("section", None),
        P("section", DP, None),
        P("section", DP, None),
        P(),
        P(DP),
        P(DP),
    )
    return jax.shard_map(
        per_device,
        mesh=finer,
        in_specs=in_specs,
        out_specs=P("section", DP, None),
        check_vma=False,
    )
```

```python
import functools

import jax
import jax.numpy as jnp
from jax import lax
from jax.experimental import pallas as pl
from jax.experimental.pallas import tpu as pltpu
from jax.sharding import Mesh
from jax.sharding import PartitionSpec as P

HEAD_DIM = 64
LEN = 48
D = 3584
QW = 896
KV = 128
XW = QW + 2 * KV
PACK = XW + QW
PAIRS = QW // 128
DP = ("dp_0", "dp_1", "dp_2")
ROPE_BASE = 1000000.0
EPS = 1e-06
SHARP = 20.0
COEF = 256.0
HALVES = 2
HALF = D // HALVES
STAGGER = 6000
EVEN = 1050
F32 = jnp.float32
BF16 = jnp.bfloat16


def dot_nn(a, b):
    return lax.dot_general(a, b, (((1,), (0,)), ((), ())), preferred_element_type=F32)


def dot_nt(a, b):
    return lax.dot_general(a, b, (((1,), (1,)), ((), ())), preferred_element_type=F32)


def dot_tn(a, b):
    return lax.dot_general(a, b, (((0,), (0,)), ((), ())), preferred_element_type=F32)


def lanes(rows):
    return lax.broadcasted_iota(jnp.int32, (rows, 128), 1)


def partner(x):
    low = lax.rem(lanes(x.shape[0]), 64) < 32
    return jnp.where(low, pltpu.roll(x, 96, 1), pltpu.roll(x, 32, 1))


def paired(z):
    left = lanes(LEN) < 64
    rolled = pltpu.roll(z, 64, 1)
    pad = jnp.zeros((16, 128), BF16)
    a_left = jnp.where(left, z, 0.0).astype(BF16)
    b_right = jnp.where(left, 0.0, z).astype(BF16)
    b_left = jnp.where(left, rolled, 0.0).astype(BF16)
    a_right = jnp.where(left, 0.0, rolled).astype(BF16)
    return (
        jnp.concatenate([a_left, pad, a_right, pad], axis=0),
        jnp.concatenate([a_left, pad, b_right, pad], axis=0),
        jnp.concatenate([b_left, pad, b_right, pad], axis=0),
    )


SPANS = ((0, 3 * LEN), (3 * LEN, 4 * LEN), (4 * LEN, 7 * LEN))


def by_pair(dot, rows, blocks):
    return jnp.concatenate(
        [dot(rows[lo:hi], block) for (lo, hi), block in zip(SPANS, blocks)], axis=0
    )


def unpaired(rows, other):
    left = lanes(LEN) < 64
    s00, s01, s11 = (dot_tn(rows[lo:hi], other[lo:hi]) for lo, hi in SPANS)
    first = jnp.where(left, s00[:LEN] + s01[:LEN], 0.0)
    first += pltpu.roll(jnp.where(left, 0.0, s00[64 : 64 + LEN]), 64, 1)
    second = jnp.where(left, 0.0, s01[64 : 64 + LEN] + s11[64 : 64 + LEN])
    second += pltpu.roll(jnp.where(left, s11[:LEN], 0.0), 64, 1)
    return first + second


def half_sums(x):
    left = lanes(x.shape[0]) < 64
    low = jnp.sum(jnp.where(left, x, 0.0), axis=1, keepdims=True)
    high = jnp.sum(jnp.where(left, 0.0, x), axis=1, keepdims=True)
    return low, high, left


def probabilities(q_rows, k_blocks, length):
    scores = by_pair(dot_nt, q_rows, k_blocks) * HEAD_DIM ** (-0.5)
    live = lax.rem(lanes(scores.shape[0]), 64) < length
    weights = jnp.where(live, jnp.exp(scores), 0.0)
    low, high, left = half_sums(weights)
    return weights * jnp.where(left, 1.0 / low, 1.0 / high)


def rows_of(x_ref):
    return jnp.concatenate([x_ref[:, 128 * i : 128 * i + 128] for i in range(PAIRS)], axis=0)


def inv_rms(wide):
    return lax.rsqrt(jnp.sum(wide * wide, axis=1, keepdims=True) * (1.0 / D) + EPS)


def forward_kernel(
    tick,
    last_stage,
    micro,
    meta,
    inbox,
    entry,
    gain,
    table,
    wq,
    wo,
    *refs,
):
    out, stash_h, stash_x, last, h_v, n_v, acc_v, x_v, ctx_v, last_v, sems = refs[-11:]
    stage = meta[0]
    slot = tick - stage

    @pl.when(jnp.logical_and(slot >= 0, slot < micro))
    def _():
        length = meta[1 + slot]
        row0 = pl.multiple_of(slot * LEN, LEN)

        first = pltpu.make_async_copy(entry.at[pl.ds(row0, LEN), :], h_v, sems.at[0])
        later = pltpu.make_async_copy(inbox, h_v, sems.at[0])

        @pl.when(stage == 0)
        def _():
            first.start()

        @pl.when(stage != 0)
        def _():
            later.start()

        @pl.when(meta[5] == 1)
        def _():
            pl.delay(STAGGER if tick == 0 else EVEN)

        later.wait()
        keep_h = pltpu.make_async_copy(h_v, stash_h.at[pl.ds(row0, LEN), :], sems.at[1])
        keep_h.start()
        wide = h_v[...].astype(F32)
        n_v[...] = (wide * inv_rms(wide) * gain[...]).astype(BF16)
        acc_v[...] = dot_nn(n_v[...], wq[...])
        cosine, sine = table[0], table[1]
        for i in range(PAIRS + 1):
            part = acc_v[:, 128 * i : 128 * i + 128]
            x_v[:, 128 * i : 128 * i + 128] = (part * cosine + partner(part) * sine).astype(BF16)
        x_v[:, QW + KV :] = acc_v[:, QW + KV :].astype(BF16)
        keep_x = pltpu.make_async_copy(x_v, stash_x.at[pl.ds(row0, LEN), :], sems.at[2])
        keep_x.start()
        k_blocks = paired(x_v[:, QW : QW + KV].astype(F32))
        v_blocks = paired(x_v[:, QW + KV :].astype(F32))
        probs = probabilities(rows_of(x_v), k_blocks, length).astype(BF16)
        context = by_pair(dot_nn, probs, v_blocks).astype(BF16)
        for i in range(PAIRS):
            ctx_v[:, 128 * i : 128 * i + 128] = context[LEN * i : LEN * i + LEN]

        @pl.loop(0, HALVES)
        def _(i):
            cols = pl.ds(pl.multiple_of(i * HALF, HALF), HALF)
            branch = dot_nn(ctx_v[...], wo[:, cols])
            out[:, cols] = (h_v[:, cols].astype(F32) + branch).astype(BF16)

        @pl.when(stage == last_stage)
        def _():
            hit = lax.broadcasted_iota(jnp.int32, (LEN, D), 0) == length - 1
            row = jnp.sum(jnp.where(hit, out[...].astype(F32), 0.0), axis=0, keepdims=True)
            last_v[...] = jnp.broadcast_to(row, (8, D))
            put = pltpu.make_async_copy(last_v, last.at[slot], sems.at[3])
            put.start()
            put.wait()

        keep_h.wait()
        keep_x.wait()


def backward_kernel(
    tick,
    last_stage,
    micro,
    meta,
    inbox,
    seed,
    gain,
    table,
    wq,
    wo,
    stash_h,
    stash_x,
    *refs,
):
    out, grads, h_v, g_v, x_v, dctx_v, dx_v, dn_v, sems = refs[-9:]
    stage = meta[0]
    slot = tick - (last_stage - stage)

    @pl.when(jnp.logical_and(slot >= 0, slot < micro))
    def _():
        length = meta[1 + slot]
        row0 = pl.multiple_of(slot * LEN, LEN)

        get_x = pltpu.make_async_copy(stash_x.at[pl.ds(row0, LEN), :], x_v, sems.at[0])
        get_h = pltpu.make_async_copy(stash_h.at[pl.ds(row0, LEN), :], h_v, sems.at[1])
        get_x.start()
        get_h.start()
        @pl.when(meta[5] == 1)
        def _():
            pl.delay(STAGGER if tick == 0 else EVEN)


        @pl.when(stage == last_stage)
        def _():
            hit = lax.broadcasted_iota(jnp.int32, (LEN, D), 0) == length - 1
            row = jnp.where(lax.broadcasted_iota(jnp.int32, (8, D), 0) == slot, seed[...], 0.0)
            row = jnp.sum(row, axis=0, keepdims=True)
            g_v[...] = jnp.where(hit, jnp.broadcast_to(row, (LEN, D)), 0.0).astype(BF16)

        @pl.when(stage != last_stage)
        def _():
            g_v[...] = inbox[...]

        dctx_v[...] = dot_nn(g_v[...], wo[...])
        get_x.wait()
        q_rows = rows_of(x_v)
        k_blocks = paired(x_v[:, QW : QW + KV].astype(F32))
        v_blocks = paired(x_v[:, QW + KV :].astype(F32))
        probs = probabilities(q_rows, k_blocks, length)
        dctx = rows_of(dctx_v).astype(BF16)
        dvalue = unpaired(probs.astype(BF16), dctx)
        dprobs = by_pair(dot_nt, dctx, v_blocks).astype(BF16).astype(F32)
        low, high, left = half_sums(dprobs * probs)
        dscores = probs * (dprobs - jnp.where(left, low, high)) * HEAD_DIM ** (-0.5)
        dscores = dscores.astype(BF16)
        dquery = by_pair(dot_nn, dscores, k_blocks).astype(BF16).astype(F32)
        dkey = unpaired(dscores, q_rows).astype(BF16).astype(F32)
        cosine, sine = table[0], table[1]
        for i in range(PAIRS):
            part = dquery[LEN * i : LEN * i + LEN]
            dx_v[:, 128 * i : 128 * i + 128] = (part * cosine - partner(part) * sine).astype(BF16)
        dx_v[:, QW : QW + KV] = (dkey * cosine - partner(dkey) * sine).astype(BF16)
        dx_v[:, QW + KV :] = dvalue.astype(BF16)

        @pl.loop(0, HALVES)
        def _(i):
            cols = pl.ds(pl.multiple_of(i * HALF, HALF), HALF)
            dn_v[:, cols] = dot_nn(dx_v[...], wq[:, cols]).astype(BF16)

        get_h.wait()
        wide = h_v[...].astype(F32)
        scale = inv_rms(wide)
        scaled = dn_v[...].astype(F32) * gain[...]
        inner = jnp.sum(scaled * wide, axis=1, keepdims=True)
        out[...] = (
            g_v[...].astype(F32)
            + scale * scaled
            - wide * (scale * scale * scale * inner * (1.0 / D))
        ).astype(BF16)
        put = pltpu.make_async_copy(out, grads.at[pl.ds(row0, LEN), :], sems.at[2])
        put.start()
        put.wait()


ANY = pl.BlockSpec(memory_space=pl.ANY)
VMEM = pl.BlockSpec(memory_space=pltpu.VMEM)
SMEM = pl.BlockSpec(memory_space=pltpu.SMEM)
HBM = pl.BlockSpec(memory_space=pltpu.HBM)
LAYER_COST = pl.CostEstimate(
    flops=2 * LEN * D * (XW + QW), bytes_accessed=2 * D * (XW + QW), transcendentals=0
)
LIMIT = 8 * 1024 * 1024
LARGE = 14 * 1024 * 1024
WHOLE = 60 * 1024 * 1024
SMALL = 8 * 1024 * 1024


def forward_layer(
    tick, last_stage, micro, meta, inbox, entry, gain, table, wq, wo, before, state
):
    rows = micro * LEN
    kept = (((rows, D), BF16), ((rows, XW), BF16), ((micro, 8, D), F32))
    return pl.pallas_call(
        functools.partial(forward_kernel, tick, last_stage, micro),
        out_shape=tuple(jax.ShapeDtypeStruct(*a) for a in (((LEN, D), BF16), *kept)),
        in_specs=[SMEM, ANY, ANY, VMEM, VMEM, VMEM, VMEM, *[ANY] * len((*before, *state))],
        out_specs=(VMEM, ANY, ANY, ANY),
        input_output_aliases={7 + len(before) + i: 1 + i for i in range(len(state))},
        scratch_shapes=[
            pltpu.VMEM((LEN, D), BF16),
            pltpu.VMEM((LEN, D), BF16),
            pltpu.VMEM((LEN, XW), F32),
            pltpu.VMEM((LEN, XW), BF16),
            pltpu.VMEM((LEN, QW), BF16),
            pltpu.VMEM((8, D), F32),
            pltpu.SemaphoreType.DMA((4,)),
        ],
        compiler_params=pltpu.CompilerParams(vmem_limit_bytes=LIMIT),
        cost_estimate=LAYER_COST,
        name="forward_layer",
    )(meta, inbox, entry, gain, table, wq, wo, *before, *state)


def backward_layer(
    tick, last_stage, micro, meta, inbox, seed, gain, table, wq_t, wo_t, stash, grads
):
    return pl.pallas_call(
        functools.partial(backward_kernel, tick, last_stage, micro),
        out_shape=(
            jax.ShapeDtypeStruct((LEN, D), BF16),
            jax.ShapeDtypeStruct((micro * LEN, D), BF16),
        ),
        in_specs=[SMEM, VMEM, VMEM, VMEM, VMEM, VMEM, VMEM, ANY, ANY, *[ANY] * len(grads)],
        out_specs=(VMEM, ANY),
        input_output_aliases={9 + i: 1 + i for i in range(len(grads))},
        scratch_shapes=[
            pltpu.VMEM((LEN, D), BF16),
            pltpu.VMEM((LEN, D), BF16),
            pltpu.VMEM((LEN, XW), BF16),
            pltpu.VMEM((LEN, QW), F32),
            pltpu.VMEM((LEN, XW), BF16),
            pltpu.VMEM((LEN, D), BF16),
            pltpu.SemaphoreType.DMA((3,)),
        ],
        compiler_params=pltpu.CompilerParams(vmem_limit_bytes=LIMIT),
        cost_estimate=LAYER_COST,
        name="backward_layer",
    )(meta, inbox, seed, gain, table, wq_t, wo_t, *stash, *grads)


TURN = 256


def turn_kernel(early, meta, after, wq, wo, *refs):
    del after
    wq_t, wo_t, wq_v, wo_v, sems = refs[-5:]
    half = lax.div(meta[7], 2)
    due = meta[0] >= half if early else meta[0] < half

    @pl.when(due)
    def _():
        def copies(i, slot):
            at = pl.ds(pl.multiple_of(i * TURN, TURN), TURN)
            return (
                pltpu.make_async_copy(wq_v.at[slot], wq_t.at[:, at], sems.at[0, slot]),
                pltpu.make_async_copy(wo_v.at[slot], wo_t.at[at, :], sems.at[1, slot]),
            )

        @pl.loop(0, D // TURN)
        def _(i):
            slot = lax.rem(i, 2)
            at = pl.ds(pl.multiple_of(i * TURN, TURN), TURN)

            @pl.when(i >= 2)
            def _():
                for copy in copies(i - 2, slot):
                    copy.wait()

            wq_v[slot] = wq[at, :].T
            wo_v[slot] = wo[:, at].T
            for copy in copies(i, slot):
                copy.start()

        for i in (D // TURN - 2, D // TURN - 1):
            for copy in copies(i, i % 2):
                copy.wait()


def turn(early, meta, after, wq, wo, turned):
    return pl.pallas_call(
        functools.partial(turn_kernel, early),
        out_shape=(jax.ShapeDtypeStruct((XW, D), BF16), jax.ShapeDtypeStruct((D, QW), BF16)),
        in_specs=[SMEM, ANY, VMEM, VMEM, *[ANY] * len(turned)],
        out_specs=(ANY, ANY),
        input_output_aliases={4 + i: i for i in range(len(turned))},
        scratch_shapes=[
            pltpu.VMEM((2, XW, TURN), BF16),
            pltpu.VMEM((2, TURN, QW), BF16),
            pltpu.SemaphoreType.DMA((2, 2)),
        ],
        compiler_params=pltpu.CompilerParams(vmem_limit_bytes=LIMIT),
        cost_estimate=pl.CostEstimate(flops=0, bytes_accessed=4 * D * (XW + QW), transcendentals=0),
        name="turn",
    )(meta, after, wq, wo, *turned)


SIDE = PACK // 2


def pack_kernel(core, w_qkv, w_out, keep, give, w_v, x_v, sems):
    first = pltpu.make_async_copy(w_out, w_v, sems.at[0])
    second = pltpu.make_async_copy(w_qkv, x_v, sems.at[1])
    first.start()
    second.start()
    first.wait()
    pieces = [w_v[:, QW * j : QW * j + QW].astype(F32) for j in range(D // QW)]
    low = jnp.concatenate(pieces, axis=0).astype(BF16)
    second.wait()

    def fill(left, right):
        left[...] = x_v[:, :SIDE]
        right[:, : XW - SIDE] = x_v[:, SIDE:]
        right[:, XW - SIDE :] = low

    @pl.when(core[0] == 0)
    def _():
        fill(keep, give)

    @pl.when(core[0] == 1)
    def _():
        fill(give, keep)


def pack(core, w_qkv, w_out):
    side = jax.ShapeDtypeStruct((w_qkv.shape[0], SIDE), BF16)
    return pl.pallas_call(
        pack_kernel,
        out_shape=(side, side),
        in_specs=[SMEM, HBM, HBM],
        out_specs=(VMEM, VMEM),
        scratch_shapes=[
            pltpu.VMEM(w_out.shape, BF16),
            pltpu.VMEM(w_qkv.shape, BF16),
            pltpu.SemaphoreType.DMA((2,)),
        ],
        compiler_params=pltpu.CompilerParams(vmem_limit_bytes=WHOLE),
        name="pack",
    )(core, w_qkv, w_out)


def unpack_kernel(place, early, *refs):
    del early
    count = (len(refs) - 4) // 2
    mine, theirs = refs[:count], refs[count : 2 * count]
    wq, wo, part_v, sems = refs[2 * count :]
    parts = D // QW
    length = D // 32
    short = length // parts
    x0, y0, core = place[0], place[1], place[2]

    def offset(step):
        return jnp.where(step == 1, 3, jnp.where(step == 2, 1, jnp.where(step == 3, 2, 0)))

    def put(blocks, color):
        for n in range(8):
            block = blocks[n]
            far, other = n // 2, n % 2

            @pl.loop(0, 4)
            def _(near):
                first = lax.rem(offset(near) + (y0 if color == 0 else x0), 4)
                second = lax.rem((0, 3, 1, 2)[far] + (x0 if color == 0 else y0), 4)
                x, y = (second, first) if color == 0 else (first, second)
                shard = x * 8 + y * 2 + (color if other == 0 else 1 - color)
                rows = pl.ds(pl.multiple_of(shard * length, length), length)
                if color == 0:
                    pltpu.make_async_copy(
                        block.at[near], wq.at[rows, pl.ds(0, SIDE)], sems.at[0]
                    ).start()
                else:
                    pltpu.make_async_copy(
                        block.at[near, :, pl.ds(0, XW - SIDE)],
                        wq.at[rows, pl.ds(SIDE, XW - SIDE)],
                        sems.at[0],
                    ).start()
                    pltpu.make_async_copy(
                        block.at[near, :, pl.ds(XW - SIDE, QW)], part_v.at[rows, :], sems.at[1]
                    ).start()

    @pl.when(core == 0)
    def _():
        put(theirs, 1)
        put(mine, 0)

    @pl.when(core == 1)
    def _():
        put(mine, 1)
        put(theirs, 0)

    pltpu.make_async_copy(part_v, part_v, sems.at[1]).wait()

    @pl.loop(0, 8)
    def _(i):
        blocks = []
        for r in range(4):
            at = pl.ds(pl.multiple_of((4 * i + r) * length, length), length)
            blocks.append(part_v[at, :].astype(F32))
        to = pl.ds(pl.multiple_of(i * length, length), length)
        for j in range(parts):
            cut = [block[short * j : short * j + short] for block in blocks]
            wo[to, QW * j : QW * j + QW] = jnp.concatenate(cut, axis=0).astype(BF16)

    pltpu.make_async_copy(wq, wq, sems.at[0]).wait()


def unpack(place, early, mine, theirs):
    return pl.pallas_call(
        unpack_kernel,
        out_shape=(jax.ShapeDtypeStruct((D, XW), BF16), jax.ShapeDtypeStruct((QW, D), BF16)),
        in_specs=[SMEM, VMEM, *[ANY] * (len(mine) + len(theirs))],
        out_specs=(VMEM, VMEM),
        scratch_shapes=[pltpu.VMEM((D, QW), BF16), pltpu.SemaphoreType.DMA((2,))],
        compiler_params=pltpu.CompilerParams(vmem_limit_bytes=LARGE),
        name="unpack",
    )(place, early, *mine, *theirs)


def ring_step(value, second, step):
    pairs = []
    for x in range(4):
        for y in range(4):
            for core in range(2):
                along_y = (core == 0) != second
                to = (x, (y + step) % 4) if along_y else ((x + step) % 4, y)
                pairs.append((x * 8 + y * 2 + core, to[0] * 8 + to[1] * 2 + core))
    return lax.ppermute(value, DP, pairs)


def swap_cores(value):
    return lax.ppermute(value, "dp_2", [(0, 1), (1, 0)])


def gather_weights(w_qkv, w_out, early):
    place = jnp.stack([lax.axis_index(name) for name in DP])
    keep, give = pack(place[2:], w_qkv, w_out)
    lines = []
    for value, forward in ((keep, 1), (swap_cores(give), -1)):
        before = ring_step(value, False, 1)
        after = ring_step(value, False, -1)
        across = ring_step(before if forward == 1 else after, False, forward)
        lines.append(jnp.stack([value, before, after, across]))
    mine = [None] * 8
    for n, (line, forward) in enumerate(zip(lines, (1, -1))):
        before = ring_step(line, True, 1)
        after = ring_step(line, True, -1)
        across = ring_step(before if forward == 1 else after, True, forward)
        mine[n::2] = [line, before, after, across]
    return unpack(place, early, mine, [swap_cores(value) for value in mine])


WIDE = HALF + 128


def pooled_rows(last):
    return jnp.concatenate([last[j, 0:1, :] for j in (0, 2, 1, 3)], axis=0)


def embed_kernel(last, final_gain, labels, out):
    rows = pooled_rows(last)
    pooled = rows * inv_rms(rows) * final_gain[...]
    unit = pooled * lax.rsqrt(jnp.sum(pooled * pooled, axis=1, keepdims=True))
    halves = jnp.concatenate([unit[:, :HALF], unit[:, HALF:]], axis=0).astype(BF16)
    which = lax.broadcasted_iota(jnp.int32, (8, 128), 0)
    label = jnp.where(which == 0, labels[0], jnp.where(which == 1, labels[1], 0))
    label = label.astype(F32).astype(BF16)
    for i in range(out.shape[0]):
        out[i, :, :HALF] = halves
        out[i, :, HALF:] = label


def embed(count, last, final_gain, labels):
    return pl.pallas_call(
        embed_kernel,
        out_shape=jax.ShapeDtypeStruct((count, 8, WIDE), BF16),
        in_specs=[VMEM, VMEM, SMEM],
        out_specs=VMEM,
        compiler_params=pltpu.CompilerParams(vmem_limit_bytes=LIMIT),
        name="embed",
    )(last, final_gain, labels)


def loss_kernel(meta, last, final_gain, here, there, seed):
    everyone = jnp.concatenate([here[...], there[...]], axis=0)
    count = everyone.shape[0]
    emb = everyone[:, :HALF]
    label = everyone[:, HALF:].astype(F32)[:, 0:1].astype(jnp.int32)
    scores = dot_nt(emb, emb)
    scores = scores + pltpu.roll(pltpu.roll(scores, count - 4, 0), count - 4, 1)
    row = lax.rem(lax.broadcasted_iota(jnp.int32, (count, count), 0), 8)
    col = lax.broadcasted_iota(jnp.int32, (count, count), 1)
    doc = jnp.logical_and(lax.rem(col, 8) >= 2, lax.rem(col, 8) < 4)
    valid = jnp.logical_and(row < 2, doc)
    weights = jnp.where(valid, jnp.exp(scores * SHARP), 0.0)
    total = jnp.sum(weights, axis=1, keepdims=True)
    prob = weights / jnp.where(row[:, :1] < 2, total, 1.0)
    owner = lax.div(label, 2)
    away = (lax.rem(owner, 2) != meta[5]).astype(jnp.int32)
    target = away * (count // 2) + lax.div(owner, 2) * 8 + 2 + lax.rem(label, 2)
    coef = jnp.where(valid, (prob - (col == target).astype(F32)) * (COEF * SHARP), 0.0)
    both = coef + coef.T
    mine = lax.broadcasted_iota(jnp.int32, (8, count), 0)
    pick = lax.broadcasted_iota(jnp.int32, (8, count), 1) == lax.div(meta[6], 2) * 8 + mine
    own = lax.dot_general(
        pick.astype(F32),
        both,
        (((1,), (0,)), ((), ())),
        precision=lax.Precision.HIGHEST,
        preferred_element_type=F32,
    )[:4]
    own = jnp.concatenate([own, pltpu.roll(own, 4, 1)], axis=0)
    top = own.astype(BF16)
    rest = own - top.astype(F32)
    mid = rest.astype(BF16)
    low = (rest - mid.astype(F32)).astype(BF16)
    grad = dot_nn(top, emb) + (dot_nn(mid, emb) + dot_nn(low, emb))
    grad = jnp.concatenate([grad[:4], grad[4:]], axis=1)
    rows = pooled_rows(last)
    gain = final_gain[...]
    scale = inv_rms(rows)
    pooled = rows * scale * gain
    norm = lax.rsqrt(jnp.sum(pooled * pooled, axis=1, keepdims=True))
    unit = pooled * norm
    dpooled = norm * (grad - unit * jnp.sum(grad * unit, axis=1, keepdims=True))
    scaled = dpooled * gain
    inner = jnp.sum(scaled * rows, axis=1, keepdims=True)
    drow = scale * scaled - rows * (scale * scale * scale * inner * (1.0 / D))
    drow = drow.astype(BF16).astype(F32)
    seed[...] = jnp.concatenate(
        [drow[0:1], drow[2:3], drow[1:2], drow[3:4], jnp.zeros((4, D), F32)], axis=0
    )


def loss_seed(meta, last, final_gain, here, there):
    return pl.pallas_call(
        loss_kernel,
        out_shape=jax.ShapeDtypeStruct((8, D), F32),
        in_specs=[SMEM, VMEM, VMEM, VMEM, VMEM],
        out_specs=VMEM,
        compiler_params=pltpu.CompilerParams(vmem_limit_bytes=LIMIT),
        name="loss_seed",
    )(meta, last, final_gain, here, there)


def rotary_table():
    lane = jnp.arange(128, dtype=jnp.int32)
    frequency = ROPE_BASE ** (-(lane % 32).astype(F32) * (2.0 / HEAD_DIM))
    angles = jnp.arange(LEN, dtype=F32)[:, None] * frequency[None, :]
    sign = jnp.where(lane % 64 < 32, -1.0, 1.0)
    return jnp.stack([jnp.cos(angles), jnp.sin(angles) * sign])


def per_device(entry, norm_gain, w_qkv, w_out, final_gain, lengths, positive):
    stage = lax.axis_index("section")
    stages = lax.axis_size("section")
    replica = lax.axis_index(DP)
    core = lax.axis_index("dp_2")
    micro = lengths.shape[0]
    gain = norm_gain
    final_row = final_gain[None, :]
    wq, wo = gather_weights(w_qkv[0], w_out[0], final_row)
    numbers = jnp.array([stages], jnp.int32)
    meta = jnp.concatenate([stage[None], lengths, core[None], replica[None], numbers])
    table = rotary_table()
    ticks = micro + stages - 1
    half = stages // 2
    state, turned = (), ()
    inbox = entry[:LEN]
    for tick in range(ticks):
        before = turned if tick in (1, half + micro) else ()
        out, *state = forward_layer(
            tick, stages - 1, micro, meta, inbox, entry, gain, table, wq, wo, before, state
        )
        if tick == 0:
            turned = turn(True, meta, out, wq, wo, turned)
        if tick == half + micro - 1:
            turned = turn(False, meta, out, wq, wo, turned)
        if tick < ticks - 1:
            pairs = [(s, s + 1) for s in range(stages - 1) if 0 <= tick - s < micro]
            inbox = lax.ppermute(out, "section", pairs)
    *stash, last = state
    count = lax.axis_size(DP[:2])
    copies = embed(count, last, final_row, positive)
    here = lax.all_to_all(copies, DP[:2], split_axis=0, concat_axis=0, tiled=True)
    here = here.reshape(count * 8, WIDE)
    there = lax.ppermute(here, "dp_2", [(0, 1), (1, 0)])
    seed = loss_seed(meta, last, final_row, here, there)
    grads = ()
    for tick in range(ticks):
        out, *grads = backward_layer(
            tick, stages - 1, micro, meta, inbox, seed, gain, table, *turned, stash, grads
        )
        if tick < ticks - 1:
            pairs = [
                (stages - 1 - s, stages - 2 - s)
                for s in range(stages - 1)
                if 0 <= tick - s < micro
            ]
            inbox = lax.ppermute(out, "section", pairs)
    return grads[0][None]


def solution(mesh):
    finer = Mesh(
        mesh.devices.reshape(mesh.shape["section"], 4, 4, 2), ("section", "dp_0", "dp_1", "dp_2")
    )
    in_specs = (
        P(DP, None),
        P("section", None),
        P("section", DP, None),
        P("section", DP, None),
        P(),
        P(DP),
        P(DP),
    )
    return jax.shard_map(
        per_device,
        mesh=finer,
        in_specs=in_specs,
        out_specs=P("section", DP, None),
        check_vma=False,
    )
```

```python
import functools

import jax
import jax.numpy as jnp
from jax import lax
from jax.experimental import pallas as pl
from jax.experimental.pallas import tpu as pltpu
from jax.sharding import Mesh
from jax.sharding import PartitionSpec as P

HEAD_DIM = 64
LEN = 48
D = 3584
QW = 896
KV = 128
XW = QW + 2 * KV
PACK = XW + QW
PAIRS = QW // 128
DP = ("dp_0", "dp_1", "dp_2")
ROPE_BASE = 1000000.0
EPS = 1e-06
SHARP = 20.0
COEF = 256.0
HALVES = 2
HALF = D // HALVES
STAGGER = 5000
EVEN = 850
F32 = jnp.float32
BF16 = jnp.bfloat16


def dot_nn(a, b):
    return lax.dot_general(a, b, (((1,), (0,)), ((), ())), preferred_element_type=F32)


def dot_nt(a, b):
    return lax.dot_general(a, b, (((1,), (1,)), ((), ())), preferred_element_type=F32)


def dot_tn(a, b):
    return lax.dot_general(a, b, (((0,), (0,)), ((), ())), preferred_element_type=F32)


def lanes(rows):
    return lax.broadcasted_iota(jnp.int32, (rows, 128), 1)


def partner(x):
    low = lax.rem(lanes(x.shape[0]), 64) < 32
    return jnp.where(low, pltpu.roll(x, 96, 1), pltpu.roll(x, 32, 1))


def paired(z):
    left = lanes(LEN) < 64
    rolled = pltpu.roll(z, 64, 1)
    pad = jnp.zeros((16, 128), BF16)
    a_left = jnp.where(left, z, 0.0).astype(BF16)
    b_right = jnp.where(left, 0.0, z).astype(BF16)
    b_left = jnp.where(left, rolled, 0.0).astype(BF16)
    a_right = jnp.where(left, 0.0, rolled).astype(BF16)
    return (
        jnp.concatenate([a_left, pad, a_right, pad], axis=0),
        jnp.concatenate([a_left, pad, b_right, pad], axis=0),
        jnp.concatenate([b_left, pad, b_right, pad], axis=0),
    )


SPANS = ((0, 3 * LEN), (3 * LEN, 4 * LEN), (4 * LEN, 7 * LEN))


def by_pair(dot, rows, blocks):
    return jnp.concatenate(
        [dot(rows[lo:hi], block) for (lo, hi), block in zip(SPANS, blocks)], axis=0
    )


def unpaired(rows, other):
    left = lanes(LEN) < 64
    s00, s01, s11 = (dot_tn(rows[lo:hi], other[lo:hi]) for lo, hi in SPANS)
    first = jnp.where(left, s00[:LEN] + s01[:LEN], 0.0)
    first += pltpu.roll(jnp.where(left, 0.0, s00[64 : 64 + LEN]), 64, 1)
    second = jnp.where(left, 0.0, s01[64 : 64 + LEN] + s11[64 : 64 + LEN])
    second += pltpu.roll(jnp.where(left, s11[:LEN], 0.0), 64, 1)
    return first + second


def half_sums(x):
    left = lanes(x.shape[0]) < 64
    low = jnp.sum(jnp.where(left, x, 0.0), axis=1, keepdims=True)
    high = jnp.sum(jnp.where(left, 0.0, x), axis=1, keepdims=True)
    return low, high, left


def probabilities(q_rows, k_blocks, length):
    scores = by_pair(dot_nt, q_rows, k_blocks) * HEAD_DIM ** (-0.5)
    live = lax.rem(lanes(scores.shape[0]), 64) < length
    weights = jnp.where(live, jnp.exp(scores), 0.0)
    low, high, left = half_sums(weights)
    return weights * jnp.where(left, 1.0 / low, 1.0 / high)


def rows_of(x_ref):
    return jnp.concatenate([x_ref[:, 128 * i : 128 * i + 128] for i in range(PAIRS)], axis=0)


def inv_rms(wide):
    return lax.rsqrt(jnp.sum(wide * wide, axis=1, keepdims=True) * (1.0 / D) + EPS)


def forward_kernel(
    tick,
    last_stage,
    micro,
    meta,
    inbox,
    entry,
    gain,
    table,
    wq,
    wo,
    *refs,
):
    out, stash_h, stash_x, last, h_v, n_v, acc_v, x_v, ctx_v, last_v, sems = refs[-11:]
    stage = meta[0]
    slot = tick - stage

    @pl.when(jnp.logical_and(slot >= 0, slot < micro))
    def _():
        length = meta[1 + slot]
        row0 = pl.multiple_of(slot * LEN, LEN)

        first = pltpu.make_async_copy(entry.at[pl.ds(row0, LEN), :], h_v, sems.at[0])
        later = pltpu.make_async_copy(inbox.at[pl.ds(0, LEN), :], h_v, sems.at[0])

        @pl.when(stage == 0)
        def _():
            first.start()

        @pl.when(stage != 0)
        def _():
            later.start()

        @pl.when(meta[5] == 1)
        def _():
            pl.delay(STAGGER if tick == 0 else EVEN)

        later.wait()
        keep_h = pltpu.make_async_copy(h_v, stash_h.at[pl.ds(row0, LEN), :], sems.at[1])
        keep_h.start()
        wide = h_v[...].astype(F32)
        n_v[...] = (wide * inv_rms(wide) * gain[...]).astype(BF16)
        acc_v[...] = jnp.zeros_like(acc_v)

        @pl.loop(0, HALVES)
        def _(i):
            cols = pl.ds(pl.multiple_of(i * HALF, HALF), HALF)
            acc_v[...] += dot_nn(n_v[:, cols], wq[cols, :])

        cosine, sine = table[0], table[1]
        for i in range(PAIRS + 1):
            part = acc_v[:, 128 * i : 128 * i + 128]
            x_v[:, 128 * i : 128 * i + 128] = (part * cosine + partner(part) * sine).astype(BF16)
        x_v[:, QW + KV :] = acc_v[:, QW + KV :].astype(BF16)
        keep_x = pltpu.make_async_copy(x_v, stash_x.at[pl.ds(row0, LEN), :], sems.at[2])
        keep_x.start()
        k_blocks = paired(x_v[:, QW : QW + KV].astype(F32))
        v_blocks = paired(x_v[:, QW + KV :].astype(F32))
        probs = probabilities(rows_of(x_v), k_blocks, length).astype(BF16)
        context = by_pair(dot_nn, probs, v_blocks).astype(BF16)
        for i in range(PAIRS):
            ctx_v[:, 128 * i : 128 * i + 128] = context[LEN * i : LEN * i + LEN]

        @pl.loop(0, HALVES)
        def _(i):
            cols = pl.ds(pl.multiple_of(i * HALF, HALF), HALF)
            branch = dot_nn(ctx_v[...], wo[:, cols])
            out[:, cols] = (h_v[:, cols].astype(F32) + branch).astype(BF16)

        @pl.when(stage == last_stage)
        def _():
            hit = lax.broadcasted_iota(jnp.int32, (LEN, D), 0) == length - 1
            row = jnp.sum(jnp.where(hit, out[...].astype(F32), 0.0), axis=0, keepdims=True)
            last_v[...] = jnp.broadcast_to(row, (8, D))
            put = pltpu.make_async_copy(last_v, last.at[slot], sems.at[3])
            put.start()
            put.wait()

        keep_h.wait()
        keep_x.wait()


def backward_kernel(
    tick,
    last_stage,
    micro,
    meta,
    inbox,
    seed,
    gain,
    table,
    wq,
    wo,
    stash_h,
    stash_x,
    *refs,
):
    out, grads, h_v, g_v, x_v, dctx_v, dx_v, dn_v, sems = refs[-9:]
    stage = meta[0]
    slot = tick - (last_stage - stage)

    @pl.when(jnp.logical_and(slot >= 0, slot < micro))
    def _():
        length = meta[1 + slot]
        row0 = pl.multiple_of(slot * LEN, LEN)

        get_x = pltpu.make_async_copy(stash_x.at[pl.ds(row0, LEN), :], x_v, sems.at[0])
        get_h = pltpu.make_async_copy(stash_h.at[pl.ds(row0, LEN), :], h_v, sems.at[1])
        get_x.start()
        get_h.start()
        @pl.when(meta[5] == 1)
        def _():
            pl.delay(STAGGER if tick == 0 else EVEN)


        @pl.when(stage == last_stage)
        def _():
            hit = lax.broadcasted_iota(jnp.int32, (LEN, D), 0) == length - 1
            row = jnp.where(lax.broadcasted_iota(jnp.int32, (8, D), 0) == slot, seed[...], 0.0)
            row = jnp.sum(row, axis=0, keepdims=True)
            g_v[...] = jnp.where(hit, jnp.broadcast_to(row, (LEN, D)), 0.0).astype(BF16)

        @pl.when(stage != last_stage)
        def _():
            g_v[...] = inbox[...]

        dctx_v[...] = jnp.zeros_like(dctx_v)

        @pl.loop(0, HALVES)
        def _(i):
            cols = pl.ds(pl.multiple_of(i * HALF, HALF), HALF)
            dctx_v[...] += dot_nn(g_v[:, cols], wo[cols, :])

        get_x.wait()
        q_rows = rows_of(x_v)
        k_blocks = paired(x_v[:, QW : QW + KV].astype(F32))
        v_blocks = paired(x_v[:, QW + KV :].astype(F32))
        probs = probabilities(q_rows, k_blocks, length)
        dctx = rows_of(dctx_v).astype(BF16)
        dvalue = unpaired(probs.astype(BF16), dctx)
        dprobs = by_pair(dot_nt, dctx, v_blocks).astype(BF16).astype(F32)
        low, high, left = half_sums(dprobs * probs)
        dscores = probs * (dprobs - jnp.where(left, low, high)) * HEAD_DIM ** (-0.5)
        dscores = dscores.astype(BF16)
        dquery = by_pair(dot_nn, dscores, k_blocks).astype(BF16).astype(F32)
        dkey = unpaired(dscores, q_rows).astype(BF16).astype(F32)
        cosine, sine = table[0], table[1]
        for i in range(PAIRS):
            part = dquery[LEN * i : LEN * i + LEN]
            dx_v[:, 128 * i : 128 * i + 128] = (part * cosine - partner(part) * sine).astype(BF16)
        dx_v[:, QW : QW + KV] = (dkey * cosine - partner(dkey) * sine).astype(BF16)
        dx_v[:, QW + KV :] = dvalue.astype(BF16)

        @pl.loop(0, HALVES)
        def _(i):
            cols = pl.ds(pl.multiple_of(i * HALF, HALF), HALF)
            dn_v[:, cols] = dot_nn(dx_v[...], wq[:, cols]).astype(BF16)

        get_h.wait()
        wide = h_v[...].astype(F32)
        scale = inv_rms(wide)
        scaled = dn_v[...].astype(F32) * gain[...]
        inner = jnp.sum(scaled * wide, axis=1, keepdims=True)
        out[...] = (
            g_v[...].astype(F32)
            + scale * scaled
            - wide * (scale * scale * scale * inner * (1.0 / D))
        ).astype(BF16)
        put = pltpu.make_async_copy(out, grads.at[pl.ds(row0, LEN), :], sems.at[2])
        put.start()
        put.wait()


ANY = pl.BlockSpec(memory_space=pl.ANY)
VMEM = pl.BlockSpec(memory_space=pltpu.VMEM)
SMEM = pl.BlockSpec(memory_space=pltpu.SMEM)
HBM = pl.BlockSpec(memory_space=pltpu.HBM)
LAYER_COST = pl.CostEstimate(
    flops=2 * LEN * D * (XW + QW), bytes_accessed=2 * D * (XW + QW), transcendentals=0
)
LIMIT = 8 * 1024 * 1024
LARGE = 14 * 1024 * 1024
WHOLE = 60 * 1024 * 1024
SMALL = 8 * 1024 * 1024


def forward_layer(
    tick, last_stage, micro, meta, inbox, entry, gain, table, wq, wo, before, state
):
    rows = micro * LEN
    kept = (((rows, D), BF16), ((rows, XW), BF16), ((micro, 8, D), F32))
    return pl.pallas_call(
        functools.partial(forward_kernel, tick, last_stage, micro),
        out_shape=tuple(jax.ShapeDtypeStruct(*a) for a in (((LEN, D), BF16), *kept)),
        in_specs=[SMEM, ANY, ANY, VMEM, VMEM, VMEM, VMEM, *[ANY] * len((*before, *state))],
        out_specs=(VMEM, ANY, ANY, ANY),
        input_output_aliases={7 + len(before) + i: 1 + i for i in range(len(state))},
        scratch_shapes=[
            pltpu.VMEM((LEN, D), BF16),
            pltpu.VMEM((LEN, D), BF16),
            pltpu.VMEM((LEN, XW), F32),
            pltpu.VMEM((LEN, XW), BF16),
            pltpu.VMEM((LEN, QW), BF16),
            pltpu.VMEM((8, D), F32),
            pltpu.SemaphoreType.DMA((4,)),
        ],
        compiler_params=pltpu.CompilerParams(vmem_limit_bytes=LIMIT),
        cost_estimate=LAYER_COST,
        name="forward_layer",
    )(meta, inbox, entry, gain, table, wq, wo, *before, *state)


def backward_layer(
    tick, last_stage, micro, meta, inbox, seed, gain, table, wq_t, wo_t, stash, grads
):
    return pl.pallas_call(
        functools.partial(backward_kernel, tick, last_stage, micro),
        out_shape=(
            jax.ShapeDtypeStruct((LEN, D), BF16),
            jax.ShapeDtypeStruct((micro * LEN, D), BF16),
        ),
        in_specs=[SMEM, VMEM, VMEM, VMEM, VMEM, VMEM, VMEM, ANY, ANY, *[ANY] * len(grads)],
        out_specs=(VMEM, ANY),
        input_output_aliases={9 + i: 1 + i for i in range(len(grads))},
        scratch_shapes=[
            pltpu.VMEM((LEN, D), BF16),
            pltpu.VMEM((LEN, D), BF16),
            pltpu.VMEM((LEN, XW), BF16),
            pltpu.VMEM((LEN, QW), F32),
            pltpu.VMEM((LEN, XW), BF16),
            pltpu.VMEM((LEN, D), BF16),
            pltpu.SemaphoreType.DMA((3,)),
        ],
        compiler_params=pltpu.CompilerParams(vmem_limit_bytes=LIMIT),
        cost_estimate=LAYER_COST,
        name="backward_layer",
    )(meta, inbox, seed, gain, table, wq_t, wo_t, *stash, *grads)


TURN = 256


def turn_kernel(early, meta, after, wq, wo, *refs):
    del after
    wq_t, wo_t, wq_v, wo_v, sems = refs[-5:]
    half = lax.div(meta[7], 2)
    due = meta[0] >= half if early else meta[0] < half

    @pl.when(due)
    def _():
        def copies(i, slot):
            at = pl.ds(pl.multiple_of(i * TURN, TURN), TURN)
            return (
                pltpu.make_async_copy(wq_v.at[slot], wq_t.at[:, at], sems.at[0, slot]),
                pltpu.make_async_copy(wo_v.at[slot], wo_t.at[at, :], sems.at[1, slot]),
            )

        @pl.loop(0, D // TURN)
        def _(i):
            slot = lax.rem(i, 2)
            at = pl.ds(pl.multiple_of(i * TURN, TURN), TURN)

            @pl.when(i >= 2)
            def _():
                for copy in copies(i - 2, slot):
                    copy.wait()

            wq_v[slot] = wq[at, :].T
            wo_v[slot] = wo[:, at].T
            for copy in copies(i, slot):
                copy.start()

        for i in (D // TURN - 2, D // TURN - 1):
            for copy in copies(i, i % 2):
                copy.wait()


def turn(early, meta, after, wq, wo, turned):
    return pl.pallas_call(
        functools.partial(turn_kernel, early),
        out_shape=(jax.ShapeDtypeStruct((XW, D), BF16), jax.ShapeDtypeStruct((D, QW), BF16)),
        in_specs=[SMEM, ANY, VMEM, VMEM, *[ANY] * len(turned)],
        out_specs=(ANY, ANY),
        input_output_aliases={4 + i: i for i in range(len(turned))},
        scratch_shapes=[
            pltpu.VMEM((2, XW, TURN), BF16),
            pltpu.VMEM((2, TURN, QW), BF16),
            pltpu.SemaphoreType.DMA((2, 2)),
        ],
        compiler_params=pltpu.CompilerParams(vmem_limit_bytes=LIMIT),
        cost_estimate=pl.CostEstimate(flops=0, bytes_accessed=4 * D * (XW + QW), transcendentals=0),
        name="turn",
    )(meta, after, wq, wo, *turned)


SIDE = PACK // 2


def pack_kernel(meta, w_qkv, w_out, keep, give, w_v, x_v, sems):
    first = pltpu.make_async_copy(w_out, w_v, sems.at[0])
    second = pltpu.make_async_copy(w_qkv, x_v, sems.at[1])
    first.start()
    second.start()
    first.wait()
    pieces = [w_v[:, QW * j : QW * j + QW].astype(F32) for j in range(D // QW)]
    low = jnp.concatenate(pieces, axis=0).astype(BF16)
    second.wait()

    def fill(left, right):
        left[...] = x_v[:, :SIDE]
        right[:, : XW - SIDE] = x_v[:, SIDE:]
        right[:, XW - SIDE :] = low

    @pl.when(meta[5] == 0)
    def _():
        fill(keep, give)

    @pl.when(meta[5] == 1)
    def _():
        fill(give, keep)


def pack(meta, w_qkv, w_out):
    side = jax.ShapeDtypeStruct((w_qkv.shape[0], SIDE), BF16)
    return pl.pallas_call(
        pack_kernel,
        out_shape=(side, side),
        in_specs=[SMEM, HBM, HBM],
        out_specs=(VMEM, VMEM),
        scratch_shapes=[
            pltpu.VMEM(w_out.shape, BF16),
            pltpu.VMEM(w_qkv.shape, BF16),
            pltpu.SemaphoreType.DMA((2,)),
        ],
        compiler_params=pltpu.CompilerParams(vmem_limit_bytes=WHOLE),
        name="pack",
    )(meta, w_qkv, w_out)


def unpack_kernel(meta, *refs):
    count = (len(refs) - 4) // 2
    mine, theirs = refs[:count], refs[count : 2 * count]
    wq, wo, part_v, sems = refs[2 * count :]
    parts = D // QW
    length = D // 32
    short = length // parts
    x0, y0, core = meta[8], meta[9], meta[5]

    def offset(step):
        return jnp.where(step == 1, 3, jnp.where(step == 2, 1, jnp.where(step == 3, 2, 0)))

    def put(blocks, color):
        for n in range(8):
            block = blocks[n]
            far, other = n // 2, n % 2

            @pl.loop(0, 4)
            def _(near):
                first = lax.rem(offset(near) + (y0 if color == 0 else x0), 4)
                second = lax.rem((0, 3, 1, 2)[far] + (x0 if color == 0 else y0), 4)
                x, y = (second, first) if color == 0 else (first, second)
                shard = x * 8 + y * 2 + (color if other == 0 else 1 - color)
                rows = pl.ds(pl.multiple_of(shard * length, length), length)
                if color == 0:
                    pltpu.make_async_copy(
                        block.at[near], wq.at[rows, pl.ds(0, SIDE)], sems.at[0]
                    ).start()
                else:
                    pltpu.make_async_copy(
                        block.at[near, :, pl.ds(0, XW - SIDE)],
                        wq.at[rows, pl.ds(SIDE, XW - SIDE)],
                        sems.at[0],
                    ).start()
                    pltpu.make_async_copy(
                        block.at[near, :, pl.ds(XW - SIDE, QW)], part_v.at[rows, :], sems.at[1]
                    ).start()

    @pl.when(core == 0)
    def _():
        put(theirs, 1)
        put(mine, 0)

    @pl.when(core == 1)
    def _():
        put(mine, 1)
        put(theirs, 0)

    pltpu.make_async_copy(part_v, part_v, sems.at[1]).wait()

    @pl.loop(0, 8)
    def _(i):
        blocks = []
        for r in range(4):
            at = pl.ds(pl.multiple_of((4 * i + r) * length, length), length)
            blocks.append(part_v[at, :].astype(F32))
        to = pl.ds(pl.multiple_of(i * length, length), length)
        for j in range(parts):
            cut = [block[short * j : short * j + short] for block in blocks]
            wo[to, QW * j : QW * j + QW] = jnp.concatenate(cut, axis=0).astype(BF16)

    pltpu.make_async_copy(wq, wq, sems.at[0]).wait()


def unpack(meta, mine, theirs):
    return pl.pallas_call(
        unpack_kernel,
        out_shape=(jax.ShapeDtypeStruct((D, XW), BF16), jax.ShapeDtypeStruct((QW, D), BF16)),
        in_specs=[SMEM, *[ANY] * (len(mine) + len(theirs))],
        out_specs=(VMEM, VMEM),
        scratch_shapes=[pltpu.VMEM((D, QW), BF16), pltpu.SemaphoreType.DMA((2,))],
        compiler_params=pltpu.CompilerParams(vmem_limit_bytes=LARGE),
        name="unpack",
    )(meta, *mine, *theirs)


def ring_step(value, second, step):
    pairs = []
    for x in range(4):
        for y in range(4):
            for core in range(2):
                along_y = (core == 0) != second
                to = (x, (y + step) % 4) if along_y else ((x + step) % 4, y)
                pairs.append((x * 8 + y * 2 + core, to[0] * 8 + to[1] * 2 + core))
    return lax.ppermute(value, DP, pairs)


def swap_cores(value):
    return lax.ppermute(value, "dp_2", [(0, 1), (1, 0)])


def join_kernel(*refs):
    *parts, out, sems = refs
    copies = [
        pltpu.make_async_copy(part, out.at[n], sems.at[n]) for n, part in enumerate(parts)
    ]
    for copy in copies:
        copy.start()
    for copy in copies:
        copy.wait()


def join(*parts):
    return pl.pallas_call(
        join_kernel,
        out_shape=jax.ShapeDtypeStruct((len(parts), *parts[0].shape), parts[0].dtype),
        in_specs=[ANY] * len(parts),
        out_specs=ANY,
        scratch_shapes=[pltpu.SemaphoreType.DMA((len(parts),))],
        compiler_params=pltpu.CompilerParams(vmem_limit_bytes=1024 * 1024),
        name="join",
    )(*parts)


def gather_weights(meta, w_qkv, w_out, others):
    keep, give = pack(meta, w_qkv, w_out)
    keep, got, others = lax.optimization_barrier((keep, swap_cores(give), others))
    lines = []
    for value, forward in ((keep, 1), (got, -1)):
        before = ring_step(value, False, 1)
        after = ring_step(value, False, -1)
        across = ring_step(before if forward == 1 else after, False, forward)
        lines.append(join(value, before, after, across))
    mine = [None] * 8
    for n, (line, forward) in enumerate(zip(lines, (1, -1))):
        before = ring_step(line, True, 1)
        after = ring_step(line, True, -1)
        across = ring_step(before if forward == 1 else after, True, forward)
        mine[n::2] = [line, before, after, across]
    return unpack(meta, mine, [swap_cores(value) for value in mine]), others


WIDE = HALF + 128


def pooled_rows(last):
    return jnp.concatenate([last[j, 0:1, :] for j in (0, 2, 1, 3)], axis=0)


def embed_kernel(last, final_gain, labels, out):
    rows = pooled_rows(last)
    pooled = rows * inv_rms(rows) * final_gain[...]
    unit = pooled * lax.rsqrt(jnp.sum(pooled * pooled, axis=1, keepdims=True))
    halves = jnp.concatenate([unit[:, :HALF], unit[:, HALF:]], axis=0).astype(BF16)
    which = lax.broadcasted_iota(jnp.int32, (8, 128), 0)
    label = jnp.where(which == 0, labels[0], jnp.where(which == 1, labels[1], 0))
    label = label.astype(F32).astype(BF16)
    for i in range(out.shape[0]):
        out[i, :, :HALF] = halves
        out[i, :, HALF:] = label


def embed(count, last, final_gain, labels):
    return pl.pallas_call(
        embed_kernel,
        out_shape=jax.ShapeDtypeStruct((count, 8, WIDE), BF16),
        in_specs=[VMEM, VMEM, SMEM],
        out_specs=VMEM,
        compiler_params=pltpu.CompilerParams(vmem_limit_bytes=LIMIT),
        name="embed",
    )(last, final_gain, labels)


def loss_kernel(meta, last, final_gain, here, there, seed):
    everyone = jnp.concatenate([here[...], there[...]], axis=0)
    count = everyone.shape[0]
    emb = everyone[:, :HALF]
    label = everyone[:, HALF:].astype(F32)[:, 0:1].astype(jnp.int32)
    scores = dot_nt(emb, emb)
    scores = scores + pltpu.roll(pltpu.roll(scores, count - 4, 0), count - 4, 1)
    row = lax.rem(lax.broadcasted_iota(jnp.int32, (count, count), 0), 8)
    col = lax.broadcasted_iota(jnp.int32, (count, count), 1)
    doc = jnp.logical_and(lax.rem(col, 8) >= 2, lax.rem(col, 8) < 4)
    valid = jnp.logical_and(row < 2, doc)
    weights = jnp.where(valid, jnp.exp(scores * SHARP), 0.0)
    total = jnp.sum(weights, axis=1, keepdims=True)
    prob = weights / jnp.where(row[:, :1] < 2, total, 1.0)
    owner = lax.div(label, 2)
    away = (lax.rem(owner, 2) != meta[5]).astype(jnp.int32)
    target = away * (count // 2) + lax.div(owner, 2) * 8 + 2 + lax.rem(label, 2)
    coef = jnp.where(valid, (prob - (col == target).astype(F32)) * (COEF * SHARP), 0.0)
    both = coef + coef.T
    mine = lax.broadcasted_iota(jnp.int32, (8, count), 0)
    pick = lax.broadcasted_iota(jnp.int32, (8, count), 1) == lax.div(meta[6], 2) * 8 + mine
    own = lax.dot_general(
        pick.astype(F32),
        both,
        (((1,), (0,)), ((), ())),
        precision=lax.Precision.HIGHEST,
        preferred_element_type=F32,
    )[:4]
    own = jnp.concatenate([own, pltpu.roll(own, 4, 1)], axis=0)
    top = own.astype(BF16)
    rest = own - top.astype(F32)
    mid = rest.astype(BF16)
    low = (rest - mid.astype(F32)).astype(BF16)
    grad = dot_nn(top, emb) + (dot_nn(mid, emb) + dot_nn(low, emb))
    grad = jnp.concatenate([grad[:4], grad[4:]], axis=1)
    rows = pooled_rows(last)
    gain = final_gain[...]
    scale = inv_rms(rows)
    pooled = rows * scale * gain
    norm = lax.rsqrt(jnp.sum(pooled * pooled, axis=1, keepdims=True))
    unit = pooled * norm
    dpooled = norm * (grad - unit * jnp.sum(grad * unit, axis=1, keepdims=True))
    scaled = dpooled * gain
    inner = jnp.sum(scaled * rows, axis=1, keepdims=True)
    drow = scale * scaled - rows * (scale * scale * scale * inner * (1.0 / D))
    drow = drow.astype(BF16).astype(F32)
    seed[...] = jnp.concatenate(
        [drow[0:1], drow[2:3], drow[1:2], drow[3:4], jnp.zeros((4, D), F32)], axis=0
    )


def loss_seed(meta, last, final_gain, here, there):
    return pl.pallas_call(
        loss_kernel,
        out_shape=jax.ShapeDtypeStruct((8, D), F32),
        in_specs=[SMEM, VMEM, VMEM, VMEM, VMEM],
        out_specs=VMEM,
        compiler_params=pltpu.CompilerParams(vmem_limit_bytes=LIMIT),
        name="loss_seed",
    )(meta, last, final_gain, here, there)


def rotary_table():
    lane = jnp.arange(128, dtype=jnp.int32)
    frequency = ROPE_BASE ** (-(lane % 32).astype(F32) * (2.0 / HEAD_DIM))
    angles = jnp.arange(LEN, dtype=F32)[:, None] * frequency[None, :]
    sign = jnp.where(lane % 64 < 32, -1.0, 1.0)
    return jnp.stack([jnp.cos(angles), jnp.sin(angles) * sign])


def per_device(entry, norm_gain, w_qkv, w_out, final_gain, lengths, positive):
    stage = lax.axis_index("section")
    stages = lax.axis_size("section")
    replica = lax.axis_index(DP)
    places = [lax.axis_index(name)[None] for name in DP]
    micro = lengths.shape[0]
    gain = norm_gain
    numbers = jnp.array([stages], jnp.int32)
    meta = jnp.concatenate(
        [stage[None], lengths, places[2], replica[None], numbers, places[0], places[1]]
    )
    (wq, wo), (final_row, table) = gather_weights(
        meta, w_qkv[0], w_out[0], (final_gain[None, :], rotary_table())
    )
    ticks = micro + stages - 1
    half = stages // 2
    state, turned = (), ()
    inbox = entry
    for tick in range(ticks):
        before = turned if tick in (1, half + micro) else ()
        out, *state = forward_layer(
            tick, stages - 1, micro, meta, inbox, entry, gain, table, wq, wo, before, state
        )
        if tick == 0:
            turned = turn(True, meta, out, wq, wo, turned)
        if tick == half + micro - 1:
            turned = turn(False, meta, out, wq, wo, turned)
        if tick < ticks - 1:
            pairs = [(s, s + 1) for s in range(stages - 1) if 0 <= tick - s < micro]
            inbox = lax.ppermute(out, "section", pairs)
    *stash, last = state
    count = lax.axis_size(DP[:2])
    copies = embed(count, last, final_row, positive)
    here = lax.all_to_all(copies, DP[:2], split_axis=0, concat_axis=0, tiled=True)
    here = here.reshape(count * 8, WIDE)
    there = lax.ppermute(here, "dp_2", [(0, 1), (1, 0)])
    seed = loss_seed(meta, last, final_row, here, there)
    grads = ()
    for tick in range(ticks):
        out, *grads = backward_layer(
            tick, stages - 1, micro, meta, inbox, seed, gain, table, *turned, stash, grads
        )
        if tick < ticks - 1:
            pairs = [
                (stages - 1 - s, stages - 2 - s)
                for s in range(stages - 1)
                if 0 <= tick - s < micro
            ]
            inbox = lax.ppermute(out, "section", pairs)
    return grads[0][None]


def solution(mesh):
    finer = Mesh(
        mesh.devices.reshape(mesh.shape["section"], 4, 4, 2), ("section", "dp_0", "dp_1", "dp_2")
    )
    in_specs = (
        P(DP, None),
        P("section", None),
        P("section", DP, None),
        P("section", DP, None),
        P(),
        P(DP),
        P(DP),
    )
    return jax.shard_map(
        per_device,
        mesh=finer,
        in_specs=in_specs,
        out_specs=P("section", DP, None),
        check_vma=False,
    )
```

```python
import functools

import jax
import jax.numpy as jnp
from jax import lax
from jax.experimental import pallas as pl
from jax.experimental.pallas import tpu as pltpu
from jax.sharding import Mesh
from jax.sharding import PartitionSpec as P

HEAD_DIM = 64
LEN = 48
D = 3584
QW = 896
KV = 128
XW = QW + 2 * KV
PACK = XW + QW
PAIRS = QW // 128
DP = ("dp_0", "dp_1", "dp_2")
ROPE_BASE = 1000000.0
EPS = 1e-06
SHARP = 20.0
COEF = 256.0
HALVES = 2
HALF = D // HALVES
STAGGER = 5000
EVEN = 850
F32 = jnp.float32
BF16 = jnp.bfloat16


def dot_nn(a, b):
    return lax.dot_general(a, b, (((1,), (0,)), ((), ())), preferred_element_type=F32)


def dot_nt(a, b):
    return lax.dot_general(a, b, (((1,), (1,)), ((), ())), preferred_element_type=F32)


def dot_tn(a, b):
    return lax.dot_general(a, b, (((0,), (0,)), ((), ())), preferred_element_type=F32)


def lanes(rows):
    return lax.broadcasted_iota(jnp.int32, (rows, 128), 1)


def partner(x):
    low = lax.rem(lanes(x.shape[0]), 64) < 32
    return jnp.where(low, pltpu.roll(x, 96, 1), pltpu.roll(x, 32, 1))


def paired(z):
    left = lanes(LEN) < 64
    rolled = pltpu.roll(z, 64, 1)
    pad = jnp.zeros((16, 128), BF16)
    a_left = jnp.where(left, z, 0.0).astype(BF16)
    b_right = jnp.where(left, 0.0, z).astype(BF16)
    b_left = jnp.where(left, rolled, 0.0).astype(BF16)
    a_right = jnp.where(left, 0.0, rolled).astype(BF16)
    return (
        jnp.concatenate([a_left, pad, a_right, pad], axis=0),
        jnp.concatenate([a_left, pad, b_right, pad], axis=0),
        jnp.concatenate([b_left, pad, b_right, pad], axis=0),
    )


SPANS = ((0, 3 * LEN), (3 * LEN, 4 * LEN), (4 * LEN, 7 * LEN))


def by_pair(dot, rows, blocks):
    return jnp.concatenate(
        [dot(rows[lo:hi], block) for (lo, hi), block in zip(SPANS, blocks)], axis=0
    )


def unpaired(rows, other):
    left = lanes(LEN) < 64
    s00, s01, s11 = (dot_tn(rows[lo:hi], other[lo:hi]) for lo, hi in SPANS)
    first = jnp.where(left, s00[:LEN] + s01[:LEN], 0.0)
    first += pltpu.roll(jnp.where(left, 0.0, s00[64 : 64 + LEN]), 64, 1)
    second = jnp.where(left, 0.0, s01[64 : 64 + LEN] + s11[64 : 64 + LEN])
    second += pltpu.roll(jnp.where(left, s11[:LEN], 0.0), 64, 1)
    return first + second


def half_sums(x):
    left = lanes(x.shape[0]) < 64
    low = jnp.sum(jnp.where(left, x, 0.0), axis=1, keepdims=True)
    high = jnp.sum(jnp.where(left, 0.0, x), axis=1, keepdims=True)
    return low, high, left


def probabilities(q_rows, k_blocks, length):
    scores = by_pair(dot_nt, q_rows, k_blocks) * HEAD_DIM ** (-0.5)
    live = lax.rem(lanes(scores.shape[0]), 64) < length
    weights = jnp.where(live, jnp.exp(scores), 0.0)
    low, high, left = half_sums(weights)
    return weights * jnp.where(left, 1.0 / low, 1.0 / high)


def rows_of(x_ref):
    return jnp.concatenate([x_ref[:, 128 * i : 128 * i + 128] for i in range(PAIRS)], axis=0)


def inv_rms(wide):
    return lax.rsqrt(jnp.sum(wide * wide, axis=1, keepdims=True) * (1.0 / D) + EPS)


def forward_kernel(
    tick,
    last_stage,
    micro,
    meta,
    inbox,
    entry,
    gain,
    table,
    wq,
    wo,
    *refs,
):
    out, stash_h, stash_x, last, h_v, n_v, acc_v, x_v, ctx_v, last_v, sems = refs[-11:]
    stage = meta[0]
    slot = tick - stage

    @pl.when(jnp.logical_and(slot >= 0, slot < micro))
    def _():
        length = meta[1 + slot]
        row0 = pl.multiple_of(slot * LEN, LEN)

        @pl.when(stage == 0)
        def _():
            fresh = pltpu.make_async_copy(entry.at[pl.ds(row0, LEN), :], h_v, sems.at[0])
            fresh.start()
            fresh.wait()

        @pl.when(stage != 0)
        def _():
            h_v[...] = inbox[:LEN]

        @pl.when(meta[5] == 1)
        def _():
            pl.delay(STAGGER if tick == 0 else EVEN)

        keep_h = pltpu.make_async_copy(h_v, stash_h.at[pl.ds(row0, LEN), :], sems.at[1])
        keep_h.start()
        wide = h_v[...].astype(F32)
        n_v[...] = (wide * inv_rms(wide) * gain[...]).astype(BF16)
        acc_v[...] = jnp.zeros_like(acc_v)

        @pl.loop(0, HALVES)
        def _(i):
            cols = pl.ds(pl.multiple_of(i * HALF, HALF), HALF)
            acc_v[...] += dot_nn(n_v[:, cols], wq[cols, :])

        cosine, sine = table[0], table[1]
        for i in range(PAIRS + 1):
            part = acc_v[:, 128 * i : 128 * i + 128]
            x_v[:, 128 * i : 128 * i + 128] = (part * cosine + partner(part) * sine).astype(BF16)
        x_v[:, QW + KV :] = acc_v[:, QW + KV :].astype(BF16)
        keep_x = pltpu.make_async_copy(x_v, stash_x.at[pl.ds(row0, LEN), :], sems.at[2])
        keep_x.start()
        k_blocks = paired(x_v[:, QW : QW + KV].astype(F32))
        v_blocks = paired(x_v[:, QW + KV :].astype(F32))
        probs = probabilities(rows_of(x_v), k_blocks, length).astype(BF16)
        context = by_pair(dot_nn, probs, v_blocks).astype(BF16)
        for i in range(PAIRS):
            ctx_v[:, 128 * i : 128 * i + 128] = context[LEN * i : LEN * i + LEN]

        @pl.loop(0, HALVES)
        def _(i):
            cols = pl.ds(pl.multiple_of(i * HALF, HALF), HALF)
            branch = dot_nn(ctx_v[...], wo[:, cols])
            out[:, cols] = (h_v[:, cols].astype(F32) + branch).astype(BF16)

        @pl.when(stage == last_stage)
        def _():
            hit = lax.broadcasted_iota(jnp.int32, (LEN, D), 0) == length - 1
            row = jnp.sum(jnp.where(hit, out[...].astype(F32), 0.0), axis=0, keepdims=True)
            last_v[...] = jnp.broadcast_to(row, (8, D))
            put = pltpu.make_async_copy(last_v, last.at[slot], sems.at[3])
            put.start()
            put.wait()

        keep_h.wait()
        keep_x.wait()


def backward_kernel(
    tick,
    last_stage,
    micro,
    meta,
    inbox,
    seed,
    gain,
    table,
    wq,
    wo,
    stash_h,
    stash_x,
    *refs,
):
    out, grads, h_v, g_v, x_v, dctx_v, dx_v, dn_v, sems = refs[-9:]
    stage = meta[0]
    slot = tick - (last_stage - stage)

    def put(value, to):
        rows = pl.ds(pl.multiple_of(to * LEN, LEN), LEN)
        return pltpu.make_async_copy(value, grads.at[rows, :], sems.at[2])

    late = jnp.logical_and(slot >= 1, slot <= micro)
    if tick > 0:

        @pl.when(late)
        def _():
            put(refs[0], slot - 1).start()

    @pl.when(jnp.logical_and(slot >= 0, slot < micro))
    def _():
        length = meta[1 + slot]
        row0 = pl.multiple_of(slot * LEN, LEN)

        get_x = pltpu.make_async_copy(stash_x.at[pl.ds(row0, LEN), :], x_v, sems.at[0])
        get_h = pltpu.make_async_copy(stash_h.at[pl.ds(row0, LEN), :], h_v, sems.at[1])
        get_x.start()
        get_h.start()

        @pl.when(meta[5] == 1)
        def _():
            pl.delay(STAGGER if tick == 0 else EVEN)

        @pl.when(stage == last_stage)
        def _():
            hit = lax.broadcasted_iota(jnp.int32, (LEN, D), 0) == length - 1
            row = jnp.where(lax.broadcasted_iota(jnp.int32, (8, D), 0) == slot, seed[...], 0.0)
            row = jnp.sum(row, axis=0, keepdims=True)
            g_v[...] = jnp.where(hit, jnp.broadcast_to(row, (LEN, D)), 0.0).astype(BF16)

        @pl.when(stage != last_stage)
        def _():
            g_v[...] = inbox[...]

        dctx_v[...] = jnp.zeros_like(dctx_v)

        @pl.loop(0, HALVES)
        def _(i):
            cols = pl.ds(pl.multiple_of(i * HALF, HALF), HALF)
            dctx_v[...] += dot_nn(g_v[:, cols], wo[cols, :])

        get_x.wait()
        q_rows = rows_of(x_v)
        k_blocks = paired(x_v[:, QW : QW + KV].astype(F32))
        v_blocks = paired(x_v[:, QW + KV :].astype(F32))
        probs = probabilities(q_rows, k_blocks, length)
        dctx = rows_of(dctx_v).astype(BF16)
        dvalue = unpaired(probs.astype(BF16), dctx)
        dprobs = by_pair(dot_nt, dctx, v_blocks).astype(BF16).astype(F32)
        low, high, left = half_sums(dprobs * probs)
        dscores = probs * (dprobs - jnp.where(left, low, high)) * HEAD_DIM ** (-0.5)
        dscores = dscores.astype(BF16)
        dquery = by_pair(dot_nn, dscores, k_blocks).astype(BF16).astype(F32)
        dkey = unpaired(dscores, q_rows).astype(BF16).astype(F32)
        cosine, sine = table[0], table[1]
        for i in range(PAIRS):
            part = dquery[LEN * i : LEN * i + LEN]
            dx_v[:, 128 * i : 128 * i + 128] = (part * cosine - partner(part) * sine).astype(BF16)
        dx_v[:, QW : QW + KV] = (dkey * cosine - partner(dkey) * sine).astype(BF16)
        dx_v[:, QW + KV :] = dvalue.astype(BF16)

        @pl.loop(0, HALVES)
        def _(i):
            cols = pl.ds(pl.multiple_of(i * HALF, HALF), HALF)
            dn_v[:, cols] = dot_nn(dx_v[...], wq[:, cols]).astype(BF16)

        get_h.wait()
        wide = h_v[...].astype(F32)
        scale = inv_rms(wide)
        scaled = dn_v[...].astype(F32) * gain[...]
        inner = jnp.sum(scaled * wide, axis=1, keepdims=True)
        out[...] = (
            g_v[...].astype(F32)
            + scale * scaled
            - wide * (scale * scale * scale * inner * (1.0 / D))
        ).astype(BF16)

    if tick > 0:

        @pl.when(late)
        def _():
            put(refs[0], slot - 1).wait()

    if tick == last_stage + micro - 1:

        @pl.when(slot == micro - 1)
        def _():
            put(out, slot).start()
            put(out, slot).wait()


ANY = pl.BlockSpec(memory_space=pl.ANY)
VMEM = pl.BlockSpec(memory_space=pltpu.VMEM)
SMEM = pl.BlockSpec(memory_space=pltpu.SMEM)
HBM = pl.BlockSpec(memory_space=pltpu.HBM)
LAYER_COST = pl.CostEstimate(
    flops=2 * LEN * D * (XW + QW), bytes_accessed=2 * D * (XW + QW), transcendentals=0
)
LIMIT = 8 * 1024 * 1024
LARGE = 14 * 1024 * 1024
WHOLE = 60 * 1024 * 1024
SMALL = 8 * 1024 * 1024


def forward_layer(
    tick, last_stage, micro, meta, inbox, entry, gain, table, wq, wo, before, state
):
    rows = micro * LEN
    kept = (((rows, D), BF16), ((rows, XW), BF16), ((micro, 8, D), F32))
    return pl.pallas_call(
        functools.partial(forward_kernel, tick, last_stage, micro),
        out_shape=tuple(jax.ShapeDtypeStruct(*a) for a in (((LEN, D), BF16), *kept)),
        in_specs=[SMEM, VMEM, ANY, VMEM, VMEM, VMEM, VMEM, *[ANY] * len((*before, *state))],
        out_specs=(VMEM, ANY, ANY, ANY),
        input_output_aliases={7 + len(before) + i: 1 + i for i in range(len(state))},
        scratch_shapes=[
            pltpu.VMEM((LEN, D), BF16),
            pltpu.VMEM((LEN, D), BF16),
            pltpu.VMEM((LEN, XW), F32),
            pltpu.VMEM((LEN, XW), BF16),
            pltpu.VMEM((LEN, QW), BF16),
            pltpu.VMEM((8, D), F32),
            pltpu.SemaphoreType.DMA((4,)),
        ],
        compiler_params=pltpu.CompilerParams(vmem_limit_bytes=LIMIT),
        cost_estimate=LAYER_COST,
        name="forward_layer",
    )(meta, inbox, entry, gain, table, wq, wo, *before, *state)


def backward_layer(
    tick, last_stage, micro, meta, inbox, seed, gain, table, wq_t, wo_t, stash, previous
):
    return pl.pallas_call(
        functools.partial(backward_kernel, tick, last_stage, micro),
        out_shape=(
            jax.ShapeDtypeStruct((LEN, D), BF16),
            jax.ShapeDtypeStruct((micro * LEN, D), BF16),
        ),
        in_specs=[SMEM, VMEM, VMEM, VMEM, VMEM, VMEM, VMEM, ANY, ANY, *[ANY] * len(previous)],
        out_specs=(VMEM, ANY),
        input_output_aliases={10: 1} if previous else {},
        scratch_shapes=[
            pltpu.VMEM((LEN, D), BF16),
            pltpu.VMEM((LEN, D), BF16),
            pltpu.VMEM((LEN, XW), BF16),
            pltpu.VMEM((LEN, QW), F32),
            pltpu.VMEM((LEN, XW), BF16),
            pltpu.VMEM((LEN, D), BF16),
            pltpu.SemaphoreType.DMA((3,)),
        ],
        compiler_params=pltpu.CompilerParams(vmem_limit_bytes=LIMIT),
        cost_estimate=LAYER_COST,
        name="backward_layer",
    )(meta, inbox, seed, gain, table, wq_t, wo_t, *stash, *previous)


TURN = 256


def turn_kernel(early, meta, after, wq, wo, *refs):
    del after
    wq_t, wo_t, wq_v, wo_v, sems = refs[-5:]
    half = lax.div(meta[7], 2)
    due = meta[0] >= half if early else meta[0] < half

    @pl.when(due)
    def _():
        def copies(i, slot):
            at = pl.ds(pl.multiple_of(i * TURN, TURN), TURN)
            return (
                pltpu.make_async_copy(wq_v.at[slot], wq_t.at[:, at], sems.at[0, slot]),
                pltpu.make_async_copy(wo_v.at[slot], wo_t.at[at, :], sems.at[1, slot]),
            )

        @pl.loop(0, D // TURN)
        def _(i):
            slot = lax.rem(i, 2)
            at = pl.ds(pl.multiple_of(i * TURN, TURN), TURN)

            @pl.when(i >= 2)
            def _():
                for copy in copies(i - 2, slot):
                    copy.wait()

            wq_v[slot] = wq[at, :].T
            wo_v[slot] = wo[:, at].T
            for copy in copies(i, slot):
                copy.start()

        for i in (D // TURN - 2, D // TURN - 1):
            for copy in copies(i, i % 2):
                copy.wait()


def turn(early, meta, after, wq, wo, turned):
    return pl.pallas_call(
        functools.partial(turn_kernel, early),
        out_shape=(jax.ShapeDtypeStruct((XW, D), BF16), jax.ShapeDtypeStruct((D, QW), BF16)),
        in_specs=[SMEM, ANY, VMEM, VMEM, *[ANY] * len(turned)],
        out_specs=(ANY, ANY),
        input_output_aliases={4 + i: i for i in range(len(turned))},
        scratch_shapes=[
            pltpu.VMEM((2, XW, TURN), BF16),
            pltpu.VMEM((2, TURN, QW), BF16),
            pltpu.SemaphoreType.DMA((2, 2)),
        ],
        compiler_params=pltpu.CompilerParams(vmem_limit_bytes=LIMIT),
        cost_estimate=pl.CostEstimate(flops=0, bytes_accessed=4 * D * (XW + QW), transcendentals=0),
        name="turn",
    )(meta, after, wq, wo, *turned)


SIDE = PACK // 2


def pack_kernel(meta, w_qkv, w_out, keep, give, w_v, x_v, sems):
    first = pltpu.make_async_copy(w_out, w_v, sems.at[0])
    second = pltpu.make_async_copy(w_qkv, x_v, sems.at[1])
    first.start()
    second.start()
    first.wait()
    pieces = [w_v[:, QW * j : QW * j + QW].astype(F32) for j in range(D // QW)]
    low = jnp.concatenate(pieces, axis=0).astype(BF16)
    second.wait()

    def fill(left, right):
        left[...] = x_v[:, :SIDE]
        right[:, : XW - SIDE] = x_v[:, SIDE:]
        right[:, XW - SIDE :] = low

    @pl.when(meta[5] == 0)
    def _():
        fill(keep, give)

    @pl.when(meta[5] == 1)
    def _():
        fill(give, keep)


def pack(meta, w_qkv, w_out):
    side = jax.ShapeDtypeStruct((w_qkv.shape[0], SIDE), BF16)
    return pl.pallas_call(
        pack_kernel,
        out_shape=(side, side),
        in_specs=[SMEM, HBM, HBM],
        out_specs=(VMEM, VMEM),
        scratch_shapes=[
            pltpu.VMEM(w_out.shape, BF16),
            pltpu.VMEM(w_qkv.shape, BF16),
            pltpu.SemaphoreType.DMA((2,)),
        ],
        compiler_params=pltpu.CompilerParams(vmem_limit_bytes=WHOLE),
        name="pack",
    )(meta, w_qkv, w_out)


def unpack_kernel(meta, *refs):
    count = (len(refs) - 4) // 2
    mine, theirs = refs[:count], refs[count : 2 * count]
    wq, wo, part_v, sems = refs[2 * count :]
    parts = D // QW
    length = D // 32
    short = length // parts
    x0, y0, core = meta[8], meta[9], meta[5]

    def offset(step):
        return jnp.where(step == 1, 3, jnp.where(step == 2, 1, jnp.where(step == 3, 2, 0)))

    def put(blocks, color):
        for n in range(8):
            block = blocks[n]
            far, other = n // 2, n % 2

            @pl.loop(0, 4)
            def _(near):
                first = lax.rem(offset(near) + (y0 if color == 0 else x0), 4)
                second = lax.rem((0, 3, 1, 2)[far] + (x0 if color == 0 else y0), 4)
                x, y = (second, first) if color == 0 else (first, second)
                shard = x * 8 + y * 2 + (color if other == 0 else 1 - color)
                rows = pl.ds(pl.multiple_of(shard * length, length), length)
                if color == 0:
                    pltpu.make_async_copy(
                        block.at[near], wq.at[rows, pl.ds(0, SIDE)], sems.at[0]
                    ).start()
                else:
                    pltpu.make_async_copy(
                        block.at[near, :, pl.ds(0, XW - SIDE)],
                        wq.at[rows, pl.ds(SIDE, XW - SIDE)],
                        sems.at[0],
                    ).start()
                    pltpu.make_async_copy(
                        block.at[near, :, pl.ds(XW - SIDE, QW)], part_v.at[rows, :], sems.at[1]
                    ).start()

    @pl.when(core == 0)
    def _():
        put(theirs, 1)
        put(mine, 0)

    @pl.when(core == 1)
    def _():
        put(mine, 1)
        put(theirs, 0)

    pltpu.make_async_copy(part_v, part_v, sems.at[1]).wait()

    @pl.loop(0, 8)
    def _(i):
        blocks = []
        for r in range(4):
            at = pl.ds(pl.multiple_of((4 * i + r) * length, length), length)
            blocks.append(part_v[at, :].astype(F32))
        to = pl.ds(pl.multiple_of(i * length, length), length)
        for j in range(parts):
            cut = [block[short * j : short * j + short] for block in blocks]
            wo[to, QW * j : QW * j + QW] = jnp.concatenate(cut, axis=0).astype(BF16)

    pltpu.make_async_copy(wq, wq, sems.at[0]).wait()


def unpack(meta, mine, theirs):
    return pl.pallas_call(
        unpack_kernel,
        out_shape=(jax.ShapeDtypeStruct((D, XW), BF16), jax.ShapeDtypeStruct((QW, D), BF16)),
        in_specs=[SMEM, *[ANY] * (len(mine) + len(theirs))],
        out_specs=(VMEM, VMEM),
        scratch_shapes=[pltpu.VMEM((D, QW), BF16), pltpu.SemaphoreType.DMA((2,))],
        compiler_params=pltpu.CompilerParams(vmem_limit_bytes=LARGE),
        name="unpack",
    )(meta, *mine, *theirs)


def ring_step(value, second, step):
    pairs = []
    for x in range(4):
        for y in range(4):
            for core in range(2):
                along_y = (core == 0) != second
                to = (x, (y + step) % 4) if along_y else ((x + step) % 4, y)
                pairs.append((x * 8 + y * 2 + core, to[0] * 8 + to[1] * 2 + core))
    return lax.ppermute(value, DP, pairs)


def swap_cores(value):
    return lax.ppermute(value, "dp_2", [(0, 1), (1, 0)])


def join_kernel(*refs):
    *parts, out, sems = refs
    copies = [
        pltpu.make_async_copy(part, out.at[n], sems.at[n]) for n, part in enumerate(parts)
    ]
    for copy in copies:
        copy.start()
    for copy in copies:
        copy.wait()


def join(*parts):
    return pl.pallas_call(
        join_kernel,
        out_shape=jax.ShapeDtypeStruct((len(parts), *parts[0].shape), parts[0].dtype),
        in_specs=[ANY] * len(parts),
        out_specs=ANY,
        scratch_shapes=[pltpu.SemaphoreType.DMA((len(parts),))],
        compiler_params=pltpu.CompilerParams(vmem_limit_bytes=1024 * 1024),
        name="join",
    )(*parts)


def gather_weights(meta, w_qkv, w_out, others):
    keep, give = pack(meta, w_qkv, w_out)
    keep, got, others = lax.optimization_barrier((keep, swap_cores(give), others))
    lines = []
    for value, forward in ((keep, 1), (got, -1)):
        before = ring_step(value, False, 1)
        after = ring_step(value, False, -1)
        across = ring_step(before if forward == 1 else after, False, forward)
        lines.append(join(value, before, after, across))
    mine = [None] * 8
    for n, (line, forward) in enumerate(zip(lines, (1, -1))):
        before = ring_step(line, True, 1)
        after = ring_step(line, True, -1)
        across = ring_step(before if forward == 1 else after, True, forward)
        mine[n::2] = [line, before, after, across]
    return unpack(meta, mine, [swap_cores(value) for value in mine]), others


WIDE = HALF + 128


def pooled_rows(last):
    return jnp.concatenate([last[j, 0:1, :] for j in (0, 2, 1, 3)], axis=0)


def embed_kernel(last, final_gain, labels, out):
    rows = pooled_rows(last)
    pooled = rows * inv_rms(rows) * final_gain[...]
    unit = pooled * lax.rsqrt(jnp.sum(pooled * pooled, axis=1, keepdims=True))
    halves = jnp.concatenate([unit[:, :HALF], unit[:, HALF:]], axis=0).astype(BF16)
    which = lax.broadcasted_iota(jnp.int32, (8, 128), 0)
    label = jnp.where(which == 0, labels[0], jnp.where(which == 1, labels[1], 0))
    label = label.astype(F32).astype(BF16)
    for i in range(out.shape[0]):
        out[i, :, :HALF] = halves
        out[i, :, HALF:] = label


def embed(count, last, final_gain, labels):
    return pl.pallas_call(
        embed_kernel,
        out_shape=jax.ShapeDtypeStruct((count, 8, WIDE), BF16),
        in_specs=[VMEM, VMEM, SMEM],
        out_specs=VMEM,
        compiler_params=pltpu.CompilerParams(vmem_limit_bytes=LIMIT),
        name="embed",
    )(last, final_gain, labels)


def loss_kernel(meta, last, final_gain, here, there, seed):
    everyone = jnp.concatenate([here[...], there[...]], axis=0)
    count = everyone.shape[0]
    emb = everyone[:, :HALF]
    label = everyone[:, HALF:].astype(F32)[:, 0:1].astype(jnp.int32)
    scores = dot_nt(emb, emb)
    scores = scores + pltpu.roll(pltpu.roll(scores, count - 4, 0), count - 4, 1)
    row = lax.rem(lax.broadcasted_iota(jnp.int32, (count, count), 0), 8)
    col = lax.broadcasted_iota(jnp.int32, (count, count), 1)
    doc = jnp.logical_and(lax.rem(col, 8) >= 2, lax.rem(col, 8) < 4)
    valid = jnp.logical_and(row < 2, doc)
    weights = jnp.where(valid, jnp.exp(scores * SHARP), 0.0)
    total = jnp.sum(weights, axis=1, keepdims=True)
    prob = weights / jnp.where(row[:, :1] < 2, total, 1.0)
    owner = lax.div(label, 2)
    away = (lax.rem(owner, 2) != meta[5]).astype(jnp.int32)
    target = away * (count // 2) + lax.div(owner, 2) * 8 + 2 + lax.rem(label, 2)
    coef = jnp.where(valid, (prob - (col == target).astype(F32)) * (COEF * SHARP), 0.0)
    both = coef + coef.T
    mine = lax.broadcasted_iota(jnp.int32, (8, count), 0)
    pick = lax.broadcasted_iota(jnp.int32, (8, count), 1) == lax.div(meta[6], 2) * 8 + mine
    own = lax.dot_general(
        pick.astype(F32),
        both,
        (((1,), (0,)), ((), ())),
        precision=lax.Precision.HIGHEST,
        preferred_element_type=F32,
    )[:4]
    own = jnp.concatenate([own, pltpu.roll(own, 4, 1)], axis=0)
    top = own.astype(BF16)
    rest = own - top.astype(F32)
    mid = rest.astype(BF16)
    low = (rest - mid.astype(F32)).astype(BF16)
    grad = dot_nn(top, emb) + (dot_nn(mid, emb) + dot_nn(low, emb))
    grad = jnp.concatenate([grad[:4], grad[4:]], axis=1)
    rows = pooled_rows(last)
    gain = final_gain[...]
    scale = inv_rms(rows)
    pooled = rows * scale * gain
    norm = lax.rsqrt(jnp.sum(pooled * pooled, axis=1, keepdims=True))
    unit = pooled * norm
    dpooled = norm * (grad - unit * jnp.sum(grad * unit, axis=1, keepdims=True))
    scaled = dpooled * gain
    inner = jnp.sum(scaled * rows, axis=1, keepdims=True)
    drow = scale * scaled - rows * (scale * scale * scale * inner * (1.0 / D))
    drow = drow.astype(BF16).astype(F32)
    seed[...] = jnp.concatenate(
        [drow[0:1], drow[2:3], drow[1:2], drow[3:4], jnp.zeros((4, D), F32)], axis=0
    )


def loss_seed(meta, last, final_gain, here, there):
    return pl.pallas_call(
        loss_kernel,
        out_shape=jax.ShapeDtypeStruct((8, D), F32),
        in_specs=[SMEM, VMEM, VMEM, VMEM, VMEM],
        out_specs=VMEM,
        compiler_params=pltpu.CompilerParams(vmem_limit_bytes=LIMIT),
        name="loss_seed",
    )(meta, last, final_gain, here, there)


def rotary_table():
    lane = jnp.arange(128, dtype=jnp.int32)
    frequency = ROPE_BASE ** (-(lane % 32).astype(F32) * (2.0 / HEAD_DIM))
    angles = jnp.arange(LEN, dtype=F32)[:, None] * frequency[None, :]
    sign = jnp.where(lane % 64 < 32, -1.0, 1.0)
    return jnp.stack([jnp.cos(angles), jnp.sin(angles) * sign])


def per_device(entry, norm_gain, w_qkv, w_out, final_gain, lengths, positive):
    stage = lax.axis_index("section")
    stages = lax.axis_size("section")
    replica = lax.axis_index(DP)
    places = [lax.axis_index(name)[None] for name in DP]
    micro = lengths.shape[0]
    gain = norm_gain
    numbers = jnp.array([stages], jnp.int32)
    meta = jnp.concatenate(
        [stage[None], lengths, places[2], replica[None], numbers, places[0], places[1]]
    )
    (wq, wo), (final_row, table) = gather_weights(
        meta, w_qkv[0], w_out[0], (final_gain[None, :], rotary_table())
    )
    ticks = micro + stages - 1
    half = stages // 2
    state, turned = (), ()
    inbox = entry
    for tick in range(ticks):
        before = turned if tick in (1, half + micro) else ()
        out, *state = forward_layer(
            tick, stages - 1, micro, meta, inbox, entry, gain, table, wq, wo, before, state
        )
        if tick == 0:
            turned = turn(True, meta, out, wq, wo, turned)
        if tick == half + micro - 1:
            turned = turn(False, meta, out, wq, wo, turned)
        if tick < ticks - 1:
            pairs = [(s, s + 1) for s in range(stages - 1) if 0 <= tick - s < micro]
            inbox = lax.ppermute(out, "section", pairs)
    *stash, last = state
    count = lax.axis_size(DP[:2])
    copies = embed(count, last, final_row, positive)
    here = lax.all_to_all(copies, DP[:2], split_axis=0, concat_axis=0, tiled=True)
    here = here.reshape(count * 8, WIDE)
    there = lax.ppermute(here, "dp_2", [(0, 1), (1, 0)])
    seed = loss_seed(meta, last, final_row, here, there)
    previous = ()
    for tick in range(ticks):
        previous = backward_layer(
            tick, stages - 1, micro, meta, inbox, seed, gain, table, *turned, stash, previous
        )
        if tick < ticks - 1:
            pairs = [
                (stages - 1 - s, stages - 2 - s)
                for s in range(stages - 1)
                if 0 <= tick - s < micro
            ]
            inbox = lax.ppermute(previous[0], "section", pairs)
    return previous[1][None]


def solution(mesh):
    finer = Mesh(
        mesh.devices.reshape(mesh.shape["section"], 4, 4, 2), ("section", "dp_0", "dp_1", "dp_2")
    )
    in_specs = (
        P(DP, None),
        P("section", None),
        P("section", DP, None),
        P("section", DP, None),
        P(),
        P(DP),
        P(DP),
    )
    return jax.shard_map(
        per_device,
        mesh=finer,
        in_specs=in_specs,
        out_specs=P("section", DP, None),
        check_vma=False,
    )
```

```python
import functools

import jax
import jax.numpy as jnp
from jax import lax
from jax.experimental import pallas as pl
from jax.experimental.pallas import tpu as pltpu
from jax.sharding import Mesh
from jax.sharding import PartitionSpec as P

HEAD_DIM = 64
LEN = 48
D = 3584
QW = 896
KV = 128
XW = QW + 2 * KV
PACK = XW + QW
PAIRS = QW // 128
DP = ("dp_0", "dp_1", "dp_2")
ROPE_BASE = 1000000.0
EPS = 1e-06
SHARP = 20.0
COEF = 256.0
HALVES = 2
HALF = D // HALVES
STAGGER = 5000
EVEN = 850
F32 = jnp.float32
BF16 = jnp.bfloat16


def dot_nn(a, b):
    return lax.dot_general(a, b, (((1,), (0,)), ((), ())), preferred_element_type=F32)


def dot_nt(a, b):
    return lax.dot_general(a, b, (((1,), (1,)), ((), ())), preferred_element_type=F32)


def dot_tn(a, b):
    return lax.dot_general(a, b, (((0,), (0,)), ((), ())), preferred_element_type=F32)


def lanes(rows):
    return lax.broadcasted_iota(jnp.int32, (rows, 128), 1)


def partner(x):
    low = lax.rem(lanes(x.shape[0]), 64) < 32
    return jnp.where(low, pltpu.roll(x, 96, 1), pltpu.roll(x, 32, 1))


def paired(z):
    left = lanes(LEN) < 64
    rolled = pltpu.roll(z, 64, 1)
    pad = jnp.zeros((16, 128), BF16)
    a_left = jnp.where(left, z, 0.0).astype(BF16)
    b_right = jnp.where(left, 0.0, z).astype(BF16)
    b_left = jnp.where(left, rolled, 0.0).astype(BF16)
    a_right = jnp.where(left, 0.0, rolled).astype(BF16)
    return (
        jnp.concatenate([a_left, pad, a_right, pad], axis=0),
        jnp.concatenate([a_left, pad, b_right, pad], axis=0),
        jnp.concatenate([b_left, pad, b_right, pad], axis=0),
    )


SPANS = ((0, 3 * LEN), (3 * LEN, 4 * LEN), (4 * LEN, 7 * LEN))


def by_pair(dot, rows, blocks):
    return jnp.concatenate(
        [dot(rows[lo:hi], block) for (lo, hi), block in zip(SPANS, blocks)], axis=0
    )


def unpaired(rows, other):
    left = lanes(LEN) < 64
    s00, s01, s11 = (dot_tn(rows[lo:hi], other[lo:hi]) for lo, hi in SPANS)
    first = jnp.where(left, s00[:LEN] + s01[:LEN], 0.0)
    first += pltpu.roll(jnp.where(left, 0.0, s00[64 : 64 + LEN]), 64, 1)
    second = jnp.where(left, 0.0, s01[64 : 64 + LEN] + s11[64 : 64 + LEN])
    second += pltpu.roll(jnp.where(left, s11[:LEN], 0.0), 64, 1)
    return first + second


def half_sums(x):
    left = lanes(x.shape[0]) < 64
    low = jnp.sum(jnp.where(left, x, 0.0), axis=1, keepdims=True)
    high = jnp.sum(jnp.where(left, 0.0, x), axis=1, keepdims=True)
    return low, high, left


def probabilities(q_rows, k_blocks, length):
    scores = by_pair(dot_nt, q_rows, k_blocks) * HEAD_DIM ** (-0.5)
    live = lax.rem(lanes(scores.shape[0]), 64) < length
    weights = jnp.where(live, jnp.exp(scores), 0.0)
    low, high, left = half_sums(weights)
    return weights * jnp.where(left, 1.0 / low, 1.0 / high)


def rows_of(x_ref):
    return jnp.concatenate([x_ref[:, 128 * i : 128 * i + 128] for i in range(PAIRS)], axis=0)


def inv_rms(wide):
    return lax.rsqrt(jnp.sum(wide * wide, axis=1, keepdims=True) * (1.0 / D) + EPS)


def forward_kernel(
    tick,
    last_stage,
    micro,
    meta,
    inbox,
    entry,
    gain,
    table,
    wq,
    wo,
    *refs,
):
    out, stash_h, stash_x, last, h_v, n_v, acc_v, x_v, ctx_v, last_v, sems = refs[-11:]
    stage = meta[0]
    slot = tick - stage

    @pl.when(jnp.logical_and(slot >= 0, slot < micro))
    def _():
        length = meta[1 + slot]
        row0 = pl.multiple_of(slot * LEN, LEN)

        @pl.when(stage == 0)
        def _():
            fresh = pltpu.make_async_copy(entry.at[pl.ds(row0, LEN), :], h_v, sems.at[0])
            fresh.start()
            fresh.wait()

        @pl.when(stage != 0)
        def _():
            h_v[...] = inbox[:LEN]

        @pl.when(jnp.logical_and(meta[5] == 1, stage != last_stage))
        def _():
            pl.delay(STAGGER if tick == 0 else EVEN)

        keep_h = pltpu.make_async_copy(h_v, stash_h.at[pl.ds(row0, LEN), :], sems.at[1])
        keep_h.start()
        wide = h_v[...].astype(F32)
        n_v[...] = (wide * inv_rms(wide) * gain[...]).astype(BF16)
        acc_v[...] = jnp.zeros_like(acc_v)

        @pl.loop(0, HALVES)
        def _(i):
            cols = pl.ds(pl.multiple_of(i * HALF, HALF), HALF)
            acc_v[...] += dot_nn(n_v[:, cols], wq[cols, :])

        cosine, sine = table[0], table[1]
        for i in range(PAIRS + 1):
            part = acc_v[:, 128 * i : 128 * i + 128]
            x_v[:, 128 * i : 128 * i + 128] = (part * cosine + partner(part) * sine).astype(BF16)
        x_v[:, QW + KV :] = acc_v[:, QW + KV :].astype(BF16)
        keep_x = pltpu.make_async_copy(x_v, stash_x.at[pl.ds(row0, LEN), :], sems.at[2])
        keep_x.start()
        k_blocks = paired(x_v[:, QW : QW + KV].astype(F32))
        v_blocks = paired(x_v[:, QW + KV :].astype(F32))
        probs = probabilities(rows_of(x_v), k_blocks, length).astype(BF16)
        context = by_pair(dot_nn, probs, v_blocks).astype(BF16)
        for i in range(PAIRS):
            ctx_v[:, 128 * i : 128 * i + 128] = context[LEN * i : LEN * i + LEN]

        @pl.loop(0, HALVES)
        def _(i):
            cols = pl.ds(pl.multiple_of(i * HALF, HALF), HALF)
            branch = dot_nn(ctx_v[...], wo[:, cols])
            out[:, cols] = (h_v[:, cols].astype(F32) + branch).astype(BF16)

        @pl.when(stage == last_stage)
        def _():
            hit = lax.broadcasted_iota(jnp.int32, (LEN, D), 0) == length - 1
            row = jnp.sum(jnp.where(hit, out[...].astype(F32), 0.0), axis=0, keepdims=True)
            last_v[...] = jnp.broadcast_to(row, (8, D))
            put = pltpu.make_async_copy(last_v, last.at[slot], sems.at[3])
            put.start()
            put.wait()

        keep_h.wait()
        keep_x.wait()


def backward_kernel(
    tick,
    last_stage,
    micro,
    meta,
    inbox,
    seed,
    gain,
    table,
    wq,
    wo,
    stash_h,
    stash_x,
    *refs,
):
    out, grads, h_v, g_v, x_v, dctx_v, dx_v, dn_v, sems = refs[-9:]
    stage = meta[0]
    slot = tick - (last_stage - stage)

    def put(value, to):
        rows = pl.ds(pl.multiple_of(to * LEN, LEN), LEN)
        return pltpu.make_async_copy(value, grads.at[rows, :], sems.at[2])

    late = jnp.logical_and(slot >= 1, slot <= micro)
    if tick > 0:

        @pl.when(late)
        def _():
            put(refs[0], slot - 1).start()

    @pl.when(jnp.logical_and(slot >= 0, slot < micro))
    def _():
        length = meta[1 + slot]
        row0 = pl.multiple_of(slot * LEN, LEN)

        get_x = pltpu.make_async_copy(stash_x.at[pl.ds(row0, LEN), :], x_v, sems.at[0])
        get_h = pltpu.make_async_copy(stash_h.at[pl.ds(row0, LEN), :], h_v, sems.at[1])
        get_x.start()
        get_h.start()

        @pl.when(jnp.logical_and(meta[5] == 1, stage != 0))
        def _():
            pl.delay(STAGGER if tick == 0 else EVEN)

        @pl.when(stage == last_stage)
        def _():
            hit = lax.broadcasted_iota(jnp.int32, (LEN, D), 0) == length - 1
            row = jnp.where(lax.broadcasted_iota(jnp.int32, (8, D), 0) == slot, seed[...], 0.0)
            row = jnp.sum(row, axis=0, keepdims=True)
            g_v[...] = jnp.where(hit, jnp.broadcast_to(row, (LEN, D)), 0.0).astype(BF16)

        @pl.when(stage != last_stage)
        def _():
            g_v[...] = inbox[...]

        dctx_v[...] = jnp.zeros_like(dctx_v)

        @pl.loop(0, HALVES)
        def _(i):
            cols = pl.ds(pl.multiple_of(i * HALF, HALF), HALF)
            dctx_v[...] += dot_nn(g_v[:, cols], wo[cols, :])

        get_x.wait()
        q_rows = rows_of(x_v)
        k_blocks = paired(x_v[:, QW : QW + KV].astype(F32))
        v_blocks = paired(x_v[:, QW + KV :].astype(F32))
        probs = probabilities(q_rows, k_blocks, length)
        dctx = rows_of(dctx_v).astype(BF16)
        dvalue = unpaired(probs.astype(BF16), dctx)
        dprobs = by_pair(dot_nt, dctx, v_blocks).astype(BF16).astype(F32)
        low, high, left = half_sums(dprobs * probs)
        dscores = probs * (dprobs - jnp.where(left, low, high)) * HEAD_DIM ** (-0.5)
        dscores = dscores.astype(BF16)
        dquery = by_pair(dot_nn, dscores, k_blocks).astype(BF16).astype(F32)
        dkey = unpaired(dscores, q_rows).astype(BF16).astype(F32)
        cosine, sine = table[0], table[1]
        for i in range(PAIRS):
            part = dquery[LEN * i : LEN * i + LEN]
            dx_v[:, 128 * i : 128 * i + 128] = (part * cosine - partner(part) * sine).astype(BF16)
        dx_v[:, QW : QW + KV] = (dkey * cosine - partner(dkey) * sine).astype(BF16)
        dx_v[:, QW + KV :] = dvalue.astype(BF16)

        @pl.loop(0, HALVES)
        def _(i):
            cols = pl.ds(pl.multiple_of(i * HALF, HALF), HALF)
            dn_v[:, cols] = dot_nn(dx_v[...], wq[:, cols]).astype(BF16)

        get_h.wait()
        wide = h_v[...].astype(F32)
        scale = inv_rms(wide)
        scaled = dn_v[...].astype(F32) * gain[...]
        inner = jnp.sum(scaled * wide, axis=1, keepdims=True)
        out[...] = (
            g_v[...].astype(F32)
            + scale * scaled
            - wide * (scale * scale * scale * inner * (1.0 / D))
        ).astype(BF16)

    if tick > 0:

        @pl.when(late)
        def _():
            put(refs[0], slot - 1).wait()

    if tick == last_stage + micro - 1:

        @pl.when(slot == micro - 1)
        def _():
            put(out, slot).start()
            put(out, slot).wait()


ANY = pl.BlockSpec(memory_space=pl.ANY)
VMEM = pl.BlockSpec(memory_space=pltpu.VMEM)
SMEM = pl.BlockSpec(memory_space=pltpu.SMEM)
HBM = pl.BlockSpec(memory_space=pltpu.HBM)
LAYER_COST = pl.CostEstimate(
    flops=2 * LEN * D * (XW + QW), bytes_accessed=2 * D * (XW + QW), transcendentals=0
)
LIMIT = 8 * 1024 * 1024
LARGE = 14 * 1024 * 1024
WHOLE = 60 * 1024 * 1024
SMALL = 8 * 1024 * 1024


def forward_layer(
    tick, last_stage, micro, meta, inbox, entry, gain, table, wq, wo, before, state
):
    rows = micro * LEN
    kept = (((rows, D), BF16), ((rows, XW), BF16), ((micro, 8, D), F32))
    return pl.pallas_call(
        functools.partial(forward_kernel, tick, last_stage, micro),
        out_shape=tuple(jax.ShapeDtypeStruct(*a) for a in (((LEN, D), BF16), *kept)),
        in_specs=[SMEM, VMEM, ANY, VMEM, VMEM, VMEM, VMEM, *[ANY] * len((*before, *state))],
        out_specs=(VMEM, ANY, ANY, ANY),
        input_output_aliases={7 + len(before) + i: 1 + i for i in range(len(state))},
        scratch_shapes=[
            pltpu.VMEM((LEN, D), BF16),
            pltpu.VMEM((LEN, D), BF16),
            pltpu.VMEM((LEN, XW), F32),
            pltpu.VMEM((LEN, XW), BF16),
            pltpu.VMEM((LEN, QW), BF16),
            pltpu.VMEM((8, D), F32),
            pltpu.SemaphoreType.DMA((4,)),
        ],
        compiler_params=pltpu.CompilerParams(vmem_limit_bytes=LIMIT),
        cost_estimate=LAYER_COST,
        name="forward_layer",
    )(meta, inbox, entry, gain, table, wq, wo, *before, *state)


def backward_layer(
    tick, last_stage, micro, meta, inbox, seed, gain, table, wq_t, wo_t, stash, previous
):
    return pl.pallas_call(
        functools.partial(backward_kernel, tick, last_stage, micro),
        out_shape=(
            jax.ShapeDtypeStruct((LEN, D), BF16),
            jax.ShapeDtypeStruct((micro * LEN, D), BF16),
        ),
        in_specs=[SMEM, VMEM, VMEM, VMEM, VMEM, VMEM, VMEM, ANY, ANY, *[ANY] * len(previous)],
        out_specs=(VMEM, ANY),
        input_output_aliases={10: 1} if previous else {},
        scratch_shapes=[
            pltpu.VMEM((LEN, D), BF16),
            pltpu.VMEM((LEN, D), BF16),
            pltpu.VMEM((LEN, XW), BF16),
            pltpu.VMEM((LEN, QW), F32),
            pltpu.VMEM((LEN, XW), BF16),
            pltpu.VMEM((LEN, D), BF16),
            pltpu.SemaphoreType.DMA((3,)),
        ],
        compiler_params=pltpu.CompilerParams(vmem_limit_bytes=LIMIT),
        cost_estimate=LAYER_COST,
        name="backward_layer",
    )(meta, inbox, seed, gain, table, wq_t, wo_t, *stash, *previous)


TURN = 256


def turn_kernel(early, meta, after, wq, wo, *refs):
    del after
    wq_t, wo_t, wq_v, wo_v, sems = refs[-5:]
    half = lax.div(meta[7], 2)
    due = meta[0] >= half if early else meta[0] < half

    @pl.when(due)
    def _():
        def copies(i, slot):
            at = pl.ds(pl.multiple_of(i * TURN, TURN), TURN)
            return (
                pltpu.make_async_copy(wq_v.at[slot], wq_t.at[:, at], sems.at[0, slot]),
                pltpu.make_async_copy(wo_v.at[slot], wo_t.at[at, :], sems.at[1, slot]),
            )

        @pl.loop(0, D // TURN)
        def _(i):
            slot = lax.rem(i, 2)
            at = pl.ds(pl.multiple_of(i * TURN, TURN), TURN)

            @pl.when(i >= 2)
            def _():
                for copy in copies(i - 2, slot):
                    copy.wait()

            wq_v[slot] = wq[at, :].T
            wo_v[slot] = wo[:, at].T
            for copy in copies(i, slot):
                copy.start()

        for i in (D // TURN - 2, D // TURN - 1):
            for copy in copies(i, i % 2):
                copy.wait()


def turn(early, meta, after, wq, wo, turned):
    return pl.pallas_call(
        functools.partial(turn_kernel, early),
        out_shape=(jax.ShapeDtypeStruct((XW, D), BF16), jax.ShapeDtypeStruct((D, QW), BF16)),
        in_specs=[SMEM, ANY, VMEM, VMEM, *[ANY] * len(turned)],
        out_specs=(ANY, ANY),
        input_output_aliases={4 + i: i for i in range(len(turned))},
        scratch_shapes=[
            pltpu.VMEM((2, XW, TURN), BF16),
            pltpu.VMEM((2, TURN, QW), BF16),
            pltpu.SemaphoreType.DMA((2, 2)),
        ],
        compiler_params=pltpu.CompilerParams(vmem_limit_bytes=LIMIT),
        cost_estimate=pl.CostEstimate(flops=0, bytes_accessed=4 * D * (XW + QW), transcendentals=0),
        name="turn",
    )(meta, after, wq, wo, *turned)


SIDE = PACK // 2


def pack_kernel(core, w_qkv, w_out, keep, give, w_v, x_v, sems):
    first = pltpu.make_async_copy(w_out, w_v, sems.at[0])
    second = pltpu.make_async_copy(w_qkv, x_v, sems.at[1])
    first.start()
    second.start()
    first.wait()
    pieces = [w_v[:, QW * j : QW * j + QW].astype(F32) for j in range(D // QW)]
    low = jnp.concatenate(pieces, axis=0).astype(BF16)
    second.wait()

    def fill(left, right):
        left[...] = x_v[:, :SIDE]
        right[:, : XW - SIDE] = x_v[:, SIDE:]
        right[:, XW - SIDE :] = low

    @pl.when(core[0] == 0)
    def _():
        fill(keep, give)

    @pl.when(core[0] == 1)
    def _():
        fill(give, keep)


def pack(core, w_qkv, w_out):
    side = jax.ShapeDtypeStruct((w_qkv.shape[0], SIDE), BF16)
    return pl.pallas_call(
        pack_kernel,
        out_shape=(side, side),
        in_specs=[SMEM, HBM, HBM],
        out_specs=(VMEM, VMEM),
        scratch_shapes=[
            pltpu.VMEM(w_out.shape, BF16),
            pltpu.VMEM(w_qkv.shape, BF16),
            pltpu.SemaphoreType.DMA((2,)),
        ],
        compiler_params=pltpu.CompilerParams(vmem_limit_bytes=WHOLE),
        name="pack",
    )(core, w_qkv, w_out)


def unpack_kernel(meta, *refs):
    count = (len(refs) - 4) // 2
    mine, theirs = refs[:count], refs[count : 2 * count]
    wq, wo, part_v, sems = refs[2 * count :]
    parts = D // QW
    length = D // 32
    short = length // parts
    x0, y0, core = meta[8], meta[9], meta[5]

    def offset(step):
        return jnp.where(step == 1, 3, jnp.where(step == 2, 1, jnp.where(step == 3, 2, 0)))

    def put(blocks, color):
        for n in range(8):
            block = blocks[n]
            far, other = n // 2, n % 2

            @pl.loop(0, 4)
            def _(near):
                first = lax.rem(offset(near) + (y0 if color == 0 else x0), 4)
                second = lax.rem((0, 3, 1, 2)[far] + (x0 if color == 0 else y0), 4)
                x, y = (second, first) if color == 0 else (first, second)
                shard = x * 8 + y * 2 + (color if other == 0 else 1 - color)
                rows = pl.ds(pl.multiple_of(shard * length, length), length)
                if color == 0:
                    pltpu.make_async_copy(
                        block.at[near], wq.at[rows, pl.ds(0, SIDE)], sems.at[0]
                    ).start()
                else:
                    pltpu.make_async_copy(
                        block.at[near, :, pl.ds(0, XW - SIDE)],
                        wq.at[rows, pl.ds(SIDE, XW - SIDE)],
                        sems.at[0],
                    ).start()
                    pltpu.make_async_copy(
                        block.at[near, :, pl.ds(XW - SIDE, QW)], part_v.at[rows, :], sems.at[1]
                    ).start()

    @pl.when(core == 0)
    def _():
        put(theirs, 1)
        put(mine, 0)

    @pl.when(core == 1)
    def _():
        put(mine, 1)
        put(theirs, 0)

    pltpu.make_async_copy(part_v, part_v, sems.at[1]).wait()

    @pl.loop(0, 8)
    def _(i):
        blocks = []
        for r in range(4):
            at = pl.ds(pl.multiple_of((4 * i + r) * length, length), length)
            blocks.append(part_v[at, :].astype(F32))
        to = pl.ds(pl.multiple_of(i * length, length), length)
        for j in range(parts):
            cut = [block[short * j : short * j + short] for block in blocks]
            wo[to, QW * j : QW * j + QW] = jnp.concatenate(cut, axis=0).astype(BF16)

    pltpu.make_async_copy(wq, wq, sems.at[0]).wait()


def unpack(meta, mine, theirs):
    return pl.pallas_call(
        unpack_kernel,
        out_shape=(jax.ShapeDtypeStruct((D, XW), BF16), jax.ShapeDtypeStruct((QW, D), BF16)),
        in_specs=[SMEM, *[ANY] * (len(mine) + len(theirs))],
        out_specs=(VMEM, VMEM),
        scratch_shapes=[pltpu.VMEM((D, QW), BF16), pltpu.SemaphoreType.DMA((2,))],
        compiler_params=pltpu.CompilerParams(vmem_limit_bytes=LARGE),
        name="unpack",
    )(meta, *mine, *theirs)


def ring_step(value, second, step):
    pairs = []
    for x in range(4):
        for y in range(4):
            for core in range(2):
                along_y = (core == 0) != second
                to = (x, (y + step) % 4) if along_y else ((x + step) % 4, y)
                pairs.append((x * 8 + y * 2 + core, to[0] * 8 + to[1] * 2 + core))
    return lax.ppermute(value, DP, pairs)


def swap_cores(value):
    return lax.ppermute(value, "dp_2", [(0, 1), (1, 0)])


def join_kernel(*refs):
    *parts, out, sems = refs
    copies = [
        pltpu.make_async_copy(part, out.at[n], sems.at[n]) for n, part in enumerate(parts)
    ]
    for copy in copies:
        copy.start()
    for copy in copies:
        copy.wait()


def join(*parts):
    return pl.pallas_call(
        join_kernel,
        out_shape=jax.ShapeDtypeStruct((len(parts), *parts[0].shape), parts[0].dtype),
        in_specs=[ANY] * len(parts),
        out_specs=ANY,
        scratch_shapes=[pltpu.SemaphoreType.DMA((len(parts),))],
        compiler_params=pltpu.CompilerParams(vmem_limit_bytes=1024 * 1024),
        name="join",
    )(*parts)


def gather_weights(core, w_qkv, w_out, others):
    keep, give = pack(core, w_qkv, w_out)
    keep, got, others = lax.optimization_barrier((keep, swap_cores(give), others))
    meta = others[0]
    lines = []
    for value, forward in ((keep, 1), (got, -1)):
        before = ring_step(value, False, 1)
        after = ring_step(value, False, -1)
        across = ring_step(before if forward == 1 else after, False, forward)
        lines.append(join(value, before, after, across))
    mine = [None] * 8
    for n, (line, forward) in enumerate(zip(lines, (1, -1))):
        before = ring_step(line, True, 1)
        after = ring_step(line, True, -1)
        across = ring_step(before if forward == 1 else after, True, forward)
        mine[n::2] = [line, before, after, across]
    return unpack(meta, mine, [swap_cores(value) for value in mine]), others


WIDE = HALF + 128


def pooled_rows(last):
    return jnp.concatenate([last[j, 0:1, :] for j in (0, 2, 1, 3)], axis=0)


def embed_kernel(last, final_gain, labels, out):
    rows = pooled_rows(last)
    pooled = rows * inv_rms(rows) * final_gain[...]
    unit = pooled * lax.rsqrt(jnp.sum(pooled * pooled, axis=1, keepdims=True))
    halves = jnp.concatenate([unit[:, :HALF], unit[:, HALF:]], axis=0).astype(BF16)
    which = lax.broadcasted_iota(jnp.int32, (8, 128), 0)
    label = jnp.where(which == 0, labels[0], jnp.where(which == 1, labels[1], 0))
    label = label.astype(F32).astype(BF16)
    for i in range(out.shape[0]):
        out[i, :, :HALF] = halves
        out[i, :, HALF:] = label


def embed(count, last, final_gain, labels):
    return pl.pallas_call(
        embed_kernel,
        out_shape=jax.ShapeDtypeStruct((count, 8, WIDE), BF16),
        in_specs=[VMEM, VMEM, SMEM],
        out_specs=VMEM,
        compiler_params=pltpu.CompilerParams(vmem_limit_bytes=LIMIT),
        name="embed",
    )(last, final_gain, labels)


def loss_kernel(meta, last, final_gain, here, there, seed):
    everyone = jnp.concatenate([here[...], there[...]], axis=0)
    count = everyone.shape[0]
    emb = everyone[:, :HALF]
    label = everyone[:, HALF:].astype(F32)[:, 0:1].astype(jnp.int32)
    scores = dot_nt(emb, emb)
    scores = scores + pltpu.roll(pltpu.roll(scores, count - 4, 0), count - 4, 1)
    row = lax.rem(lax.broadcasted_iota(jnp.int32, (count, count), 0), 8)
    col = lax.broadcasted_iota(jnp.int32, (count, count), 1)
    doc = jnp.logical_and(lax.rem(col, 8) >= 2, lax.rem(col, 8) < 4)
    valid = jnp.logical_and(row < 2, doc)
    weights = jnp.where(valid, jnp.exp(scores * SHARP), 0.0)
    total = jnp.sum(weights, axis=1, keepdims=True)
    prob = weights / jnp.where(row[:, :1] < 2, total, 1.0)
    owner = lax.div(label, 2)
    away = (lax.rem(owner, 2) != meta[5]).astype(jnp.int32)
    target = away * (count // 2) + lax.div(owner, 2) * 8 + 2 + lax.rem(label, 2)
    coef = jnp.where(valid, (prob - (col == target).astype(F32)) * (COEF * SHARP), 0.0)
    both = coef + coef.T
    mine = lax.broadcasted_iota(jnp.int32, (8, count), 0)
    pick = lax.broadcasted_iota(jnp.int32, (8, count), 1) == lax.div(meta[6], 2) * 8 + mine
    own = lax.dot_general(
        pick.astype(F32),
        both,
        (((1,), (0,)), ((), ())),
        precision=lax.Precision.HIGHEST,
        preferred_element_type=F32,
    )[:4]
    own = jnp.concatenate([own, pltpu.roll(own, 4, 1)], axis=0)
    top = own.astype(BF16)
    rest = own - top.astype(F32)
    mid = rest.astype(BF16)
    low = (rest - mid.astype(F32)).astype(BF16)
    grad = dot_nn(top, emb) + (dot_nn(mid, emb) + dot_nn(low, emb))
    grad = jnp.concatenate([grad[:4], grad[4:]], axis=1)
    rows = pooled_rows(last)
    gain = final_gain[...]
    scale = inv_rms(rows)
    pooled = rows * scale * gain
    norm = lax.rsqrt(jnp.sum(pooled * pooled, axis=1, keepdims=True))
    unit = pooled * norm
    dpooled = norm * (grad - unit * jnp.sum(grad * unit, axis=1, keepdims=True))
    scaled = dpooled * gain
    inner = jnp.sum(scaled * rows, axis=1, keepdims=True)
    drow = scale * scaled - rows * (scale * scale * scale * inner * (1.0 / D))
    drow = drow.astype(BF16).astype(F32)
    seed[...] = jnp.concatenate(
        [drow[0:1], drow[2:3], drow[1:2], drow[3:4], jnp.zeros((4, D), F32)], axis=0
    )


def loss_seed(meta, last, final_gain, here, there):
    return pl.pallas_call(
        loss_kernel,
        out_shape=jax.ShapeDtypeStruct((8, D), F32),
        in_specs=[SMEM, VMEM, VMEM, VMEM, VMEM],
        out_specs=VMEM,
        compiler_params=pltpu.CompilerParams(vmem_limit_bytes=LIMIT),
        name="loss_seed",
    )(meta, last, final_gain, here, there)


def rotary_table():
    lane = jnp.arange(128, dtype=jnp.int32)
    frequency = ROPE_BASE ** (-(lane % 32).astype(F32) * (2.0 / HEAD_DIM))
    angles = jnp.arange(LEN, dtype=F32)[:, None] * frequency[None, :]
    sign = jnp.where(lane % 64 < 32, -1.0, 1.0)
    return jnp.stack([jnp.cos(angles), jnp.sin(angles) * sign])


def per_device(entry, norm_gain, w_qkv, w_out, final_gain, lengths, positive):
    stage = lax.axis_index("section")
    stages = lax.axis_size("section")
    replica = lax.axis_index(DP)
    places = [lax.axis_index(name)[None] for name in DP]
    micro = lengths.shape[0]
    gain = norm_gain
    numbers = jnp.array([stages], jnp.int32)
    meta = jnp.concatenate(
        [stage[None], lengths, places[2], replica[None], numbers, places[0], places[1]]
    )
    (wq, wo), (meta, final_row, table) = gather_weights(
        places[2], w_qkv[0], w_out[0], (meta, final_gain[None, :], rotary_table())
    )
    ticks = micro + stages - 1
    half = stages // 2
    state, turned = (), ()
    inbox = entry
    for tick in range(ticks):
        before = turned if tick in (1, half + micro) else ()
        out, *state = forward_layer(
            tick, stages - 1, micro, meta, inbox, entry, gain, table, wq, wo, before, state
        )
        if tick == 0:
            turned = turn(True, meta, out, wq, wo, turned)
        if tick == half + micro - 1:
            turned = turn(False, meta, out, wq, wo, turned)
        if tick < ticks - 1:
            pairs = [(s, s + 1) for s in range(stages - 1) if 0 <= tick - s < micro]
            inbox = lax.ppermute(out, "section", pairs)
    *stash, last = state
    count = lax.axis_size(DP[:2])
    copies = embed(count, last, final_row, positive)
    here = lax.all_to_all(copies, DP[:2], split_axis=0, concat_axis=0, tiled=True)
    here = here.reshape(count * 8, WIDE)
    there = lax.ppermute(here, "dp_2", [(0, 1), (1, 0)])
    seed = loss_seed(meta, last, final_row, here, there)
    previous = ()
    for tick in range(ticks):
        previous = backward_layer(
            tick, stages - 1, micro, meta, inbox, seed, gain, table, *turned, stash, previous
        )
        if tick < ticks - 1:
            pairs = [
                (stages - 1 - s, stages - 2 - s)
                for s in range(stages - 1)
                if 0 <= tick - s < micro
            ]
            inbox = lax.ppermute(previous[0], "section", pairs)
    return previous[1][None]


def solution(mesh):
    finer = Mesh(
        mesh.devices.reshape(mesh.shape["section"], 4, 4, 2), ("section", "dp_0", "dp_1", "dp_2")
    )
    in_specs = (
        P(DP, None),
        P("section", None),
        P("section", DP, None),
        P("section", DP, None),
        P(),
        P(DP),
        P(DP),
    )
    return jax.shard_map(
        per_device,
        mesh=finer,
        in_specs=in_specs,
        out_specs=P("section", DP, None),
        check_vma=False,
    )
```

```python
import functools

import jax
import jax.numpy as jnp
from jax import lax
from jax.experimental import pallas as pl
from jax.experimental.pallas import tpu as pltpu
from jax.sharding import Mesh
from jax.sharding import PartitionSpec as P

HEAD_DIM = 64
LEN = 48
D = 3584
QW = 896
KV = 128
XW = QW + 2 * KV
PACK = XW + QW
PAIRS = QW // 128
DP = ("dp_0", "dp_1", "dp_2")
ROPE_BASE = 1000000.0
EPS = 1e-06
SHARP = 20.0
COEF = 256.0
HALVES = 2
HALF = D // HALVES
STAGGER = 4400
EVEN = 800
F32 = jnp.float32
BF16 = jnp.bfloat16


def dot_nn(a, b):
    return lax.dot_general(a, b, (((1,), (0,)), ((), ())), preferred_element_type=F32)


def dot_nt(a, b):
    return lax.dot_general(a, b, (((1,), (1,)), ((), ())), preferred_element_type=F32)


def dot_tn(a, b):
    return lax.dot_general(a, b, (((0,), (0,)), ((), ())), preferred_element_type=F32)


def lanes(rows):
    return lax.broadcasted_iota(jnp.int32, (rows, 128), 1)


def partner(x):
    low = lax.rem(lanes(x.shape[0]), 64) < 32
    return jnp.where(low, pltpu.roll(x, 96, 1), pltpu.roll(x, 32, 1))


def paired(z):
    left = lanes(LEN) < 64
    rolled = pltpu.roll(z, 64, 1)
    pad = jnp.zeros((16, 128), BF16)
    a_left = jnp.where(left, z, 0.0).astype(BF16)
    b_right = jnp.where(left, 0.0, z).astype(BF16)
    b_left = jnp.where(left, rolled, 0.0).astype(BF16)
    a_right = jnp.where(left, 0.0, rolled).astype(BF16)
    return (
        jnp.concatenate([a_left, pad, a_right, pad], axis=0),
        jnp.concatenate([a_left, pad, b_right, pad], axis=0),
        jnp.concatenate([b_left, pad, b_right, pad], axis=0),
    )


SPANS = ((0, 3 * LEN), (3 * LEN, 4 * LEN), (4 * LEN, 7 * LEN))


def by_pair(dot, rows, blocks):
    return jnp.concatenate(
        [dot(rows[lo:hi], block) for (lo, hi), block in zip(SPANS, blocks)], axis=0
    )


def unpaired(rows, other):
    left = lanes(LEN) < 64
    s00, s01, s11 = (dot_tn(rows[lo:hi], other[lo:hi]) for lo, hi in SPANS)
    first = jnp.where(left, s00[:LEN] + s01[:LEN], 0.0)
    first += pltpu.roll(jnp.where(left, 0.0, s00[64 : 64 + LEN]), 64, 1)
    second = jnp.where(left, 0.0, s01[64 : 64 + LEN] + s11[64 : 64 + LEN])
    second += pltpu.roll(jnp.where(left, s11[:LEN], 0.0), 64, 1)
    return first + second


def half_sums(x):
    left = lanes(x.shape[0]) < 64
    low = jnp.sum(jnp.where(left, x, 0.0), axis=1, keepdims=True)
    high = jnp.sum(jnp.where(left, 0.0, x), axis=1, keepdims=True)
    return low, high, left


def probabilities(q_rows, k_blocks, length):
    scores = by_pair(dot_nt, q_rows, k_blocks) * HEAD_DIM ** (-0.5)
    live = lax.rem(lanes(scores.shape[0]), 64) < length
    weights = jnp.where(live, jnp.exp(scores), 0.0)
    low, high, left = half_sums(weights)
    return weights * jnp.where(left, 1.0 / low, 1.0 / high)


def rows_of(x_ref):
    return jnp.concatenate([x_ref[:, 128 * i : 128 * i + 128] for i in range(PAIRS)], axis=0)


def inv_rms(wide):
    return lax.rsqrt(jnp.sum(wide * wide, axis=1, keepdims=True) * (1.0 / D) + EPS)


def forward_kernel(
    tick,
    last_stage,
    micro,
    meta,
    inbox,
    entry,
    gain,
    table,
    wq,
    wo,
    *refs,
):
    out, stash_h, stash_x, last, h_v, n_v, acc_v, x_v, ctx_v, last_v, sems = refs[-11:]
    stage = meta[0]
    slot = tick - stage

    @pl.when(jnp.logical_and(slot >= 0, slot < micro))
    def _():
        length = meta[1 + slot]
        row0 = pl.multiple_of(slot * LEN, LEN)

        @pl.when(stage == 0)
        def _():
            fresh = pltpu.make_async_copy(entry.at[pl.ds(row0, LEN), :], h_v, sems.at[0])
            fresh.start()
            fresh.wait()

        @pl.when(stage != 0)
        def _():
            h_v[...] = inbox[:LEN]

        @pl.when(jnp.logical_and(meta[5] == 1, stage != last_stage))
        def _():
            pl.delay(STAGGER if tick == 0 else EVEN)

        keep_h = pltpu.make_async_copy(h_v, stash_h.at[pl.ds(row0, LEN), :], sems.at[1])
        keep_h.start()
        wide = h_v[...].astype(F32)
        n_v[...] = (wide * inv_rms(wide) * gain[...]).astype(BF16)
        acc_v[...] = dot_nn(n_v[...], wq[...])
        cosine, sine = table[0], table[1]
        for i in range(PAIRS + 1):
            part = acc_v[:, 128 * i : 128 * i + 128]
            x_v[:, 128 * i : 128 * i + 128] = (part * cosine + partner(part) * sine).astype(BF16)
        x_v[:, QW + KV :] = acc_v[:, QW + KV :].astype(BF16)
        keep_x = pltpu.make_async_copy(x_v, stash_x.at[pl.ds(row0, LEN), :], sems.at[2])
        keep_x.start()
        k_blocks = paired(x_v[:, QW : QW + KV].astype(F32))
        v_blocks = paired(x_v[:, QW + KV :].astype(F32))
        probs = probabilities(rows_of(x_v), k_blocks, length).astype(BF16)
        context = by_pair(dot_nn, probs, v_blocks).astype(BF16)
        for i in range(PAIRS):
            ctx_v[:, 128 * i : 128 * i + 128] = context[LEN * i : LEN * i + LEN]

        @pl.loop(0, HALVES)
        def _(i):
            cols = pl.ds(pl.multiple_of(i * HALF, HALF), HALF)
            branch = dot_nn(ctx_v[...], wo[:, cols])
            out[:, cols] = (h_v[:, cols].astype(F32) + branch).astype(BF16)

        @pl.when(stage == last_stage)
        def _():
            hit = lax.broadcasted_iota(jnp.int32, (LEN, D), 0) == length - 1
            row = jnp.sum(jnp.where(hit, out[...].astype(F32), 0.0), axis=0, keepdims=True)
            last_v[...] = jnp.broadcast_to(row, (8, D))
            put = pltpu.make_async_copy(last_v, last.at[slot], sems.at[3])
            put.start()
            put.wait()

        keep_h.wait()
        keep_x.wait()


def backward_kernel(
    tick,
    last_stage,
    micro,
    meta,
    inbox,
    seed,
    gain,
    table,
    wq,
    wo,
    stash_h,
    stash_x,
    *refs,
):
    out, grads, h_v, g_v, x_v, dctx_v, dx_v, dn_v, sems = refs[-9:]
    stage = meta[0]
    slot = tick - (last_stage - stage)

    def put(value, to):
        rows = pl.ds(pl.multiple_of(to * LEN, LEN), LEN)
        return pltpu.make_async_copy(value, grads.at[rows, :], sems.at[2])

    late = jnp.logical_and(slot >= 1, slot <= micro)
    if tick > 0:

        @pl.when(late)
        def _():
            put(refs[0], slot - 1).start()

    @pl.when(jnp.logical_and(slot >= 0, slot < micro))
    def _():
        length = meta[1 + slot]
        row0 = pl.multiple_of(slot * LEN, LEN)

        get_x = pltpu.make_async_copy(stash_x.at[pl.ds(row0, LEN), :], x_v, sems.at[0])
        get_h = pltpu.make_async_copy(stash_h.at[pl.ds(row0, LEN), :], h_v, sems.at[1])
        get_x.start()
        get_h.start()

        @pl.when(jnp.logical_and(meta[5] == 1, stage != 0))
        def _():
            pl.delay(STAGGER if tick == 0 else EVEN)

        @pl.when(stage == last_stage)
        def _():
            hit = lax.broadcasted_iota(jnp.int32, (LEN, D), 0) == length - 1
            row = jnp.where(lax.broadcasted_iota(jnp.int32, (8, D), 0) == slot, seed[...], 0.0)
            row = jnp.sum(row, axis=0, keepdims=True)
            g_v[...] = jnp.where(hit, jnp.broadcast_to(row, (LEN, D)), 0.0).astype(BF16)

        @pl.when(stage != last_stage)
        def _():
            g_v[...] = inbox[...]

        dctx_v[...] = jnp.zeros_like(dctx_v)

        @pl.loop(0, HALVES)
        def _(i):
            cols = pl.ds(pl.multiple_of(i * HALF, HALF), HALF)
            dctx_v[...] += dot_nn(g_v[:, cols], wo[cols, :])

        get_x.wait()
        q_rows = rows_of(x_v)
        k_blocks = paired(x_v[:, QW : QW + KV].astype(F32))
        v_blocks = paired(x_v[:, QW + KV :].astype(F32))
        probs = probabilities(q_rows, k_blocks, length)
        dctx = rows_of(dctx_v).astype(BF16)
        dvalue = unpaired(probs.astype(BF16), dctx)
        dprobs = by_pair(dot_nt, dctx, v_blocks).astype(BF16).astype(F32)
        low, high, left = half_sums(dprobs * probs)
        dscores = probs * (dprobs - jnp.where(left, low, high)) * HEAD_DIM ** (-0.5)
        dscores = dscores.astype(BF16)
        dquery = by_pair(dot_nn, dscores, k_blocks).astype(BF16).astype(F32)
        dkey = unpaired(dscores, q_rows).astype(BF16).astype(F32)
        cosine, sine = table[0], table[1]
        for i in range(PAIRS):
            part = dquery[LEN * i : LEN * i + LEN]
            dx_v[:, 128 * i : 128 * i + 128] = (part * cosine - partner(part) * sine).astype(BF16)
        dx_v[:, QW : QW + KV] = (dkey * cosine - partner(dkey) * sine).astype(BF16)
        dx_v[:, QW + KV :] = dvalue.astype(BF16)

        @pl.loop(0, HALVES)
        def _(i):
            cols = pl.ds(pl.multiple_of(i * HALF, HALF), HALF)
            dn_v[:, cols] = dot_nn(dx_v[...], wq[:, cols]).astype(BF16)

        get_h.wait()
        wide = h_v[...].astype(F32)
        scale = inv_rms(wide)
        scaled = dn_v[...].astype(F32) * gain[...]
        inner = jnp.sum(scaled * wide, axis=1, keepdims=True)
        out[...] = (
            g_v[...].astype(F32)
            + scale * scaled
            - wide * (scale * scale * scale * inner * (1.0 / D))
        ).astype(BF16)

    if tick > 0:

        @pl.when(late)
        def _():
            put(refs[0], slot - 1).wait()

    if tick == last_stage + micro - 1:

        @pl.when(slot == micro - 1)
        def _():
            put(out, slot).start()
            put(out, slot).wait()


ANY = pl.BlockSpec(memory_space=pl.ANY)
VMEM = pl.BlockSpec(memory_space=pltpu.VMEM)
SMEM = pl.BlockSpec(memory_space=pltpu.SMEM)
HBM = pl.BlockSpec(memory_space=pltpu.HBM)
LAYER_COST = pl.CostEstimate(
    flops=2 * LEN * D * (XW + QW), bytes_accessed=2 * D * (XW + QW), transcendentals=0
)
LIMIT = 8 * 1024 * 1024
LARGE = 14 * 1024 * 1024
WHOLE = 60 * 1024 * 1024
SMALL = 8 * 1024 * 1024


def forward_layer(
    tick, last_stage, micro, meta, inbox, entry, gain, table, wq, wo, before, state
):
    rows = micro * LEN
    kept = (((rows, D), BF16), ((rows, XW), BF16), ((micro, 8, D), F32))
    return pl.pallas_call(
        functools.partial(forward_kernel, tick, last_stage, micro),
        out_shape=tuple(jax.ShapeDtypeStruct(*a) for a in (((LEN, D), BF16), *kept)),
        in_specs=[SMEM, VMEM, ANY, VMEM, VMEM, VMEM, VMEM, *[ANY] * len((*before, *state))],
        out_specs=(VMEM, ANY, ANY, ANY),
        input_output_aliases={7 + len(before) + i: 1 + i for i in range(len(state))},
        scratch_shapes=[
            pltpu.VMEM((LEN, D), BF16),
            pltpu.VMEM((LEN, D), BF16),
            pltpu.VMEM((LEN, XW), F32),
            pltpu.VMEM((LEN, XW), BF16),
            pltpu.VMEM((LEN, QW), BF16),
            pltpu.VMEM((8, D), F32),
            pltpu.SemaphoreType.DMA((4,)),
        ],
        compiler_params=pltpu.CompilerParams(vmem_limit_bytes=LIMIT),
        cost_estimate=LAYER_COST,
        name="forward_layer",
    )(meta, inbox, entry, gain, table, wq, wo, *before, *state)


def backward_layer(
    tick, last_stage, micro, meta, inbox, seed, gain, table, wq_t, wo_t, stash, previous
):
    return pl.pallas_call(
        functools.partial(backward_kernel, tick, last_stage, micro),
        out_shape=(
            jax.ShapeDtypeStruct((LEN, D), BF16),
            jax.ShapeDtypeStruct((micro * LEN, D), BF16),
        ),
        in_specs=[SMEM, VMEM, VMEM, VMEM, VMEM, VMEM, VMEM, ANY, ANY, *[ANY] * len(previous)],
        out_specs=(VMEM, ANY),
        input_output_aliases={10: 1} if previous else {},
        scratch_shapes=[
            pltpu.VMEM((LEN, D), BF16),
            pltpu.VMEM((LEN, D), BF16),
            pltpu.VMEM((LEN, XW), BF16),
            pltpu.VMEM((LEN, QW), F32),
            pltpu.VMEM((LEN, XW), BF16),
            pltpu.VMEM((LEN, D), BF16),
            pltpu.SemaphoreType.DMA((3,)),
        ],
        compiler_params=pltpu.CompilerParams(vmem_limit_bytes=LIMIT),
        cost_estimate=LAYER_COST,
        name="backward_layer",
    )(meta, inbox, seed, gain, table, wq_t, wo_t, *stash, *previous)


TURN = 256


def turn_kernel(early, meta, after, wq, wo, *refs):
    del after
    wq_t, wo_t, wq_v, wo_v, sems = refs[-5:]
    half = lax.div(meta[7], 2)
    due = meta[0] >= half if early else meta[0] < half

    @pl.when(due)
    def _():
        def copies(i, slot):
            at = pl.ds(pl.multiple_of(i * TURN, TURN), TURN)
            return (
                pltpu.make_async_copy(wq_v.at[slot], wq_t.at[:, at], sems.at[0, slot]),
                pltpu.make_async_copy(wo_v.at[slot], wo_t.at[at, :], sems.at[1, slot]),
            )

        @pl.loop(0, D // TURN)
        def _(i):
            slot = lax.rem(i, 2)
            at = pl.ds(pl.multiple_of(i * TURN, TURN), TURN)

            @pl.when(i >= 2)
            def _():
                for copy in copies(i - 2, slot):
                    copy.wait()

            wq_v[slot] = wq[at, :].T
            wo_v[slot] = wo[:, at].T
            for copy in copies(i, slot):
                copy.start()

        for i in (D // TURN - 2, D // TURN - 1):
            for copy in copies(i, i % 2):
                copy.wait()


def turn(early, meta, after, wq, wo, turned):
    return pl.pallas_call(
        functools.partial(turn_kernel, early),
        out_shape=(jax.ShapeDtypeStruct((XW, D), BF16), jax.ShapeDtypeStruct((D, QW), BF16)),
        in_specs=[SMEM, ANY, VMEM, VMEM, *[ANY] * len(turned)],
        out_specs=(ANY, ANY),
        input_output_aliases={4 + i: i for i in range(len(turned))},
        scratch_shapes=[
            pltpu.VMEM((2, XW, TURN), BF16),
            pltpu.VMEM((2, TURN, QW), BF16),
            pltpu.SemaphoreType.DMA((2, 2)),
        ],
        compiler_params=pltpu.CompilerParams(vmem_limit_bytes=LIMIT),
        cost_estimate=pl.CostEstimate(flops=0, bytes_accessed=4 * D * (XW + QW), transcendentals=0),
        name="turn",
    )(meta, after, wq, wo, *turned)


SIDE = PACK // 2


def pack_kernel(core, w_qkv, w_out, keep, give, w_v, x_v, sems):
    first = pltpu.make_async_copy(w_out, w_v, sems.at[0])
    second = pltpu.make_async_copy(w_qkv, x_v, sems.at[1])
    first.start()
    second.start()
    first.wait()
    pieces = [w_v[:, QW * j : QW * j + QW].astype(F32) for j in range(D // QW)]
    low = jnp.concatenate(pieces, axis=0).astype(BF16)
    second.wait()

    def fill(left, right):
        left[...] = x_v[:, :SIDE]
        right[:, : XW - SIDE] = x_v[:, SIDE:]
        right[:, XW - SIDE :] = low

    @pl.when(core[0] == 0)
    def _():
        fill(keep, give)

    @pl.when(core[0] == 1)
    def _():
        fill(give, keep)


def pack(core, w_qkv, w_out):
    side = jax.ShapeDtypeStruct((w_qkv.shape[0], SIDE), BF16)
    return pl.pallas_call(
        pack_kernel,
        out_shape=(side, side),
        in_specs=[SMEM, HBM, HBM],
        out_specs=(VMEM, VMEM),
        scratch_shapes=[
            pltpu.VMEM(w_out.shape, BF16),
            pltpu.VMEM(w_qkv.shape, BF16),
            pltpu.SemaphoreType.DMA((2,)),
        ],
        compiler_params=pltpu.CompilerParams(vmem_limit_bytes=WHOLE),
        name="pack",
    )(core, w_qkv, w_out)


def unpack_kernel(meta, *refs):
    count = (len(refs) - 4) // 2
    mine, theirs = refs[:count], refs[count : 2 * count]
    wq, wo, part_v, sems = refs[2 * count :]
    parts = D // QW
    length = D // 32
    short = length // parts
    x0, y0, core = meta[8], meta[9], meta[5]

    def offset(step):
        return jnp.where(step == 1, 3, jnp.where(step == 2, 1, jnp.where(step == 3, 2, 0)))

    def put(blocks, color):
        for n in range(8):
            block = blocks[n]
            far, other = n // 2, n % 2

            @pl.loop(0, 4)
            def _(near):
                first = lax.rem(offset(near) + (y0 if color == 0 else x0), 4)
                second = lax.rem((0, 3, 1, 2)[far] + (x0 if color == 0 else y0), 4)
                x, y = (second, first) if color == 0 else (first, second)
                shard = x * 8 + y * 2 + (color if other == 0 else 1 - color)
                rows = pl.ds(pl.multiple_of(shard * length, length), length)
                if color == 0:
                    pltpu.make_async_copy(
                        block.at[near], wq.at[rows, pl.ds(0, SIDE)], sems.at[0]
                    ).start()
                else:
                    pltpu.make_async_copy(
                        block.at[near, :, pl.ds(0, XW - SIDE)],
                        wq.at[rows, pl.ds(SIDE, XW - SIDE)],
                        sems.at[0],
                    ).start()
                    pltpu.make_async_copy(
                        block.at[near, :, pl.ds(XW - SIDE, QW)], part_v.at[rows, :], sems.at[1]
                    ).start()

    @pl.when(core == 0)
    def _():
        put(theirs, 1)
        put(mine, 0)

    @pl.when(core == 1)
    def _():
        put(mine, 1)
        put(theirs, 0)

    pltpu.make_async_copy(part_v, part_v, sems.at[1]).wait()

    @pl.loop(0, 8)
    def _(i):
        blocks = []
        for r in range(4):
            at = pl.ds(pl.multiple_of((4 * i + r) * length, length), length)
            blocks.append(part_v[at, :].astype(F32))
        to = pl.ds(pl.multiple_of(i * length, length), length)
        for j in range(parts):
            cut = [block[short * j : short * j + short] for block in blocks]
            wo[to, QW * j : QW * j + QW] = jnp.concatenate(cut, axis=0).astype(BF16)

    pltpu.make_async_copy(wq, wq, sems.at[0]).wait()


def unpack(meta, mine, theirs):
    return pl.pallas_call(
        unpack_kernel,
        out_shape=(jax.ShapeDtypeStruct((D, XW), BF16), jax.ShapeDtypeStruct((QW, D), BF16)),
        in_specs=[SMEM, *[ANY] * (len(mine) + len(theirs))],
        out_specs=(VMEM, VMEM),
        scratch_shapes=[pltpu.VMEM((D, QW), BF16), pltpu.SemaphoreType.DMA((2,))],
        compiler_params=pltpu.CompilerParams(vmem_limit_bytes=LARGE),
        name="unpack",
    )(meta, *mine, *theirs)


def ring_step(value, second, step):
    pairs = []
    for x in range(4):
        for y in range(4):
            for core in range(2):
                along_y = (core == 0) != second
                to = (x, (y + step) % 4) if along_y else ((x + step) % 4, y)
                pairs.append((x * 8 + y * 2 + core, to[0] * 8 + to[1] * 2 + core))
    return lax.ppermute(value, DP, pairs)


def swap_cores(value):
    return lax.ppermute(value, "dp_2", [(0, 1), (1, 0)])


def join_kernel(*refs):
    *parts, out, sems = refs
    copies = [
        pltpu.make_async_copy(part, out.at[n], sems.at[n]) for n, part in enumerate(parts)
    ]
    for copy in copies:
        copy.start()
    for copy in copies:
        copy.wait()


def join(*parts):
    return pl.pallas_call(
        join_kernel,
        out_shape=jax.ShapeDtypeStruct((len(parts), *parts[0].shape), parts[0].dtype),
        in_specs=[ANY] * len(parts),
        out_specs=ANY,
        scratch_shapes=[pltpu.SemaphoreType.DMA((len(parts),))],
        compiler_params=pltpu.CompilerParams(vmem_limit_bytes=1024 * 1024),
        name="join",
    )(*parts)


def gather_weights(core, w_qkv, w_out, others):
    keep, give = pack(core, w_qkv, w_out)
    keep, got, others = lax.optimization_barrier((keep, swap_cores(give), others))
    meta = others[0]
    lines = []
    for value, forward in ((keep, 1), (got, -1)):
        before = ring_step(value, False, 1)
        after = ring_step(value, False, -1)
        across = ring_step(before if forward == 1 else after, False, forward)
        lines.append(join(value, before, after, across))
    mine = [None] * 8
    for n, (line, forward) in enumerate(zip(lines, (1, -1))):
        before = ring_step(line, True, 1)
        after = ring_step(line, True, -1)
        across = ring_step(before if forward == 1 else after, True, forward)
        mine[n::2] = [line, before, after, across]
    return unpack(meta, mine, [swap_cores(value) for value in mine]), others


WIDE = HALF + 128


def pooled_rows(last):
    return jnp.concatenate([last[j, 0:1, :] for j in (0, 2, 1, 3)], axis=0)


def embed_kernel(last, final_gain, labels, out):
    rows = pooled_rows(last)
    pooled = rows * inv_rms(rows) * final_gain[...]
    unit = pooled * lax.rsqrt(jnp.sum(pooled * pooled, axis=1, keepdims=True))
    halves = jnp.concatenate([unit[:, :HALF], unit[:, HALF:]], axis=0).astype(BF16)
    which = lax.broadcasted_iota(jnp.int32, (8, 128), 0)
    label = jnp.where(which == 0, labels[0], jnp.where(which == 1, labels[1], 0))
    label = label.astype(F32).astype(BF16)
    for i in range(out.shape[0]):
        out[i, :, :HALF] = halves
        out[i, :, HALF:] = label


def embed(count, last, final_gain, labels):
    return pl.pallas_call(
        embed_kernel,
        out_shape=jax.ShapeDtypeStruct((count, 8, WIDE), BF16),
        in_specs=[VMEM, VMEM, SMEM],
        out_specs=VMEM,
        compiler_params=pltpu.CompilerParams(vmem_limit_bytes=LIMIT),
        name="embed",
    )(last, final_gain, labels)


def loss_kernel(meta, last, final_gain, here, there, seed):
    everyone = jnp.concatenate([here[...], there[...]], axis=0)
    count = everyone.shape[0]
    emb = everyone[:, :HALF]
    label = everyone[:, HALF:].astype(F32)[:, 0:1].astype(jnp.int32)
    scores = dot_nt(emb, emb)
    scores = scores + pltpu.roll(pltpu.roll(scores, count - 4, 0), count - 4, 1)
    row = lax.rem(lax.broadcasted_iota(jnp.int32, (count, count), 0), 8)
    col = lax.broadcasted_iota(jnp.int32, (count, count), 1)
    doc = jnp.logical_and(lax.rem(col, 8) >= 2, lax.rem(col, 8) < 4)
    valid = jnp.logical_and(row < 2, doc)
    weights = jnp.where(valid, jnp.exp(scores * SHARP), 0.0)
    total = jnp.sum(weights, axis=1, keepdims=True)
    prob = weights / jnp.where(row[:, :1] < 2, total, 1.0)
    owner = lax.div(label, 2)
    away = (lax.rem(owner, 2) != meta[5]).astype(jnp.int32)
    target = away * (count // 2) + lax.div(owner, 2) * 8 + 2 + lax.rem(label, 2)
    coef = jnp.where(valid, (prob - (col == target).astype(F32)) * (COEF * SHARP), 0.0)
    both = coef + coef.T
    mine = lax.broadcasted_iota(jnp.int32, (8, count), 0)
    pick = lax.broadcasted_iota(jnp.int32, (8, count), 1) == lax.div(meta[6], 2) * 8 + mine
    own = lax.dot_general(
        pick.astype(F32),
        both,
        (((1,), (0,)), ((), ())),
        precision=lax.Precision.HIGHEST,
        preferred_element_type=F32,
    )[:4]
    own = jnp.concatenate([own, pltpu.roll(own, 4, 1)], axis=0)
    top = own.astype(BF16)
    rest = own - top.astype(F32)
    mid = rest.astype(BF16)
    low = (rest - mid.astype(F32)).astype(BF16)
    split = dot_nn(jnp.concatenate([top, mid, low, low], axis=0), emb)
    grad = split[:8] + (split[8:16] + split[16:24])
    grad = jnp.concatenate([grad[:4], grad[4:]], axis=1)
    rows = pooled_rows(last)
    gain = final_gain[...]
    scale = inv_rms(rows)
    pooled = rows * scale * gain
    norm = lax.rsqrt(jnp.sum(pooled * pooled, axis=1, keepdims=True))
    unit = pooled * norm
    dpooled = norm * (grad - unit * jnp.sum(grad * unit, axis=1, keepdims=True))
    scaled = dpooled * gain
    inner = jnp.sum(scaled * rows, axis=1, keepdims=True)
    drow = scale * scaled - rows * (scale * scale * scale * inner * (1.0 / D))
    drow = drow.astype(BF16).astype(F32)
    seed[...] = jnp.concatenate(
        [drow[0:1], drow[2:3], drow[1:2], drow[3:4], jnp.zeros((4, D), F32)], axis=0
    )


def loss_seed(meta, last, final_gain, here, there):
    return pl.pallas_call(
        loss_kernel,
        out_shape=jax.ShapeDtypeStruct((8, D), F32),
        in_specs=[SMEM, VMEM, VMEM, VMEM, VMEM],
        out_specs=VMEM,
        compiler_params=pltpu.CompilerParams(vmem_limit_bytes=LIMIT),
        name="loss_seed",
    )(meta, last, final_gain, here, there)


def rotary_table():
    lane = jnp.arange(128, dtype=jnp.int32)
    frequency = ROPE_BASE ** (-(lane % 32).astype(F32) * (2.0 / HEAD_DIM))
    angles = jnp.arange(LEN, dtype=F32)[:, None] * frequency[None, :]
    sign = jnp.where(lane % 64 < 32, -1.0, 1.0)
    return jnp.stack([jnp.cos(angles), jnp.sin(angles) * sign])


def per_device(entry, norm_gain, w_qkv, w_out, final_gain, lengths, positive):
    stage = lax.axis_index("section")
    stages = lax.axis_size("section")
    replica = lax.axis_index(DP)
    places = [lax.axis_index(name)[None] for name in DP]
    micro = lengths.shape[0]
    gain = norm_gain
    numbers = jnp.array([stages], jnp.int32)
    meta = jnp.concatenate(
        [stage[None], lengths, places[2], replica[None], numbers, places[0], places[1]]
    )
    (wq, wo), (meta, final_row, table) = gather_weights(
        places[2], w_qkv[0], w_out[0], (meta, final_gain[None, :], rotary_table())
    )
    ticks = micro + stages - 1
    half = stages // 2
    state, turned = (), ()
    inbox = entry
    for tick in range(ticks):
        before = turned if tick in (1, half + micro) else ()
        out, *state = forward_layer(
            tick, stages - 1, micro, meta, inbox, entry, gain, table, wq, wo, before, state
        )
        if tick == 0:
            turned = turn(True, meta, out, wq, wo, turned)
        if tick == half + micro - 1:
            turned = turn(False, meta, out, wq, wo, turned)
        if tick < ticks - 1:
            pairs = [(s, s + 1) for s in range(stages - 1) if 0 <= tick - s < micro]
            inbox = lax.ppermute(out, "section", pairs)
    *stash, last = state
    count = lax.axis_size(DP[:2])
    copies = embed(count, last, final_row, positive)
    here = lax.all_to_all(copies, DP[:2], split_axis=0, concat_axis=0, tiled=True)
    here = here.reshape(count * 8, WIDE)
    there = lax.ppermute(here, "dp_2", [(0, 1), (1, 0)])
    seed = loss_seed(meta, last, final_row, here, there)
    previous = ()
    for tick in range(ticks):
        previous = backward_layer(
            tick, stages - 1, micro, meta, inbox, seed, gain, table, *turned, stash, previous
        )
        if tick < ticks - 1:
            pairs = [
                (stages - 1 - s, stages - 2 - s)
                for s in range(stages - 1)
                if 0 <= tick - s < micro
            ]
            inbox = lax.ppermute(previous[0], "section", pairs)
    return previous[1][None]


def solution(mesh):
    finer = Mesh(
        mesh.devices.reshape(mesh.shape["section"], 4, 4, 2), ("section", "dp_0", "dp_1", "dp_2")
    )
    in_specs = (
        P(DP, None),
        P("section", None),
        P("section", DP, None),
        P("section", DP, None),
        P(),
        P(DP),
        P(DP),
    )
    return jax.shard_map(
        per_device,
        mesh=finer,
        in_specs=in_specs,
        out_specs=P("section", DP, None),
        check_vma=False,
    )
```

```python
import functools

import jax
import jax.numpy as jnp
from jax import lax
from jax.experimental import pallas as pl
from jax.experimental.pallas import tpu as pltpu
from jax.sharding import Mesh
from jax.sharding import PartitionSpec as P

HEAD_DIM = 64
LEN = 48
D = 3584
QW = 896
KV = 128
XW = QW + 2 * KV
PACK = XW + QW
PAIRS = QW // 128
DP = ("dp_0", "dp_1", "dp_2")
ROPE_BASE = 1000000.0
EPS = 1e-06
SHARP = 20.0
COEF = 256.0
HALVES = 2
HALF = D // HALVES
STAGGER = 5000
EVEN = 850
F32 = jnp.float32
BF16 = jnp.bfloat16


def dot_nn(a, b):
    return lax.dot_general(a, b, (((1,), (0,)), ((), ())), preferred_element_type=F32)


def dot_nt(a, b):
    return lax.dot_general(a, b, (((1,), (1,)), ((), ())), preferred_element_type=F32)


def dot_tn(a, b):
    return lax.dot_general(a, b, (((0,), (0,)), ((), ())), preferred_element_type=F32)


def lanes(rows):
    return lax.broadcasted_iota(jnp.int32, (rows, 128), 1)


def partner(x):
    low = lax.rem(lanes(x.shape[0]), 64) < 32
    return jnp.where(low, pltpu.roll(x, 96, 1), pltpu.roll(x, 32, 1))


def paired(z):
    left = lanes(LEN) < 64
    rolled = pltpu.roll(z, 64, 1)
    pad = jnp.zeros((16, 128), BF16)
    a_left = jnp.where(left, z, 0.0).astype(BF16)
    b_right = jnp.where(left, 0.0, z).astype(BF16)
    b_left = jnp.where(left, rolled, 0.0).astype(BF16)
    a_right = jnp.where(left, 0.0, rolled).astype(BF16)
    return (
        jnp.concatenate([a_left, pad, a_right, pad], axis=0),
        jnp.concatenate([a_left, pad, b_right, pad], axis=0),
        jnp.concatenate([b_left, pad, b_right, pad], axis=0),
    )


SPANS = ((0, 3 * LEN), (3 * LEN, 4 * LEN), (4 * LEN, 7 * LEN))


def by_pair(dot, rows, blocks):
    return jnp.concatenate(
        [dot(rows[lo:hi], block) for (lo, hi), block in zip(SPANS, blocks)], axis=0
    )


def unpaired(rows, other):
    left = lanes(LEN) < 64
    s00, s01, s11 = (dot_tn(rows[lo:hi], other[lo:hi]) for lo, hi in SPANS)
    first = jnp.where(left, s00[:LEN] + s01[:LEN], 0.0)
    first += pltpu.roll(jnp.where(left, 0.0, s00[64 : 64 + LEN]), 64, 1)
    second = jnp.where(left, 0.0, s01[64 : 64 + LEN] + s11[64 : 64 + LEN])
    second += pltpu.roll(jnp.where(left, s11[:LEN], 0.0), 64, 1)
    return first + second


def half_sums(x):
    left = lanes(x.shape[0]) < 64
    low = jnp.sum(jnp.where(left, x, 0.0), axis=1, keepdims=True)
    high = jnp.sum(jnp.where(left, 0.0, x), axis=1, keepdims=True)
    return low, high, left


def probabilities(q_rows, k_blocks, length):
    scores = by_pair(dot_nt, q_rows, k_blocks) * HEAD_DIM ** (-0.5)
    live = lax.rem(lanes(scores.shape[0]), 64) < length
    weights = jnp.where(live, jnp.exp(scores), 0.0)
    low, high, left = half_sums(weights)
    return weights * jnp.where(left, 1.0 / low, 1.0 / high)


def rows_of(x_ref):
    return jnp.concatenate([x_ref[:, 128 * i : 128 * i + 128] for i in range(PAIRS)], axis=0)


def inv_rms(wide):
    return lax.rsqrt(jnp.sum(wide * wide, axis=1, keepdims=True) * (1.0 / D) + EPS)


def forward_kernel(
    tick,
    last_stage,
    micro,
    meta,
    inbox,
    entry,
    gain,
    table,
    wq,
    wo,
    *refs,
):
    out, stash_h, stash_x, last, h_v, n_v, acc_v, x_v, ctx_v, last_v, sems = refs[-11:]
    stage = meta[0]
    slot = tick - stage

    @pl.when(jnp.logical_and(slot >= 0, slot < micro))
    def _():
        length = meta[1 + slot]
        row0 = pl.multiple_of(slot * LEN, LEN)

        @pl.when(stage == 0)
        def _():
            fresh = pltpu.make_async_copy(entry.at[pl.ds(row0, LEN), :], h_v, sems.at[0])
            fresh.start()
            fresh.wait()

        @pl.when(stage != 0)
        def _():
            h_v[...] = inbox[:LEN]

        @pl.when(jnp.logical_and(meta[5] == 1, stage != last_stage))
        def _():
            pl.delay(STAGGER if tick == 0 else EVEN)

        keep_h = pltpu.make_async_copy(h_v, stash_h.at[pl.ds(row0, LEN), :], sems.at[1])
        keep_h.start()
        wide = h_v[...].astype(F32)
        n_v[...] = (wide * inv_rms(wide) * gain[...]).astype(BF16)
        acc_v[...] = jnp.zeros_like(acc_v)

        @pl.loop(0, HALVES)
        def _(i):
            cols = pl.ds(pl.multiple_of(i * HALF, HALF), HALF)
            acc_v[...] += dot_nn(n_v[:, cols], wq[cols, :])

        cosine, sine = table[0], table[1]
        for i in range(PAIRS + 1):
            part = acc_v[:, 128 * i : 128 * i + 128]
            x_v[:, 128 * i : 128 * i + 128] = (part * cosine + partner(part) * sine).astype(BF16)
        x_v[:, QW + KV :] = acc_v[:, QW + KV :].astype(BF16)
        keep_x = pltpu.make_async_copy(x_v, stash_x.at[pl.ds(row0, LEN), :], sems.at[2])
        keep_x.start()
        k_blocks = paired(x_v[:, QW : QW + KV].astype(F32))
        v_blocks = paired(x_v[:, QW + KV :].astype(F32))
        probs = probabilities(rows_of(x_v), k_blocks, length).astype(BF16)
        context = by_pair(dot_nn, probs, v_blocks).astype(BF16)
        for i in range(PAIRS):
            ctx_v[:, 128 * i : 128 * i + 128] = context[LEN * i : LEN * i + LEN]

        @pl.loop(0, HALVES)
        def _(i):
            cols = pl.ds(pl.multiple_of(i * HALF, HALF), HALF)
            branch = dot_nn(ctx_v[...], wo[:, cols])
            out[:, cols] = (h_v[:, cols].astype(F32) + branch).astype(BF16)

        @pl.when(stage == last_stage)
        def _():
            hit = lax.broadcasted_iota(jnp.int32, (LEN, D), 0) == length - 1
            row = jnp.sum(jnp.where(hit, out[...].astype(F32), 0.0), axis=0, keepdims=True)
            last_v[...] = jnp.broadcast_to(row, (8, D))
            put = pltpu.make_async_copy(last_v, last.at[slot], sems.at[3])
            put.start()
            put.wait()

        keep_h.wait()
        keep_x.wait()


def backward_kernel(
    tick,
    last_stage,
    micro,
    meta,
    inbox,
    seed,
    gain,
    table,
    wq,
    wo,
    stash_h,
    stash_x,
    *refs,
):
    out, grads, h_v, g_v, x_v, dctx_v, dx_v, dn_v, sems = refs[-9:]
    stage = meta[0]
    slot = tick - (last_stage - stage)

    def put(value, to):
        rows = pl.ds(pl.multiple_of(to * LEN, LEN), LEN)
        return pltpu.make_async_copy(value, grads.at[rows, :], sems.at[2])

    late = jnp.logical_and(slot >= 1, slot <= micro)
    if tick > 0:

        @pl.when(late)
        def _():
            put(refs[0], slot - 1).start()

    @pl.when(jnp.logical_and(slot >= 0, slot < micro))
    def _():
        length = meta[1 + slot]
        row0 = pl.multiple_of(slot * LEN, LEN)

        get_x = pltpu.make_async_copy(stash_x.at[pl.ds(row0, LEN), :], x_v, sems.at[0])
        get_h = pltpu.make_async_copy(stash_h.at[pl.ds(row0, LEN), :], h_v, sems.at[1])
        get_x.start()
        get_h.start()

        @pl.when(jnp.logical_and(meta[5] == 1, stage != 0))
        def _():
            pl.delay(STAGGER if tick == 0 else EVEN)

        @pl.when(stage == last_stage)
        def _():
            hit = lax.broadcasted_iota(jnp.int32, (LEN, D), 0) == length - 1
            row = jnp.where(lax.broadcasted_iota(jnp.int32, (8, D), 0) == slot, seed[...], 0.0)
            row = jnp.sum(row, axis=0, keepdims=True)
            g_v[...] = jnp.where(hit, jnp.broadcast_to(row, (LEN, D)), 0.0).astype(BF16)

        @pl.when(stage != last_stage)
        def _():
            g_v[...] = inbox[...]

        dctx_v[...] = jnp.zeros_like(dctx_v)

        @pl.loop(0, HALVES)
        def _(i):
            cols = pl.ds(pl.multiple_of(i * HALF, HALF), HALF)
            dctx_v[...] += dot_nn(g_v[:, cols], wo[cols, :])

        get_x.wait()
        q_rows = rows_of(x_v)
        k_blocks = paired(x_v[:, QW : QW + KV].astype(F32))
        v_blocks = paired(x_v[:, QW + KV :].astype(F32))
        probs = probabilities(q_rows, k_blocks, length)
        dctx = rows_of(dctx_v).astype(BF16)
        dvalue = unpaired(probs.astype(BF16), dctx)
        dprobs = by_pair(dot_nt, dctx, v_blocks).astype(BF16).astype(F32)
        low, high, left = half_sums(dprobs * probs)
        dscores = probs * (dprobs - jnp.where(left, low, high)) * HEAD_DIM ** (-0.5)
        dscores = dscores.astype(BF16)
        dquery = by_pair(dot_nn, dscores, k_blocks).astype(BF16).astype(F32)
        dkey = unpaired(dscores, q_rows).astype(BF16).astype(F32)
        cosine, sine = table[0], table[1]
        for i in range(PAIRS):
            part = dquery[LEN * i : LEN * i + LEN]
            dx_v[:, 128 * i : 128 * i + 128] = (part * cosine - partner(part) * sine).astype(BF16)
        dx_v[:, QW : QW + KV] = (dkey * cosine - partner(dkey) * sine).astype(BF16)
        dx_v[:, QW + KV :] = dvalue.astype(BF16)

        @pl.loop(0, HALVES)
        def _(i):
            cols = pl.ds(pl.multiple_of(i * HALF, HALF), HALF)
            dn_v[:, cols] = dot_nn(dx_v[...], wq[:, cols]).astype(BF16)

        get_h.wait()
        wide = h_v[...].astype(F32)
        scale = inv_rms(wide)
        scaled = dn_v[...].astype(F32) * gain[...]
        inner = jnp.sum(scaled * wide, axis=1, keepdims=True)
        out[...] = (
            g_v[...].astype(F32)
            + scale * scaled
            - wide * (scale * scale * scale * inner * (1.0 / D))
        ).astype(BF16)

    if tick > 0:

        @pl.when(late)
        def _():
            put(refs[0], slot - 1).wait()

    if tick == last_stage + micro - 1:

        @pl.when(slot == micro - 1)
        def _():
            put(out, slot).start()
            put(out, slot).wait()


ANY = pl.BlockSpec(memory_space=pl.ANY)
VMEM = pl.BlockSpec(memory_space=pltpu.VMEM)
SMEM = pl.BlockSpec(memory_space=pltpu.SMEM)
HBM = pl.BlockSpec(memory_space=pltpu.HBM)
LAYER_COST = pl.CostEstimate(
    flops=2 * LEN * D * (XW + QW), bytes_accessed=2 * D * (XW + QW), transcendentals=0
)
LIMIT = 8 * 1024 * 1024
LARGE = 14 * 1024 * 1024
WHOLE = 60 * 1024 * 1024
SMALL = 8 * 1024 * 1024


def forward_layer(
    tick, last_stage, micro, meta, inbox, entry, gain, table, wq, wo, before, state
):
    rows = micro * LEN
    kept = (((rows, D), BF16), ((rows, XW), BF16), ((micro, 8, D), F32))
    return pl.pallas_call(
        functools.partial(forward_kernel, tick, last_stage, micro),
        out_shape=tuple(jax.ShapeDtypeStruct(*a) for a in (((LEN, D), BF16), *kept)),
        in_specs=[SMEM, VMEM, ANY, VMEM, VMEM, VMEM, VMEM, *[ANY] * len((*before, *state))],
        out_specs=(VMEM, ANY, ANY, ANY),
        input_output_aliases={7 + len(before) + i: 1 + i for i in range(len(state))},
        scratch_shapes=[
            pltpu.VMEM((LEN, D), BF16),
            pltpu.VMEM((LEN, D), BF16),
            pltpu.VMEM((LEN, XW), F32),
            pltpu.VMEM((LEN, XW), BF16),
            pltpu.VMEM((LEN, QW), BF16),
            pltpu.VMEM((8, D), F32),
            pltpu.SemaphoreType.DMA((4,)),
        ],
        compiler_params=pltpu.CompilerParams(vmem_limit_bytes=LIMIT),
        cost_estimate=LAYER_COST,
        name="forward_layer",
    )(meta, inbox, entry, gain, table, wq, wo, *before, *state)


def backward_layer(
    tick, last_stage, micro, meta, inbox, seed, gain, table, wq_t, wo_t, stash, previous
):
    return pl.pallas_call(
        functools.partial(backward_kernel, tick, last_stage, micro),
        out_shape=(
            jax.ShapeDtypeStruct((LEN, D), BF16),
            jax.ShapeDtypeStruct((micro * LEN, D), BF16),
        ),
        in_specs=[SMEM, VMEM, VMEM, VMEM, VMEM, VMEM, VMEM, ANY, ANY, *[ANY] * len(previous)],
        out_specs=(VMEM, ANY),
        input_output_aliases={10: 1} if previous else {},
        scratch_shapes=[
            pltpu.VMEM((LEN, D), BF16),
            pltpu.VMEM((LEN, D), BF16),
            pltpu.VMEM((LEN, XW), BF16),
            pltpu.VMEM((LEN, QW), F32),
            pltpu.VMEM((LEN, XW), BF16),
            pltpu.VMEM((LEN, D), BF16),
            pltpu.SemaphoreType.DMA((3,)),
        ],
        compiler_params=pltpu.CompilerParams(vmem_limit_bytes=LIMIT),
        cost_estimate=LAYER_COST,
        name="backward_layer",
    )(meta, inbox, seed, gain, table, wq_t, wo_t, *stash, *previous)


TURN = 256


def turn_kernel(early, meta, after, wq, wo, *refs):
    del after
    wq_t, wo_t, wq_v, wo_v, sems = refs[-5:]
    half = lax.div(meta[7], 2)
    due = meta[0] >= half if early else meta[0] < half

    @pl.when(due)
    def _():
        def copies(i, slot):
            at = pl.ds(pl.multiple_of(i * TURN, TURN), TURN)
            return (
                pltpu.make_async_copy(wq_v.at[slot], wq_t.at[:, at], sems.at[0, slot]),
                pltpu.make_async_copy(wo_v.at[slot], wo_t.at[at, :], sems.at[1, slot]),
            )

        @pl.loop(0, D // TURN)
        def _(i):
            slot = lax.rem(i, 2)
            at = pl.ds(pl.multiple_of(i * TURN, TURN), TURN)

            @pl.when(i >= 2)
            def _():
                for copy in copies(i - 2, slot):
                    copy.wait()

            wq_v[slot] = wq[at, :].T
            wo_v[slot] = wo[:, at].T
            for copy in copies(i, slot):
                copy.start()

        for i in (D // TURN - 2, D // TURN - 1):
            for copy in copies(i, i % 2):
                copy.wait()


def turn(early, meta, after, wq, wo, turned):
    return pl.pallas_call(
        functools.partial(turn_kernel, early),
        out_shape=(jax.ShapeDtypeStruct((XW, D), BF16), jax.ShapeDtypeStruct((D, QW), BF16)),
        in_specs=[SMEM, ANY, VMEM, VMEM, *[ANY] * len(turned)],
        out_specs=(ANY, ANY),
        input_output_aliases={4 + i: i for i in range(len(turned))},
        scratch_shapes=[
            pltpu.VMEM((2, XW, TURN), BF16),
            pltpu.VMEM((2, TURN, QW), BF16),
            pltpu.SemaphoreType.DMA((2, 2)),
        ],
        compiler_params=pltpu.CompilerParams(vmem_limit_bytes=LIMIT),
        cost_estimate=pl.CostEstimate(flops=0, bytes_accessed=4 * D * (XW + QW), transcendentals=0),
        name="turn",
    )(meta, after, wq, wo, *turned)


SIDE = PACK // 2


def pack_kernel(core, w_qkv, w_out, keep, give, w_v, x_v, sems):
    first = pltpu.make_async_copy(w_out, w_v, sems.at[0])
    second = pltpu.make_async_copy(w_qkv, x_v, sems.at[1])
    first.start()
    second.start()
    first.wait()
    pieces = [w_v[:, QW * j : QW * j + QW].astype(F32) for j in range(D // QW)]
    low = jnp.concatenate(pieces, axis=0).astype(BF16)
    second.wait()

    def fill(left, right):
        left[...] = x_v[:, :SIDE]
        right[:, : XW - SIDE] = x_v[:, SIDE:]
        right[:, XW - SIDE :] = low

    @pl.when(core[0] == 0)
    def _():
        fill(keep, give)

    @pl.when(core[0] == 1)
    def _():
        fill(give, keep)


def pack(core, w_qkv, w_out):
    side = jax.ShapeDtypeStruct((w_qkv.shape[0], SIDE), BF16)
    return pl.pallas_call(
        pack_kernel,
        out_shape=(side, side),
        in_specs=[SMEM, HBM, HBM],
        out_specs=(VMEM, VMEM),
        scratch_shapes=[
            pltpu.VMEM(w_out.shape, BF16),
            pltpu.VMEM(w_qkv.shape, BF16),
            pltpu.SemaphoreType.DMA((2,)),
        ],
        compiler_params=pltpu.CompilerParams(vmem_limit_bytes=WHOLE),
        name="pack",
    )(core, w_qkv, w_out)


def unpack_kernel(meta, *refs):
    count = (len(refs) - 4) // 2
    mine, theirs = refs[:count], refs[count : 2 * count]
    wq, wo, part_v, sems = refs[2 * count :]
    parts = D // QW
    length = D // 32
    short = length // parts
    x0, y0, core = meta[8], meta[9], meta[5]

    def offset(step):
        return jnp.where(step == 1, 3, jnp.where(step == 2, 1, jnp.where(step == 3, 2, 0)))

    def put(blocks, color):
        for n in range(8):
            block = blocks[n]
            far, other = n // 2, n % 2

            @pl.loop(0, 4)
            def _(near):
                first = lax.rem(offset(near) + (y0 if color == 0 else x0), 4)
                second = lax.rem((0, 3, 1, 2)[far] + (x0 if color == 0 else y0), 4)
                x, y = (second, first) if color == 0 else (first, second)
                shard = x * 8 + y * 2 + (color if other == 0 else 1 - color)
                rows = pl.ds(pl.multiple_of(shard * length, length), length)
                if color == 0:
                    pltpu.make_async_copy(
                        block.at[near], wq.at[rows, pl.ds(0, SIDE)], sems.at[0]
                    ).start()
                else:
                    pltpu.make_async_copy(
                        block.at[near, :, pl.ds(0, XW - SIDE)],
                        wq.at[rows, pl.ds(SIDE, XW - SIDE)],
                        sems.at[0],
                    ).start()
                    pltpu.make_async_copy(
                        block.at[near, :, pl.ds(XW - SIDE, QW)], part_v.at[rows, :], sems.at[1]
                    ).start()

    @pl.when(core == 0)
    def _():
        put(theirs, 1)
        put(mine, 0)

    @pl.when(core == 1)
    def _():
        put(mine, 1)
        put(theirs, 0)

    pltpu.make_async_copy(part_v, part_v, sems.at[1]).wait()

    @pl.loop(0, 8)
    def _(i):
        blocks = []
        for r in range(4):
            at = pl.ds(pl.multiple_of((4 * i + r) * length, length), length)
            blocks.append(part_v[at, :].astype(F32))
        to = pl.ds(pl.multiple_of(i * length, length), length)
        for j in range(parts):
            cut = [block[short * j : short * j + short] for block in blocks]
            wo[to, QW * j : QW * j + QW] = jnp.concatenate(cut, axis=0).astype(BF16)

    pltpu.make_async_copy(wq, wq, sems.at[0]).wait()


def unpack(meta, mine, theirs):
    return pl.pallas_call(
        unpack_kernel,
        out_shape=(jax.ShapeDtypeStruct((D, XW), BF16), jax.ShapeDtypeStruct((QW, D), BF16)),
        in_specs=[SMEM, *[ANY] * (len(mine) + len(theirs))],
        out_specs=(VMEM, VMEM),
        scratch_shapes=[pltpu.VMEM((D, QW), BF16), pltpu.SemaphoreType.DMA((2,))],
        compiler_params=pltpu.CompilerParams(vmem_limit_bytes=LARGE),
        name="unpack",
    )(meta, *mine, *theirs)


def ring_step(value, second, step):
    pairs = []
    for x in range(4):
        for y in range(4):
            for core in range(2):
                along_y = (core == 0) != second
                to = (x, (y + step) % 4) if along_y else ((x + step) % 4, y)
                pairs.append((x * 8 + y * 2 + core, to[0] * 8 + to[1] * 2 + core))
    return lax.ppermute(value, DP, pairs)


def swap_cores(value):
    return lax.ppermute(value, "dp_2", [(0, 1), (1, 0)])


def join_kernel(*refs):
    *parts, out, sems = refs
    copies = [
        pltpu.make_async_copy(part, out.at[n], sems.at[n]) for n, part in enumerate(parts)
    ]
    for copy in copies:
        copy.start()
    for copy in copies:
        copy.wait()


def join(*parts):
    return pl.pallas_call(
        join_kernel,
        out_shape=jax.ShapeDtypeStruct((len(parts), *parts[0].shape), parts[0].dtype),
        in_specs=[ANY] * len(parts),
        out_specs=ANY,
        scratch_shapes=[pltpu.SemaphoreType.DMA((len(parts),))],
        compiler_params=pltpu.CompilerParams(vmem_limit_bytes=1024 * 1024),
        name="join",
    )(*parts)


def gather_weights(core, w_qkv, w_out, others):
    keep, give = pack(core, w_qkv, w_out)
    got, others = lax.optimization_barrier((swap_cores(give), others))
    meta = others[0]
    lines = []
    for value, forward in ((keep, 1), (got, -1)):
        before = ring_step(value, False, 1)
        after = ring_step(value, False, -1)
        across = ring_step(before if forward == 1 else after, False, forward)
        lines.append(join(value, before, after, across))
    mine = [None] * 8
    for n, (line, forward) in enumerate(zip(lines, (1, -1))):
        before = ring_step(line, True, 1)
        after = ring_step(line, True, -1)
        across = ring_step(before if forward == 1 else after, True, forward)
        mine[n::2] = [line, before, after, across]
    return unpack(meta, mine, [swap_cores(value) for value in mine]), others


WIDE = HALF + 128


def pooled_rows(last):
    return jnp.concatenate([last[j, 0:1, :] for j in (0, 2, 1, 3)], axis=0)


def embed_kernel(last, final_gain, labels, out):
    rows = pooled_rows(last)
    pooled = rows * inv_rms(rows) * final_gain[...]
    unit = pooled * lax.rsqrt(jnp.sum(pooled * pooled, axis=1, keepdims=True))
    halves = jnp.concatenate([unit[:, :HALF], unit[:, HALF:]], axis=0).astype(BF16)
    which = lax.broadcasted_iota(jnp.int32, (8, 128), 0)
    label = jnp.where(which == 0, labels[0], jnp.where(which == 1, labels[1], 0))
    label = label.astype(F32).astype(BF16)
    for i in range(out.shape[0]):
        out[i, :, :HALF] = halves
        out[i, :, HALF:] = label


def embed(count, last, final_gain, labels):
    return pl.pallas_call(
        embed_kernel,
        out_shape=jax.ShapeDtypeStruct((count, 8, WIDE), BF16),
        in_specs=[VMEM, VMEM, SMEM],
        out_specs=VMEM,
        compiler_params=pltpu.CompilerParams(vmem_limit_bytes=LIMIT),
        name="embed",
    )(last, final_gain, labels)


def loss_kernel(meta, last, final_gain, here, there, seed):
    everyone = jnp.concatenate([here[...], there[...]], axis=0)
    count = everyone.shape[0]
    emb = everyone[:, :HALF]
    label = everyone[:, HALF:].astype(F32)[:, 0:1].astype(jnp.int32)
    scores = dot_nt(emb, emb)
    scores = scores + pltpu.roll(pltpu.roll(scores, count - 4, 0), count - 4, 1)
    row = lax.rem(lax.broadcasted_iota(jnp.int32, (count, count), 0), 8)
    col = lax.broadcasted_iota(jnp.int32, (count, count), 1)
    doc = jnp.logical_and(lax.rem(col, 8) >= 2, lax.rem(col, 8) < 4)
    valid = jnp.logical_and(row < 2, doc)
    weights = jnp.where(valid, jnp.exp(scores * SHARP), 0.0)
    total = jnp.sum(weights, axis=1, keepdims=True)
    prob = weights / jnp.where(row[:, :1] < 2, total, 1.0)
    owner = lax.div(label, 2)
    away = (lax.rem(owner, 2) != meta[5]).astype(jnp.int32)
    target = away * (count // 2) + lax.div(owner, 2) * 8 + 2 + lax.rem(label, 2)
    coef = jnp.where(valid, (prob - (col == target).astype(F32)) * (COEF * SHARP), 0.0)
    both = coef + coef.T
    mine = lax.broadcasted_iota(jnp.int32, (8, count), 0)
    pick = lax.broadcasted_iota(jnp.int32, (8, count), 1) == lax.div(meta[6], 2) * 8 + mine
    own = lax.dot_general(
        pick.astype(F32),
        both,
        (((1,), (0,)), ((), ())),
        precision=lax.Precision.HIGHEST,
        preferred_element_type=F32,
    )[:4]
    own = jnp.concatenate([own, pltpu.roll(own, 4, 1)], axis=0)
    top = own.astype(BF16)
    rest = own - top.astype(F32)
    mid = rest.astype(BF16)
    low = (rest - mid.astype(F32)).astype(BF16)
    split = dot_nn(jnp.concatenate([top, mid, low, low], axis=0), emb)
    grad = split[:8] + (split[8:16] + split[16:24])
    grad = jnp.concatenate([grad[:4], grad[4:]], axis=1)
    rows = pooled_rows(last)
    gain = final_gain[...]
    scale = inv_rms(rows)
    pooled = rows * scale * gain
    norm = lax.rsqrt(jnp.sum(pooled * pooled, axis=1, keepdims=True))
    unit = pooled * norm
    dpooled = norm * (grad - unit * jnp.sum(grad * unit, axis=1, keepdims=True))
    scaled = dpooled * gain
    inner = jnp.sum(scaled * rows, axis=1, keepdims=True)
    drow = scale * scaled - rows * (scale * scale * scale * inner * (1.0 / D))
    drow = drow.astype(BF16).astype(F32)
    seed[...] = jnp.concatenate(
        [drow[0:1], drow[2:3], drow[1:2], drow[3:4], jnp.zeros((4, D), F32)], axis=0
    )


def loss_seed(meta, last, final_gain, here, there):
    return pl.pallas_call(
        loss_kernel,
        out_shape=jax.ShapeDtypeStruct((8, D), F32),
        in_specs=[SMEM, VMEM, VMEM, VMEM, VMEM],
        out_specs=VMEM,
        compiler_params=pltpu.CompilerParams(vmem_limit_bytes=LIMIT),
        name="loss_seed",
    )(meta, last, final_gain, here, there)


def rotary_table():
    lane = jnp.arange(128, dtype=jnp.int32)
    frequency = ROPE_BASE ** (-(lane % 32).astype(F32) * (2.0 / HEAD_DIM))
    angles = jnp.arange(LEN, dtype=F32)[:, None] * frequency[None, :]
    sign = jnp.where(lane % 64 < 32, -1.0, 1.0)
    return jnp.stack([jnp.cos(angles), jnp.sin(angles) * sign])


def per_device(entry, norm_gain, w_qkv, w_out, final_gain, lengths, positive):
    stage = lax.axis_index("section")
    stages = lax.axis_size("section")
    replica = lax.axis_index(DP)
    places = [lax.axis_index(name)[None] for name in DP]
    micro = lengths.shape[0]
    gain = norm_gain
    numbers = jnp.array([stages], jnp.int32)
    meta = jnp.concatenate(
        [stage[None], lengths, places[2], replica[None], numbers, places[0], places[1]]
    )
    (wq, wo), (meta, final_row, table) = gather_weights(
        places[2], w_qkv[0], w_out[0], (meta, final_gain[None, :], rotary_table())
    )
    ticks = micro + stages - 1
    half = stages // 2
    state, turned = (), ()
    inbox = entry
    for tick in range(ticks):
        before = turned if tick in (1, half + micro) else ()
        out, *state = forward_layer(
            tick, stages - 1, micro, meta, inbox, entry, gain, table, wq, wo, before, state
        )
        if tick == 0:
            turned = turn(True, meta, out, wq, wo, turned)
        if tick == half + micro - 1:
            turned = turn(False, meta, out, wq, wo, turned)
        if tick < ticks - 1:
            pairs = [(s, s + 1) for s in range(stages - 1) if 0 <= tick - s < micro]
            inbox = lax.ppermute(out, "section", pairs)
    *stash, last = state
    count = lax.axis_size(DP[:2])
    copies = embed(count, last, final_row, positive)
    here = lax.all_to_all(copies, DP[:2], split_axis=0, concat_axis=0, tiled=True)
    here = here.reshape(count * 8, WIDE)
    there = lax.ppermute(here, "dp_2", [(0, 1), (1, 0)])
    seed = loss_seed(meta, last, final_row, here, there)
    previous = ()
    for tick in range(ticks):
        previous = backward_layer(
            tick, stages - 1, micro, meta, inbox, seed, gain, table, *turned, stash, previous
        )
        if tick < ticks - 1:
            pairs = [
                (stages - 1 - s, stages - 2 - s)
                for s in range(stages - 1)
                if 0 <= tick - s < micro
            ]
            inbox = lax.ppermute(previous[0], "section", pairs)
    return previous[1][None]


def solution(mesh):
    finer = Mesh(
        mesh.devices.reshape(mesh.shape["section"], 4, 4, 2), ("section", "dp_0", "dp_1", "dp_2")
    )
    in_specs = (
        P(DP, None),
        P("section", None),
        P("section", DP, None),
        P("section", DP, None),
        P(),
        P(DP),
        P(DP),
    )
    return jax.shard_map(
        per_device,
        mesh=finer,
        in_specs=in_specs,
        out_specs=P("section", DP, None),
        check_vma=False,
    )
```

```python
import functools

import jax
import jax.numpy as jnp
from jax import lax
from jax.experimental import pallas as pl
from jax.experimental.pallas import tpu as pltpu
from jax.sharding import Mesh
from jax.sharding import PartitionSpec as P

HEAD_DIM = 64
LEN = 48
D = 3584
QW = 896
KV = 128
XW = QW + 2 * KV
PACK = XW + QW
PAIRS = QW // 128
DP = ("dp_0", "dp_1", "dp_2")
ROPE_BASE = 1000000.0
EPS = 1e-06
SHARP = 20.0
COEF = 256.0
HALVES = 2
HALF = D // HALVES
STAGGER = 5000
EVEN = 850
F32 = jnp.float32
BF16 = jnp.bfloat16


def dot_nn(a, b):
    return lax.dot_general(a, b, (((1,), (0,)), ((), ())), preferred_element_type=F32)


def dot_nt(a, b):
    return lax.dot_general(a, b, (((1,), (1,)), ((), ())), preferred_element_type=F32)


def dot_tn(a, b):
    return lax.dot_general(a, b, (((0,), (0,)), ((), ())), preferred_element_type=F32)


def lanes(rows):
    return lax.broadcasted_iota(jnp.int32, (rows, 128), 1)


def partner(x):
    low = lax.rem(lanes(x.shape[0]), 64) < 32
    return jnp.where(low, pltpu.roll(x, 96, 1), pltpu.roll(x, 32, 1))


def paired(z):
    left = lanes(LEN) < 64
    rolled = pltpu.roll(z, 64, 1)
    pad = jnp.zeros((16, 128), BF16)
    a_left = jnp.where(left, z, 0.0).astype(BF16)
    b_right = jnp.where(left, 0.0, z).astype(BF16)
    b_left = jnp.where(left, rolled, 0.0).astype(BF16)
    a_right = jnp.where(left, 0.0, rolled).astype(BF16)
    return (
        jnp.concatenate([a_left, pad, a_right, pad], axis=0),
        jnp.concatenate([a_left, pad, b_right, pad], axis=0),
        jnp.concatenate([b_left, pad, b_right, pad], axis=0),
    )


SPANS = ((0, 3 * LEN), (3 * LEN, 4 * LEN), (4 * LEN, 7 * LEN))


def by_pair(dot, rows, blocks):
    return jnp.concatenate(
        [dot(rows[lo:hi], block) for (lo, hi), block in zip(SPANS, blocks)], axis=0
    )


def unpaired(rows, other):
    left = lanes(LEN) < 64
    s00, s01, s11 = (dot_tn(rows[lo:hi], other[lo:hi]) for lo, hi in SPANS)
    first = jnp.where(left, s00[:LEN] + s01[:LEN], 0.0)
    first += pltpu.roll(jnp.where(left, 0.0, s00[64 : 64 + LEN]), 64, 1)
    second = jnp.where(left, 0.0, s01[64 : 64 + LEN] + s11[64 : 64 + LEN])
    second += pltpu.roll(jnp.where(left, s11[:LEN], 0.0), 64, 1)
    return first + second


def half_sums(x):
    left = lanes(x.shape[0]) < 64
    low = jnp.sum(jnp.where(left, x, 0.0), axis=1, keepdims=True)
    high = jnp.sum(jnp.where(left, 0.0, x), axis=1, keepdims=True)
    return low, high, left


def probabilities(q_rows, k_blocks, length):
    scores = by_pair(dot_nt, q_rows, k_blocks) * HEAD_DIM ** (-0.5)
    live = lax.rem(lanes(scores.shape[0]), 64) < length
    weights = jnp.where(live, jnp.exp(scores), 0.0)
    low, high, left = half_sums(weights)
    return weights * jnp.where(left, 1.0 / low, 1.0 / high)


def rows_of(x_ref):
    return jnp.concatenate([x_ref[:, 128 * i : 128 * i + 128] for i in range(PAIRS)], axis=0)


def inv_rms(wide):
    return lax.rsqrt(jnp.sum(wide * wide, axis=1, keepdims=True) * (1.0 / D) + EPS)


def forward_kernel(
    tick,
    last_stage,
    micro,
    meta,
    inbox,
    entry,
    gain,
    table,
    wq,
    wo,
    *refs,
):
    out, stash_h, stash_x, last, stash_p = refs[-13:-8]
    h_v, n_v, acc_v, x_v, ctx_v, last_v, p_v, sems = refs[-8:]
    stage = meta[0]
    slot = tick - stage

    @pl.when(jnp.logical_and(slot >= 0, slot < micro))
    def _():
        length = meta[1 + slot]
        row0 = pl.multiple_of(slot * LEN, LEN)

        @pl.when(stage == 0)
        def _():
            fresh = pltpu.make_async_copy(entry.at[pl.ds(row0, LEN), :], h_v, sems.at[0])
            fresh.start()
            fresh.wait()

        @pl.when(stage != 0)
        def _():
            h_v[...] = inbox[:LEN]

        @pl.when(jnp.logical_and(meta[5] == 1, stage != last_stage))
        def _():
            pl.delay(STAGGER if tick == 0 else EVEN)

        keep_h = pltpu.make_async_copy(h_v, stash_h.at[pl.ds(row0, LEN), :], sems.at[1])
        keep_h.start()
        wide = h_v[...].astype(F32)
        n_v[...] = (wide * inv_rms(wide) * gain[...]).astype(BF16)
        acc_v[...] = jnp.zeros_like(acc_v)

        @pl.loop(0, HALVES)
        def _(i):
            cols = pl.ds(pl.multiple_of(i * HALF, HALF), HALF)
            acc_v[...] += dot_nn(n_v[:, cols], wq[cols, :])

        cosine, sine = table[0], table[1]
        for i in range(PAIRS + 1):
            part = acc_v[:, 128 * i : 128 * i + 128]
            x_v[:, 128 * i : 128 * i + 128] = (part * cosine + partner(part) * sine).astype(BF16)
        x_v[:, QW + KV :] = acc_v[:, QW + KV :].astype(BF16)
        keep_x = pltpu.make_async_copy(x_v, stash_x.at[pl.ds(row0, LEN), :], sems.at[2])
        keep_x.start()
        k_blocks = paired(x_v[:, QW : QW + KV].astype(F32))
        v_blocks = paired(x_v[:, QW + KV :].astype(F32))
        probs = probabilities(rows_of(x_v), k_blocks, length)
        p_v[...] = probs
        keep_p = pltpu.make_async_copy(p_v, stash_p.at[slot], sems.at[4])
        keep_p.start()
        context = by_pair(dot_nn, probs.astype(BF16), v_blocks).astype(BF16)
        for i in range(PAIRS):
            ctx_v[:, 128 * i : 128 * i + 128] = context[LEN * i : LEN * i + LEN]

        @pl.loop(0, HALVES)
        def _(i):
            cols = pl.ds(pl.multiple_of(i * HALF, HALF), HALF)
            branch = dot_nn(ctx_v[...], wo[:, cols])
            out[:, cols] = (h_v[:, cols].astype(F32) + branch).astype(BF16)

        @pl.when(stage == last_stage)
        def _():
            hit = lax.broadcasted_iota(jnp.int32, (LEN, D), 0) == length - 1
            row = jnp.sum(jnp.where(hit, out[...].astype(F32), 0.0), axis=0, keepdims=True)
            last_v[...] = jnp.broadcast_to(row, (8, D))
            put = pltpu.make_async_copy(last_v, last.at[slot], sems.at[3])
            put.start()
            put.wait()

        keep_h.wait()
        keep_x.wait()
        keep_p.wait()


def backward_kernel(
    tick,
    last_stage,
    micro,
    meta,
    inbox,
    seed,
    gain,
    table,
    wq,
    wo,
    stash_h,
    stash_x,
    stash_p,
    *refs,
):
    out, grads, h_v, g_v, x_v, dctx_v, dx_v, dn_v, p_v, sems = refs[-10:]
    stage = meta[0]
    slot = tick - (last_stage - stage)

    def put(value, to):
        rows = pl.ds(pl.multiple_of(to * LEN, LEN), LEN)
        return pltpu.make_async_copy(value, grads.at[rows, :], sems.at[2])

    late = jnp.logical_and(slot >= 1, slot <= micro)
    if tick > 0:

        @pl.when(late)
        def _():
            put(refs[0], slot - 1).start()

    @pl.when(jnp.logical_and(slot >= 0, slot < micro))
    def _():
        length = meta[1 + slot]
        row0 = pl.multiple_of(slot * LEN, LEN)

        get_x = pltpu.make_async_copy(stash_x.at[pl.ds(row0, LEN), :], x_v, sems.at[0])
        get_h = pltpu.make_async_copy(stash_h.at[pl.ds(row0, LEN), :], h_v, sems.at[1])
        get_p = pltpu.make_async_copy(stash_p.at[slot], p_v, sems.at[3])
        get_x.start()
        get_p.start()
        get_h.start()

        @pl.when(jnp.logical_and(meta[5] == 1, stage != 0))
        def _():
            pl.delay(STAGGER if tick == 0 else EVEN)

        @pl.when(stage == last_stage)
        def _():
            hit = lax.broadcasted_iota(jnp.int32, (LEN, D), 0) == length - 1
            row = jnp.where(lax.broadcasted_iota(jnp.int32, (8, D), 0) == slot, seed[...], 0.0)
            row = jnp.sum(row, axis=0, keepdims=True)
            g_v[...] = jnp.where(hit, jnp.broadcast_to(row, (LEN, D)), 0.0).astype(BF16)

        @pl.when(stage != last_stage)
        def _():
            g_v[...] = inbox[...]

        dctx_v[...] = jnp.zeros_like(dctx_v)

        @pl.loop(0, HALVES)
        def _(i):
            cols = pl.ds(pl.multiple_of(i * HALF, HALF), HALF)
            dctx_v[...] += dot_nn(g_v[:, cols], wo[cols, :])

        get_x.wait()
        get_p.wait()
        q_rows = rows_of(x_v)
        k_blocks = paired(x_v[:, QW : QW + KV].astype(F32))
        v_blocks = paired(x_v[:, QW + KV :].astype(F32))
        probs = p_v[...]
        dctx = rows_of(dctx_v).astype(BF16)
        dvalue = unpaired(probs.astype(BF16), dctx)
        dprobs = by_pair(dot_nt, dctx, v_blocks).astype(BF16).astype(F32)
        low, high, left = half_sums(dprobs * probs)
        dscores = probs * (dprobs - jnp.where(left, low, high)) * HEAD_DIM ** (-0.5)
        dscores = dscores.astype(BF16)
        dquery = by_pair(dot_nn, dscores, k_blocks).astype(BF16).astype(F32)
        dkey = unpaired(dscores, q_rows).astype(BF16).astype(F32)
        cosine, sine = table[0], table[1]
        for i in range(PAIRS):
            part = dquery[LEN * i : LEN * i + LEN]
            dx_v[:, 128 * i : 128 * i + 128] = (part * cosine - partner(part) * sine).astype(BF16)
        dx_v[:, QW : QW + KV] = (dkey * cosine - partner(dkey) * sine).astype(BF16)
        dx_v[:, QW + KV :] = dvalue.astype(BF16)

        @pl.loop(0, HALVES)
        def _(i):
            cols = pl.ds(pl.multiple_of(i * HALF, HALF), HALF)
            dn_v[:, cols] = dot_nn(dx_v[...], wq[:, cols]).astype(BF16)

        get_h.wait()
        wide = h_v[...].astype(F32)
        scale = inv_rms(wide)
        scaled = dn_v[...].astype(F32) * gain[...]
        inner = jnp.sum(scaled * wide, axis=1, keepdims=True)
        out[...] = (
            g_v[...].astype(F32)
            + scale * scaled
            - wide * (scale * scale * scale * inner * (1.0 / D))
        ).astype(BF16)

    if tick > 0:

        @pl.when(late)
        def _():
            put(refs[0], slot - 1).wait()

    if tick == last_stage + micro - 1:

        @pl.when(slot == micro - 1)
        def _():
            put(out, slot).start()
            put(out, slot).wait()


ANY = pl.BlockSpec(memory_space=pl.ANY)
VMEM = pl.BlockSpec(memory_space=pltpu.VMEM)
SMEM = pl.BlockSpec(memory_space=pltpu.SMEM)
HBM = pl.BlockSpec(memory_space=pltpu.HBM)
LAYER_COST = pl.CostEstimate(
    flops=2 * LEN * D * (XW + QW), bytes_accessed=2 * D * (XW + QW), transcendentals=0
)
LIMIT = 8 * 1024 * 1024
LARGE = 14 * 1024 * 1024
WHOLE = 60 * 1024 * 1024
SMALL = 8 * 1024 * 1024


def forward_layer(
    tick, last_stage, micro, meta, inbox, entry, gain, table, wq, wo, before, state
):
    rows = micro * LEN
    kept = (
        ((rows, D), BF16),
        ((rows, XW), BF16),
        ((micro, 8, D), F32),
        ((micro, PAIRS * LEN, 128), F32),
    )
    return pl.pallas_call(
        functools.partial(forward_kernel, tick, last_stage, micro),
        out_shape=tuple(jax.ShapeDtypeStruct(*a) for a in (((LEN, D), BF16), *kept)),
        in_specs=[SMEM, VMEM, ANY, VMEM, VMEM, VMEM, VMEM, *[ANY] * len((*before, *state))],
        out_specs=(VMEM, ANY, ANY, ANY, ANY),
        input_output_aliases={7 + len(before) + i: 1 + i for i in range(len(state))},
        scratch_shapes=[
            pltpu.VMEM((LEN, D), BF16),
            pltpu.VMEM((LEN, D), BF16),
            pltpu.VMEM((LEN, XW), F32),
            pltpu.VMEM((LEN, XW), BF16),
            pltpu.VMEM((LEN, QW), BF16),
            pltpu.VMEM((8, D), F32),
            pltpu.VMEM((PAIRS * LEN, 128), F32),
            pltpu.SemaphoreType.DMA((5,)),
        ],
        compiler_params=pltpu.CompilerParams(vmem_limit_bytes=LIMIT),
        cost_estimate=LAYER_COST,
        name="forward_layer",
    )(meta, inbox, entry, gain, table, wq, wo, *before, *state)


def backward_layer(
    tick, last_stage, micro, meta, inbox, seed, gain, table, wq_t, wo_t, stash, previous
):
    return pl.pallas_call(
        functools.partial(backward_kernel, tick, last_stage, micro),
        out_shape=(
            jax.ShapeDtypeStruct((LEN, D), BF16),
            jax.ShapeDtypeStruct((micro * LEN, D), BF16),
        ),
        in_specs=[SMEM, VMEM, VMEM, VMEM, VMEM, VMEM, VMEM, ANY, ANY, ANY, *[ANY] * len(previous)],
        out_specs=(VMEM, ANY),
        input_output_aliases={11: 1} if previous else {},
        scratch_shapes=[
            pltpu.VMEM((LEN, D), BF16),
            pltpu.VMEM((LEN, D), BF16),
            pltpu.VMEM((LEN, XW), BF16),
            pltpu.VMEM((LEN, QW), F32),
            pltpu.VMEM((LEN, XW), BF16),
            pltpu.VMEM((LEN, D), BF16),
            pltpu.VMEM((PAIRS * LEN, 128), F32),
            pltpu.SemaphoreType.DMA((4,)),
        ],
        compiler_params=pltpu.CompilerParams(vmem_limit_bytes=LIMIT),
        cost_estimate=LAYER_COST,
        name="backward_layer",
    )(meta, inbox, seed, gain, table, wq_t, wo_t, *stash, *previous)


TURN = 256


def turn_kernel(early, meta, after, wq, wo, *refs):
    del after
    wq_t, wo_t, wq_v, wo_v, sems = refs[-5:]
    half = lax.div(meta[7], 2)
    due = meta[0] >= half if early else meta[0] < half

    @pl.when(due)
    def _():
        def copies(i, slot):
            at = pl.ds(pl.multiple_of(i * TURN, TURN), TURN)
            return (
                pltpu.make_async_copy(wq_v.at[slot], wq_t.at[:, at], sems.at[0, slot]),
                pltpu.make_async_copy(wo_v.at[slot], wo_t.at[at, :], sems.at[1, slot]),
            )

        @pl.loop(0, D // TURN)
        def _(i):
            slot = lax.rem(i, 2)
            at = pl.ds(pl.multiple_of(i * TURN, TURN), TURN)

            @pl.when(i >= 2)
            def _():
                for copy in copies(i - 2, slot):
                    copy.wait()

            wq_v[slot] = wq[at, :].T
            wo_v[slot] = wo[:, at].T
            for copy in copies(i, slot):
                copy.start()

        for i in (D // TURN - 2, D // TURN - 1):
            for copy in copies(i, i % 2):
                copy.wait()


def turn(early, meta, after, wq, wo, turned):
    return pl.pallas_call(
        functools.partial(turn_kernel, early),
        out_shape=(jax.ShapeDtypeStruct((XW, D), BF16), jax.ShapeDtypeStruct((D, QW), BF16)),
        in_specs=[SMEM, ANY, VMEM, VMEM, *[ANY] * len(turned)],
        out_specs=(ANY, ANY),
        input_output_aliases={4 + i: i for i in range(len(turned))},
        scratch_shapes=[
            pltpu.VMEM((2, XW, TURN), BF16),
            pltpu.VMEM((2, TURN, QW), BF16),
            pltpu.SemaphoreType.DMA((2, 2)),
        ],
        compiler_params=pltpu.CompilerParams(vmem_limit_bytes=LIMIT),
        cost_estimate=pl.CostEstimate(flops=0, bytes_accessed=4 * D * (XW + QW), transcendentals=0),
        name="turn",
    )(meta, after, wq, wo, *turned)


SIDE = PACK // 2


def pack_kernel(core, w_qkv, w_out, keep, give, w_v, x_v, sems):
    first = pltpu.make_async_copy(w_out, w_v, sems.at[0])
    second = pltpu.make_async_copy(w_qkv, x_v, sems.at[1])
    first.start()
    second.start()
    first.wait()
    pieces = [w_v[:, QW * j : QW * j + QW].astype(F32) for j in range(D // QW)]
    low = jnp.concatenate(pieces, axis=0).astype(BF16)
    second.wait()

    def fill(left, right):
        left[...] = x_v[:, :SIDE]
        right[:, : XW - SIDE] = x_v[:, SIDE:]
        right[:, XW - SIDE :] = low

    @pl.when(core[0] == 0)
    def _():
        fill(keep, give)

    @pl.when(core[0] == 1)
    def _():
        fill(give, keep)


def pack(core, w_qkv, w_out):
    side = jax.ShapeDtypeStruct((w_qkv.shape[0], SIDE), BF16)
    return pl.pallas_call(
        pack_kernel,
        out_shape=(side, side),
        in_specs=[SMEM, HBM, HBM],
        out_specs=(VMEM, VMEM),
        scratch_shapes=[
            pltpu.VMEM(w_out.shape, BF16),
            pltpu.VMEM(w_qkv.shape, BF16),
            pltpu.SemaphoreType.DMA((2,)),
        ],
        compiler_params=pltpu.CompilerParams(vmem_limit_bytes=WHOLE),
        name="pack",
    )(core, w_qkv, w_out)


def unpack_kernel(meta, *refs):
    count = (len(refs) - 4) // 2
    mine, theirs = refs[:count], refs[count : 2 * count]
    wq, wo, part_v, sems = refs[2 * count :]
    parts = D // QW
    length = D // 32
    short = length // parts
    x0, y0, core = meta[8], meta[9], meta[5]

    def offset(step):
        return jnp.where(step == 1, 3, jnp.where(step == 2, 1, jnp.where(step == 3, 2, 0)))

    def put(blocks, color):
        for n in range(8):
            block = blocks[n]
            far, other = n // 2, n % 2

            @pl.loop(0, 4)
            def _(near):
                first = lax.rem(offset(near) + (y0 if color == 0 else x0), 4)
                second = lax.rem((0, 3, 1, 2)[far] + (x0 if color == 0 else y0), 4)
                x, y = (second, first) if color == 0 else (first, second)
                shard = x * 8 + y * 2 + (color if other == 0 else 1 - color)
                rows = pl.ds(pl.multiple_of(shard * length, length), length)
                if color == 0:
                    pltpu.make_async_copy(
                        block.at[near], wq.at[rows, pl.ds(0, SIDE)], sems.at[0]
                    ).start()
                else:
                    pltpu.make_async_copy(
                        block.at[near, :, pl.ds(0, XW - SIDE)],
                        wq.at[rows, pl.ds(SIDE, XW - SIDE)],
                        sems.at[0],
                    ).start()
                    pltpu.make_async_copy(
                        block.at[near, :, pl.ds(XW - SIDE, QW)], part_v.at[rows, :], sems.at[1]
                    ).start()

    @pl.when(core == 0)
    def _():
        put(theirs, 1)
        put(mine, 0)

    @pl.when(core == 1)
    def _():
        put(mine, 1)
        put(theirs, 0)

    pltpu.make_async_copy(part_v, part_v, sems.at[1]).wait()

    @pl.loop(0, 8)
    def _(i):
        blocks = []
        for r in range(4):
            at = pl.ds(pl.multiple_of((4 * i + r) * length, length), length)
            blocks.append(part_v[at, :].astype(F32))
        to = pl.ds(pl.multiple_of(i * length, length), length)
        for j in range(parts):
            cut = [block[short * j : short * j + short] for block in blocks]
            wo[to, QW * j : QW * j + QW] = jnp.concatenate(cut, axis=0).astype(BF16)

    pltpu.make_async_copy(wq, wq, sems.at[0]).wait()


def unpack(meta, mine, theirs):
    return pl.pallas_call(
        unpack_kernel,
        out_shape=(jax.ShapeDtypeStruct((D, XW), BF16), jax.ShapeDtypeStruct((QW, D), BF16)),
        in_specs=[SMEM, *[ANY] * (len(mine) + len(theirs))],
        out_specs=(VMEM, VMEM),
        scratch_shapes=[pltpu.VMEM((D, QW), BF16), pltpu.SemaphoreType.DMA((2,))],
        compiler_params=pltpu.CompilerParams(vmem_limit_bytes=LARGE),
        name="unpack",
    )(meta, *mine, *theirs)


def ring_step(value, second, step):
    pairs = []
    for x in range(4):
        for y in range(4):
            for core in range(2):
                along_y = (core == 0) != second
                to = (x, (y + step) % 4) if along_y else ((x + step) % 4, y)
                pairs.append((x * 8 + y * 2 + core, to[0] * 8 + to[1] * 2 + core))
    return lax.ppermute(value, DP, pairs)


def swap_cores(value):
    return lax.ppermute(value, "dp_2", [(0, 1), (1, 0)])


def join_kernel(*refs):
    *parts, out, sems = refs
    copies = [
        pltpu.make_async_copy(part, out.at[n], sems.at[n]) for n, part in enumerate(parts)
    ]
    for copy in copies:
        copy.start()
    for copy in copies:
        copy.wait()


def join(*parts):
    return pl.pallas_call(
        join_kernel,
        out_shape=jax.ShapeDtypeStruct((len(parts), *parts[0].shape), parts[0].dtype),
        in_specs=[ANY] * len(parts),
        out_specs=ANY,
        scratch_shapes=[pltpu.SemaphoreType.DMA((len(parts),))],
        compiler_params=pltpu.CompilerParams(vmem_limit_bytes=1024 * 1024),
        name="join",
    )(*parts)


def gather_weights(core, w_qkv, w_out, others):
    keep, give = pack(core, w_qkv, w_out)
    got, others = lax.optimization_barrier((swap_cores(give), others))
    meta = others[0]
    lines = []
    for value, forward in ((keep, 1), (got, -1)):
        before = ring_step(value, False, 1)
        after = ring_step(value, False, -1)
        across = ring_step(before if forward == 1 else after, False, forward)
        lines.append(join(value, before, after, across))
    mine = [None] * 8
    for n, (line, forward) in enumerate(zip(lines, (1, -1))):
        before = ring_step(line, True, 1)
        after = ring_step(line, True, -1)
        across = ring_step(before if forward == 1 else after, True, forward)
        mine[n::2] = [line, before, after, across]
    return unpack(meta, mine, [swap_cores(value) for value in mine]), others


WIDE = HALF + 128


def pooled_rows(last):
    return jnp.concatenate([last[j, 0:1, :] for j in (0, 2, 1, 3)], axis=0)


def embed_kernel(last, final_gain, labels, out):
    rows = pooled_rows(last)
    pooled = rows * inv_rms(rows) * final_gain[...]
    unit = pooled * lax.rsqrt(jnp.sum(pooled * pooled, axis=1, keepdims=True))
    halves = jnp.concatenate([unit[:, :HALF], unit[:, HALF:]], axis=0).astype(BF16)
    which = lax.broadcasted_iota(jnp.int32, (8, 128), 0)
    label = jnp.where(which == 0, labels[0], jnp.where(which == 1, labels[1], 0))
    label = label.astype(F32).astype(BF16)
    for i in range(out.shape[0]):
        out[i, :, :HALF] = halves
        out[i, :, HALF:] = label


def embed(count, last, final_gain, labels):
    return pl.pallas_call(
        embed_kernel,
        out_shape=jax.ShapeDtypeStruct((count, 8, WIDE), BF16),
        in_specs=[VMEM, VMEM, SMEM],
        out_specs=VMEM,
        compiler_params=pltpu.CompilerParams(vmem_limit_bytes=LIMIT),
        name="embed",
    )(last, final_gain, labels)


def loss_kernel(meta, last, final_gain, here, there, seed):
    everyone = jnp.concatenate([here[...], there[...]], axis=0)
    count = everyone.shape[0]
    emb = everyone[:, :HALF]
    label = everyone[:, HALF:].astype(F32)[:, 0:1].astype(jnp.int32)
    scores = dot_nt(emb, emb)
    scores = scores + pltpu.roll(pltpu.roll(scores, count - 4, 0), count - 4, 1)
    row = lax.rem(lax.broadcasted_iota(jnp.int32, (count, count), 0), 8)
    col = lax.broadcasted_iota(jnp.int32, (count, count), 1)
    doc = jnp.logical_and(lax.rem(col, 8) >= 2, lax.rem(col, 8) < 4)
    valid = jnp.logical_and(row < 2, doc)
    weights = jnp.where(valid, jnp.exp(scores * SHARP), 0.0)
    total = jnp.sum(weights, axis=1, keepdims=True)
    prob = weights / jnp.where(row[:, :1] < 2, total, 1.0)
    owner = lax.div(label, 2)
    away = (lax.rem(owner, 2) != meta[5]).astype(jnp.int32)
    target = away * (count // 2) + lax.div(owner, 2) * 8 + 2 + lax.rem(label, 2)
    coef = jnp.where(valid, (prob - (col == target).astype(F32)) * (COEF * SHARP), 0.0)
    both = coef + coef.T
    mine = lax.broadcasted_iota(jnp.int32, (8, count), 0)
    pick = lax.broadcasted_iota(jnp.int32, (8, count), 1) == lax.div(meta[6], 2) * 8 + mine
    own = lax.dot_general(
        pick.astype(F32),
        both,
        (((1,), (0,)), ((), ())),
        precision=lax.Precision.HIGHEST,
        preferred_element_type=F32,
    )[:4]
    own = jnp.concatenate([own, pltpu.roll(own, 4, 1)], axis=0)
    top = own.astype(BF16)
    rest = own - top.astype(F32)
    mid = rest.astype(BF16)
    low = (rest - mid.astype(F32)).astype(BF16)
    split = dot_nn(jnp.concatenate([top, mid, low, low], axis=0), emb)
    grad = split[:8] + (split[8:16] + split[16:24])
    grad = jnp.concatenate([grad[:4], grad[4:]], axis=1)
    rows = pooled_rows(last)
    gain = final_gain[...]
    scale = inv_rms(rows)
    pooled = rows * scale * gain
    norm = lax.rsqrt(jnp.sum(pooled * pooled, axis=1, keepdims=True))
    unit = pooled * norm
    dpooled = norm * (grad - unit * jnp.sum(grad * unit, axis=1, keepdims=True))
    scaled = dpooled * gain
    inner = jnp.sum(scaled * rows, axis=1, keepdims=True)
    drow = scale * scaled - rows * (scale * scale * scale * inner * (1.0 / D))
    drow = drow.astype(BF16).astype(F32)
    seed[...] = jnp.concatenate(
        [drow[0:1], drow[2:3], drow[1:2], drow[3:4], jnp.zeros((4, D), F32)], axis=0
    )


def loss_seed(meta, last, final_gain, here, there):
    return pl.pallas_call(
        loss_kernel,
        out_shape=jax.ShapeDtypeStruct((8, D), F32),
        in_specs=[SMEM, VMEM, VMEM, VMEM, VMEM],
        out_specs=VMEM,
        compiler_params=pltpu.CompilerParams(vmem_limit_bytes=LIMIT),
        name="loss_seed",
    )(meta, last, final_gain, here, there)


def rotary_table():
    lane = jnp.arange(128, dtype=jnp.int32)
    frequency = ROPE_BASE ** (-(lane % 32).astype(F32) * (2.0 / HEAD_DIM))
    angles = jnp.arange(LEN, dtype=F32)[:, None] * frequency[None, :]
    sign = jnp.where(lane % 64 < 32, -1.0, 1.0)
    return jnp.stack([jnp.cos(angles), jnp.sin(angles) * sign])


def per_device(entry, norm_gain, w_qkv, w_out, final_gain, lengths, positive):
    stage = lax.axis_index("section")
    stages = lax.axis_size("section")
    replica = lax.axis_index(DP)
    places = [lax.axis_index(name)[None] for name in DP]
    micro = lengths.shape[0]
    gain = norm_gain
    numbers = jnp.array([stages], jnp.int32)
    meta = jnp.concatenate(
        [stage[None], lengths, places[2], replica[None], numbers, places[0], places[1]]
    )
    (wq, wo), (meta, final_row, table) = gather_weights(
        places[2], w_qkv[0], w_out[0], (meta, final_gain[None, :], rotary_table())
    )
    ticks = micro + stages - 1
    half = stages // 2
    state, turned = (), ()
    inbox = entry
    for tick in range(ticks):
        before = turned if tick in (1, half + micro) else ()
        out, *state = forward_layer(
            tick, stages - 1, micro, meta, inbox, entry, gain, table, wq, wo, before, state
        )
        if tick == 0:
            turned = turn(True, meta, out, wq, wo, turned)
        if tick == half + micro - 1:
            turned = turn(False, meta, out, wq, wo, turned)
        if tick < ticks - 1:
            pairs = [(s, s + 1) for s in range(stages - 1) if 0 <= tick - s < micro]
            inbox = lax.ppermute(out, "section", pairs)
    stash_h, stash_x, last, stash_p = state
    stash = (stash_h, stash_x, stash_p)
    count = lax.axis_size(DP[:2])
    copies = embed(count, last, final_row, positive)
    here = lax.all_to_all(copies, DP[:2], split_axis=0, concat_axis=0, tiled=True)
    here = here.reshape(count * 8, WIDE)
    there = lax.ppermute(here, "dp_2", [(0, 1), (1, 0)])
    seed = loss_seed(meta, last, final_row, here, there)
    previous = ()
    for tick in range(ticks):
        previous = backward_layer(
            tick, stages - 1, micro, meta, inbox, seed, gain, table, *turned, stash, previous
        )
        if tick < ticks - 1:
            pairs = [
                (stages - 1 - s, stages - 2 - s)
                for s in range(stages - 1)
                if 0 <= tick - s < micro
            ]
            inbox = lax.ppermute(previous[0], "section", pairs)
    return previous[1][None]


def solution(mesh):
    finer = Mesh(
        mesh.devices.reshape(mesh.shape["section"], 4, 4, 2), ("section", "dp_0", "dp_1", "dp_2")
    )
    in_specs = (
        P(DP, None),
        P("section", None),
        P("section", DP, None),
        P("section", DP, None),
        P(),
        P(DP),
        P(DP),
    )
    return jax.shard_map(
        per_device,
        mesh=finer,
        in_specs=in_specs,
        out_specs=P("section", DP, None),
        check_vma=False,
    )
```

```python
import functools

import jax
import jax.numpy as jnp
from jax import lax
from jax.experimental import pallas as pl
from jax.experimental.pallas import tpu as pltpu
from jax.sharding import Mesh
from jax.sharding import PartitionSpec as P

HEAD_DIM = 64
LEN = 48
D = 3584
QW = 896
KV = 128
XW = QW + 2 * KV
PACK = XW + QW
PAIRS = QW // 128
DP = ("dp_0", "dp_1", "dp_2")
ROPE_BASE = 1000000.0
EPS = 1e-06
SHARP = 20.0
COEF = 256.0
HALVES = 2
HALF = D // HALVES
STAGGER = 5000
EVEN = 850
F32 = jnp.float32
BF16 = jnp.bfloat16


def dot_nn(a, b):
    return lax.dot_general(a, b, (((1,), (0,)), ((), ())), preferred_element_type=F32)


def dot_nt(a, b):
    return lax.dot_general(a, b, (((1,), (1,)), ((), ())), preferred_element_type=F32)


def dot_tn(a, b):
    return lax.dot_general(a, b, (((0,), (0,)), ((), ())), preferred_element_type=F32)


def lanes(rows):
    return lax.broadcasted_iota(jnp.int32, (rows, 128), 1)


def partner(x):
    low = lax.rem(lanes(x.shape[0]), 64) < 32
    return jnp.where(low, pltpu.roll(x, 96, 1), pltpu.roll(x, 32, 1))


def paired(z):
    left = lanes(LEN) < 64
    rolled = pltpu.roll(z, 64, 1)
    pad = jnp.zeros((16, 128), BF16)
    a_left = jnp.where(left, z, 0.0).astype(BF16)
    b_right = jnp.where(left, 0.0, z).astype(BF16)
    b_left = jnp.where(left, rolled, 0.0).astype(BF16)
    a_right = jnp.where(left, 0.0, rolled).astype(BF16)
    return (
        jnp.concatenate([a_left, pad, a_right, pad], axis=0),
        jnp.concatenate([a_left, pad, b_right, pad], axis=0),
        jnp.concatenate([b_left, pad, b_right, pad], axis=0),
    )


SPANS = ((0, 3 * LEN), (3 * LEN, 4 * LEN), (4 * LEN, 7 * LEN))


def by_pair(dot, rows, blocks):
    return jnp.concatenate(
        [dot(rows[lo:hi], block) for (lo, hi), block in zip(SPANS, blocks)], axis=0
    )


def unpaired(rows, other):
    left = lanes(LEN) < 64
    s00, s01, s11 = (dot_tn(rows[lo:hi], other[lo:hi]) for lo, hi in SPANS)
    first = jnp.where(left, s00[:LEN] + s01[:LEN], 0.0)
    first += pltpu.roll(jnp.where(left, 0.0, s00[64 : 64 + LEN]), 64, 1)
    second = jnp.where(left, 0.0, s01[64 : 64 + LEN] + s11[64 : 64 + LEN])
    second += pltpu.roll(jnp.where(left, s11[:LEN], 0.0), 64, 1)
    return first + second


def half_sums(x):
    left = lanes(x.shape[0]) < 64
    low = jnp.sum(jnp.where(left, x, 0.0), axis=1, keepdims=True)
    high = jnp.sum(jnp.where(left, 0.0, x), axis=1, keepdims=True)
    return low, high, left


def probabilities(q_rows, k_blocks, length):
    scores = by_pair(dot_nt, q_rows, k_blocks) * HEAD_DIM ** (-0.5)
    live = lax.rem(lanes(scores.shape[0]), 64) < length
    weights = jnp.where(live, jnp.exp(scores), 0.0)
    low, high, left = half_sums(weights)
    return weights * jnp.where(left, 1.0 / low, 1.0 / high)


def rows_of(x_ref):
    return jnp.concatenate([x_ref[:, 128 * i : 128 * i + 128] for i in range(PAIRS)], axis=0)


def inv_rms(wide):
    return lax.rsqrt(jnp.sum(wide * wide, axis=1, keepdims=True) * (1.0 / D) + EPS)


def forward_kernel(
    tick,
    last_stage,
    micro,
    meta,
    inbox,
    entry,
    gain,
    table,
    wq,
    wo,
    *refs,
):
    out, stash_h, stash_x, last, h_v, n_v, acc_v, x_v, ctx_v, last_v, sems = refs[-11:]
    stage = meta[0]
    slot = tick - stage

    @pl.when(jnp.logical_and(slot >= 0, slot < micro))
    def _():
        length = meta[1 + slot]
        row0 = pl.multiple_of(slot * LEN, LEN)

        @pl.when(stage == 0)
        def _():
            fresh = pltpu.make_async_copy(entry.at[pl.ds(row0, LEN), :], h_v, sems.at[0])
            fresh.start()
            fresh.wait()

        @pl.when(stage != 0)
        def _():
            h_v[...] = inbox[:LEN]

        @pl.when(jnp.logical_and(meta[5] == 1, stage != last_stage))
        def _():
            pl.delay(STAGGER if tick == 0 else EVEN)

        keep_h = pltpu.make_async_copy(h_v, stash_h.at[pl.ds(row0, LEN), :], sems.at[1])
        keep_h.start()
        wide = h_v[...].astype(F32)
        n_v[...] = (wide * inv_rms(wide) * gain[...]).astype(BF16)
        acc_v[...] = jnp.zeros_like(acc_v)

        @pl.loop(0, HALVES)
        def _(i):
            cols = pl.ds(pl.multiple_of(i * HALF, HALF), HALF)
            acc_v[...] += dot_nn(n_v[:, cols], wq[cols, :])

        cosine, sine = table[0], table[1]
        for i in range(PAIRS + 1):
            part = acc_v[:, 128 * i : 128 * i + 128]
            x_v[:, 128 * i : 128 * i + 128] = (part * cosine + partner(part) * sine).astype(BF16)
        x_v[:, QW + KV :] = acc_v[:, QW + KV :].astype(BF16)
        keep_x = pltpu.make_async_copy(x_v, stash_x.at[pl.ds(row0, LEN), :], sems.at[2])
        keep_x.start()
        k_blocks = paired(x_v[:, QW : QW + KV].astype(F32))
        v_blocks = paired(x_v[:, QW + KV :].astype(F32))
        probs = probabilities(rows_of(x_v), k_blocks, length).astype(BF16)
        context = by_pair(dot_nn, probs, v_blocks).astype(BF16)
        for i in range(PAIRS):
            ctx_v[:, 128 * i : 128 * i + 128] = context[LEN * i : LEN * i + LEN]

        @pl.loop(0, HALVES)
        def _(i):
            cols = pl.ds(pl.multiple_of(i * HALF, HALF), HALF)
            branch = dot_nn(ctx_v[...], wo[:, cols])
            out[:, cols] = (h_v[:, cols].astype(F32) + branch).astype(BF16)

        @pl.when(stage == last_stage)
        def _():
            hit = lax.broadcasted_iota(jnp.int32, (LEN, D), 0) == length - 1
            row = jnp.sum(jnp.where(hit, out[...].astype(F32), 0.0), axis=0, keepdims=True)
            last_v[...] = jnp.broadcast_to(row, (8, D))
            put = pltpu.make_async_copy(last_v, last.at[slot], sems.at[3])
            put.start()
            put.wait()

        keep_h.wait()
        keep_x.wait()


def backward_kernel(
    tick,
    last_stage,
    micro,
    meta,
    inbox,
    seed,
    gain,
    table,
    wq,
    wo,
    stash_h,
    stash_x,
    *refs,
):
    out, grads, h_v, g_v, x_v, dctx_v, dx_v, dn_v, sems = refs[-9:]
    stage = meta[0]
    slot = tick - (last_stage - stage)

    def put(value, to):
        rows = pl.ds(pl.multiple_of(to * LEN, LEN), LEN)
        return pltpu.make_async_copy(value, grads.at[rows, :], sems.at[2])

    def put_half(half):
        rows = pl.ds(pl.multiple_of(slot * LEN, LEN), LEN)
        cols = pl.ds(half * HALF, HALF)
        return pltpu.make_async_copy(out.at[:, cols], grads.at[rows, cols], sems.at[half])

    final = tick == last_stage + micro - 1
    late = jnp.logical_and(slot >= 1, slot <= micro)
    if tick > 0:

        @pl.when(late)
        def _():
            put(refs[0], slot - 1).start()

    @pl.when(jnp.logical_and(slot >= 0, slot < micro))
    def _():
        length = meta[1 + slot]
        row0 = pl.multiple_of(slot * LEN, LEN)

        get_x = pltpu.make_async_copy(stash_x.at[pl.ds(row0, LEN), :], x_v, sems.at[0])
        get_h = pltpu.make_async_copy(stash_h.at[pl.ds(row0, LEN), :], h_v, sems.at[1])
        get_x.start()
        get_h.start()

        @pl.when(jnp.logical_and(meta[5] == 1, stage != 0))
        def _():
            pl.delay(STAGGER if tick == 0 else EVEN)

        @pl.when(stage == last_stage)
        def _():
            hit = lax.broadcasted_iota(jnp.int32, (LEN, D), 0) == length - 1
            row = jnp.where(lax.broadcasted_iota(jnp.int32, (8, D), 0) == slot, seed[...], 0.0)
            row = jnp.sum(row, axis=0, keepdims=True)
            g_v[...] = jnp.where(hit, jnp.broadcast_to(row, (LEN, D)), 0.0).astype(BF16)

        @pl.when(stage != last_stage)
        def _():
            g_v[...] = inbox[...]

        dctx_v[...] = jnp.zeros_like(dctx_v)

        @pl.loop(0, HALVES)
        def _(i):
            cols = pl.ds(pl.multiple_of(i * HALF, HALF), HALF)
            dctx_v[...] += dot_nn(g_v[:, cols], wo[cols, :])

        get_x.wait()
        q_rows = rows_of(x_v)
        k_blocks = paired(x_v[:, QW : QW + KV].astype(F32))
        v_blocks = paired(x_v[:, QW + KV :].astype(F32))
        probs = probabilities(q_rows, k_blocks, length)
        dctx = rows_of(dctx_v).astype(BF16)
        dvalue = unpaired(probs.astype(BF16), dctx)
        dprobs = by_pair(dot_nt, dctx, v_blocks).astype(BF16).astype(F32)
        low, high, left = half_sums(dprobs * probs)
        dscores = probs * (dprobs - jnp.where(left, low, high)) * HEAD_DIM ** (-0.5)
        dscores = dscores.astype(BF16)
        dquery = by_pair(dot_nn, dscores, k_blocks).astype(BF16).astype(F32)
        dkey = unpaired(dscores, q_rows).astype(BF16).astype(F32)
        cosine, sine = table[0], table[1]
        for i in range(PAIRS):
            part = dquery[LEN * i : LEN * i + LEN]
            dx_v[:, 128 * i : 128 * i + 128] = (part * cosine - partner(part) * sine).astype(BF16)
        dx_v[:, QW : QW + KV] = (dkey * cosine - partner(dkey) * sine).astype(BF16)
        dx_v[:, QW + KV :] = dvalue.astype(BF16)

        @pl.loop(0, HALVES)
        def _(i):
            cols = pl.ds(pl.multiple_of(i * HALF, HALF), HALF)
            dn_v[:, cols] = dot_nn(dx_v[...], wq[:, cols]).astype(BF16)

        get_h.wait()
        wide = h_v[...].astype(F32)
        scale = inv_rms(wide)
        scaled = dn_v[...].astype(F32) * gain[...]
        inner = jnp.sum(scaled * wide, axis=1, keepdims=True)
        pull = scale * scale * scale * inner * (1.0 / D)
        for half in range(HALVES):
            cols = slice(half * HALF, half * HALF + HALF)
            near = g_v[:, cols].astype(F32) + scale * scaled[:, cols]
            out[:, cols] = (near - wide[:, cols] * pull).astype(BF16)
            if final:

                @pl.when(slot == micro - 1)
                def _():
                    put_half(half).start()

    if tick > 0:

        @pl.when(late)
        def _():
            put(refs[0], slot - 1).wait()

    if final:

        @pl.when(slot == micro - 1)
        def _():
            for half in range(HALVES):
                put_half(half).wait()


ANY = pl.BlockSpec(memory_space=pl.ANY)
VMEM = pl.BlockSpec(memory_space=pltpu.VMEM)
SMEM = pl.BlockSpec(memory_space=pltpu.SMEM)
HBM = pl.BlockSpec(memory_space=pltpu.HBM)
LAYER_COST = pl.CostEstimate(
    flops=2 * LEN * D * (XW + QW), bytes_accessed=2 * D * (XW + QW), transcendentals=0
)
LIMIT = 8 * 1024 * 1024
LARGE = 14 * 1024 * 1024
WHOLE = 60 * 1024 * 1024
SMALL = 8 * 1024 * 1024


def forward_layer(
    tick, last_stage, micro, meta, inbox, entry, gain, table, wq, wo, before, state
):
    rows = micro * LEN
    kept = (((rows, D), BF16), ((rows, XW), BF16), ((micro, 8, D), F32))
    return pl.pallas_call(
        functools.partial(forward_kernel, tick, last_stage, micro),
        out_shape=tuple(jax.ShapeDtypeStruct(*a) for a in (((LEN, D), BF16), *kept)),
        in_specs=[SMEM, VMEM, ANY, VMEM, VMEM, VMEM, VMEM, *[ANY] * len((*before, *state))],
        out_specs=(VMEM, ANY, ANY, ANY),
        input_output_aliases={7 + len(before) + i: 1 + i for i in range(len(state))},
        scratch_shapes=[
            pltpu.VMEM((LEN, D), BF16),
            pltpu.VMEM((LEN, D), BF16),
            pltpu.VMEM((LEN, XW), F32),
            pltpu.VMEM((LEN, XW), BF16),
            pltpu.VMEM((LEN, QW), BF16),
            pltpu.VMEM((8, D), F32),
            pltpu.SemaphoreType.DMA((4,)),
        ],
        compiler_params=pltpu.CompilerParams(vmem_limit_bytes=LIMIT),
        cost_estimate=LAYER_COST,
        name="forward_layer",
    )(meta, inbox, entry, gain, table, wq, wo, *before, *state)


def backward_layer(
    tick, last_stage, micro, meta, inbox, seed, gain, table, wq_t, wo_t, stash, previous
):
    return pl.pallas_call(
        functools.partial(backward_kernel, tick, last_stage, micro),
        out_shape=(
            jax.ShapeDtypeStruct((LEN, D), BF16),
            jax.ShapeDtypeStruct((micro * LEN, D), BF16),
        ),
        in_specs=[SMEM, VMEM, VMEM, VMEM, VMEM, VMEM, VMEM, ANY, ANY, *[ANY] * len(previous)],
        out_specs=(VMEM, ANY),
        input_output_aliases={10: 1} if previous else {},
        scratch_shapes=[
            pltpu.VMEM((LEN, D), BF16),
            pltpu.VMEM((LEN, D), BF16),
            pltpu.VMEM((LEN, XW), BF16),
            pltpu.VMEM((LEN, QW), F32),
            pltpu.VMEM((LEN, XW), BF16),
            pltpu.VMEM((LEN, D), BF16),
            pltpu.SemaphoreType.DMA((3,)),
        ],
        compiler_params=pltpu.CompilerParams(vmem_limit_bytes=LIMIT),
        cost_estimate=LAYER_COST,
        name="backward_layer",
    )(meta, inbox, seed, gain, table, wq_t, wo_t, *stash, *previous)


TURN = 256


def turn_kernel(early, meta, after, wq, wo, *refs):
    del after
    wq_t, wo_t, wq_v, wo_v, sems = refs[-5:]
    half = lax.div(meta[7], 2)
    due = meta[0] >= half if early else meta[0] < half

    @pl.when(due)
    def _():
        def copies(i, slot):
            at = pl.ds(pl.multiple_of(i * TURN, TURN), TURN)
            return (
                pltpu.make_async_copy(wq_v.at[slot], wq_t.at[:, at], sems.at[0, slot]),
                pltpu.make_async_copy(wo_v.at[slot], wo_t.at[at, :], sems.at[1, slot]),
            )

        @pl.loop(0, D // TURN)
        def _(i):
            slot = lax.rem(i, 2)
            at = pl.ds(pl.multiple_of(i * TURN, TURN), TURN)

            @pl.when(i >= 2)
            def _():
                for copy in copies(i - 2, slot):
                    copy.wait()

            wq_v[slot] = wq[at, :].T
            wo_v[slot] = wo[:, at].T
            for copy in copies(i, slot):
                copy.start()

        for i in (D // TURN - 2, D // TURN - 1):
            for copy in copies(i, i % 2):
                copy.wait()


def turn(early, meta, after, wq, wo, turned):
    return pl.pallas_call(
        functools.partial(turn_kernel, early),
        out_shape=(jax.ShapeDtypeStruct((XW, D), BF16), jax.ShapeDtypeStruct((D, QW), BF16)),
        in_specs=[SMEM, ANY, VMEM, VMEM, *[ANY] * len(turned)],
        out_specs=(ANY, ANY),
        input_output_aliases={4 + i: i for i in range(len(turned))},
        scratch_shapes=[
            pltpu.VMEM((2, XW, TURN), BF16),
            pltpu.VMEM((2, TURN, QW), BF16),
            pltpu.SemaphoreType.DMA((2, 2)),
        ],
        compiler_params=pltpu.CompilerParams(vmem_limit_bytes=LIMIT),
        cost_estimate=pl.CostEstimate(flops=0, bytes_accessed=4 * D * (XW + QW), transcendentals=0),
        name="turn",
    )(meta, after, wq, wo, *turned)


SIDE = PACK // 2


def pack_kernel(core, w_qkv, w_out, keep, give, w_v, x_v, sems):
    first = pltpu.make_async_copy(w_out, w_v, sems.at[0])
    second = pltpu.make_async_copy(w_qkv, x_v, sems.at[1])
    first.start()
    second.start()
    first.wait()
    pieces = [w_v[:, QW * j : QW * j + QW].astype(F32) for j in range(D // QW)]
    low = jnp.concatenate(pieces, axis=0).astype(BF16)
    second.wait()

    def fill(left, right):
        left[...] = x_v[:, :SIDE]
        right[:, : XW - SIDE] = x_v[:, SIDE:]
        right[:, XW - SIDE :] = low

    @pl.when(core[0] == 0)
    def _():
        fill(keep, give)

    @pl.when(core[0] == 1)
    def _():
        fill(give, keep)


def pack(core, w_qkv, w_out):
    side = jax.ShapeDtypeStruct((w_qkv.shape[0], SIDE), BF16)
    return pl.pallas_call(
        pack_kernel,
        out_shape=(side, side),
        in_specs=[SMEM, HBM, HBM],
        out_specs=(VMEM, VMEM),
        scratch_shapes=[
            pltpu.VMEM(w_out.shape, BF16),
            pltpu.VMEM(w_qkv.shape, BF16),
            pltpu.SemaphoreType.DMA((2,)),
        ],
        compiler_params=pltpu.CompilerParams(vmem_limit_bytes=WHOLE),
        name="pack",
    )(core, w_qkv, w_out)


def unpack_kernel(meta, *refs):
    count = (len(refs) - 4) // 2
    mine, theirs = refs[:count], refs[count : 2 * count]
    wq, wo, part_v, sems = refs[2 * count :]
    parts = D // QW
    length = D // 32
    short = length // parts
    x0, y0, core = meta[8], meta[9], meta[5]

    def offset(step):
        return jnp.where(step == 1, 3, jnp.where(step == 2, 1, jnp.where(step == 3, 2, 0)))

    def put(blocks, color):
        for n in range(8):
            block = blocks[n]
            far, other = n // 2, n % 2

            @pl.loop(0, 4)
            def _(near):
                first = lax.rem(offset(near) + (y0 if color == 0 else x0), 4)
                second = lax.rem((0, 3, 1, 2)[far] + (x0 if color == 0 else y0), 4)
                x, y = (second, first) if color == 0 else (first, second)
                shard = x * 8 + y * 2 + (color if other == 0 else 1 - color)
                rows = pl.ds(pl.multiple_of(shard * length, length), length)
                if color == 0:
                    pltpu.make_async_copy(
                        block.at[near], wq.at[rows, pl.ds(0, SIDE)], sems.at[0]
                    ).start()
                else:
                    pltpu.make_async_copy(
                        block.at[near, :, pl.ds(0, XW - SIDE)],
                        wq.at[rows, pl.ds(SIDE, XW - SIDE)],
                        sems.at[0],
                    ).start()
                    pltpu.make_async_copy(
                        block.at[near, :, pl.ds(XW - SIDE, QW)], part_v.at[rows, :], sems.at[1]
                    ).start()

    @pl.when(core == 0)
    def _():
        put(theirs, 1)
        put(mine, 0)

    @pl.when(core == 1)
    def _():
        put(mine, 1)
        put(theirs, 0)

    pltpu.make_async_copy(part_v, part_v, sems.at[1]).wait()

    @pl.loop(0, 8)
    def _(i):
        blocks = []
        for r in range(4):
            at = pl.ds(pl.multiple_of((4 * i + r) * length, length), length)
            blocks.append(part_v[at, :].astype(F32))
        to = pl.ds(pl.multiple_of(i * length, length), length)
        for j in range(parts):
            cut = [block[short * j : short * j + short] for block in blocks]
            wo[to, QW * j : QW * j + QW] = jnp.concatenate(cut, axis=0).astype(BF16)

    pltpu.make_async_copy(wq, wq, sems.at[0]).wait()


def unpack(meta, mine, theirs):
    return pl.pallas_call(
        unpack_kernel,
        out_shape=(jax.ShapeDtypeStruct((D, XW), BF16), jax.ShapeDtypeStruct((QW, D), BF16)),
        in_specs=[SMEM, *[ANY] * (len(mine) + len(theirs))],
        out_specs=(VMEM, VMEM),
        scratch_shapes=[pltpu.VMEM((D, QW), BF16), pltpu.SemaphoreType.DMA((2,))],
        compiler_params=pltpu.CompilerParams(vmem_limit_bytes=LARGE),
        name="unpack",
    )(meta, *mine, *theirs)


def ring_step(value, second, step):
    pairs = []
    for x in range(4):
        for y in range(4):
            for core in range(2):
                along_y = (core == 0) != second
                to = (x, (y + step) % 4) if along_y else ((x + step) % 4, y)
                pairs.append((x * 8 + y * 2 + core, to[0] * 8 + to[1] * 2 + core))
    return lax.ppermute(value, DP, pairs)


def swap_cores(value):
    return lax.ppermute(value, "dp_2", [(0, 1), (1, 0)])


def join_kernel(*refs):
    *parts, out, sems = refs
    copies = [
        pltpu.make_async_copy(part, out.at[n], sems.at[n]) for n, part in enumerate(parts)
    ]
    for copy in copies:
        copy.start()
    for copy in copies:
        copy.wait()


def join(*parts):
    return pl.pallas_call(
        join_kernel,
        out_shape=jax.ShapeDtypeStruct((len(parts), *parts[0].shape), parts[0].dtype),
        in_specs=[ANY] * len(parts),
        out_specs=ANY,
        scratch_shapes=[pltpu.SemaphoreType.DMA((len(parts),))],
        compiler_params=pltpu.CompilerParams(vmem_limit_bytes=1024 * 1024),
        name="join",
    )(*parts)


def gather_weights(core, w_qkv, w_out, others):
    keep, give = pack(core, w_qkv, w_out)
    got, others = lax.optimization_barrier((swap_cores(give), others))
    meta = others[0]
    lines = []
    for value, forward in ((keep, 1), (got, -1)):
        before = ring_step(value, False, 1)
        after = ring_step(value, False, -1)
        across = ring_step(before if forward == 1 else after, False, forward)
        lines.append(join(value, before, after, across))
    mine = [None] * 8
    for n, (line, forward) in enumerate(zip(lines, (1, -1))):
        before = ring_step(line, True, 1)
        after = ring_step(line, True, -1)
        across = ring_step(before if forward == 1 else after, True, forward)
        mine[n::2] = [line, before, after, across]
    return unpack(meta, mine, [swap_cores(value) for value in mine]), others


WIDE = HALF + 128


def pooled_rows(last):
    return jnp.concatenate([last[j, 0:1, :] for j in (0, 2, 1, 3)], axis=0)


def embed_kernel(last, final_gain, labels, out):
    rows = pooled_rows(last)
    pooled = rows * inv_rms(rows) * final_gain[...]
    unit = pooled * lax.rsqrt(jnp.sum(pooled * pooled, axis=1, keepdims=True))
    halves = jnp.concatenate([unit[:, :HALF], unit[:, HALF:]], axis=0).astype(BF16)
    which = lax.broadcasted_iota(jnp.int32, (8, 128), 0)
    label = jnp.where(which == 0, labels[0], jnp.where(which == 1, labels[1], 0))
    label = label.astype(F32).astype(BF16)
    for i in range(out.shape[0]):
        out[i, :, :HALF] = halves
        out[i, :, HALF:] = label


def embed(count, last, final_gain, labels):
    return pl.pallas_call(
        embed_kernel,
        out_shape=jax.ShapeDtypeStruct((count, 8, WIDE), BF16),
        in_specs=[VMEM, VMEM, SMEM],
        out_specs=VMEM,
        compiler_params=pltpu.CompilerParams(vmem_limit_bytes=LIMIT),
        name="embed",
    )(last, final_gain, labels)


def loss_kernel(meta, last, final_gain, here, there, seed):
    everyone = jnp.concatenate([here[...], there[...]], axis=0)
    count = everyone.shape[0]
    emb = everyone[:, :HALF]
    label = everyone[:, HALF:].astype(F32)[:, 0:1].astype(jnp.int32)
    scores = dot_nt(emb, emb)
    scores = scores + pltpu.roll(pltpu.roll(scores, count - 4, 0), count - 4, 1)
    row = lax.rem(lax.broadcasted_iota(jnp.int32, (count, count), 0), 8)
    col = lax.broadcasted_iota(jnp.int32, (count, count), 1)
    doc = jnp.logical_and(lax.rem(col, 8) >= 2, lax.rem(col, 8) < 4)
    valid = jnp.logical_and(row < 2, doc)
    weights = jnp.where(valid, jnp.exp(scores * SHARP), 0.0)
    total = jnp.sum(weights, axis=1, keepdims=True)
    prob = weights / jnp.where(row[:, :1] < 2, total, 1.0)
    owner = lax.div(label, 2)
    away = (lax.rem(owner, 2) != meta[5]).astype(jnp.int32)
    target = away * (count // 2) + lax.div(owner, 2) * 8 + 2 + lax.rem(label, 2)
    coef = jnp.where(valid, (prob - (col == target).astype(F32)) * (COEF * SHARP), 0.0)
    both = coef + coef.T
    mine = lax.broadcasted_iota(jnp.int32, (8, count), 0)
    pick = lax.broadcasted_iota(jnp.int32, (8, count), 1) == lax.div(meta[6], 2) * 8 + mine
    own = lax.dot_general(
        pick.astype(F32),
        both,
        (((1,), (0,)), ((), ())),
        precision=lax.Precision.HIGHEST,
        preferred_element_type=F32,
    )[:4]
    own = jnp.concatenate([own, pltpu.roll(own, 4, 1)], axis=0)
    top = own.astype(BF16)
    rest = own - top.astype(F32)
    mid = rest.astype(BF16)
    low = (rest - mid.astype(F32)).astype(BF16)
    split = dot_nn(jnp.concatenate([top, mid, low, low], axis=0), emb)
    grad = split[:8] + (split[8:16] + split[16:24])
    grad = jnp.concatenate([grad[:4], grad[4:]], axis=1)
    rows = pooled_rows(last)
    gain = final_gain[...]
    scale = inv_rms(rows)
    pooled = rows * scale * gain
    norm = lax.rsqrt(jnp.sum(pooled * pooled, axis=1, keepdims=True))
    unit = pooled * norm
    dpooled = norm * (grad - unit * jnp.sum(grad * unit, axis=1, keepdims=True))
    scaled = dpooled * gain
    inner = jnp.sum(scaled * rows, axis=1, keepdims=True)
    drow = scale * scaled - rows * (scale * scale * scale * inner * (1.0 / D))
    drow = drow.astype(BF16).astype(F32)
    seed[...] = jnp.concatenate(
        [drow[0:1], drow[2:3], drow[1:2], drow[3:4], jnp.zeros((4, D), F32)], axis=0
    )


def loss_seed(meta, last, final_gain, here, there):
    return pl.pallas_call(
        loss_kernel,
        out_shape=jax.ShapeDtypeStruct((8, D), F32),
        in_specs=[SMEM, VMEM, VMEM, VMEM, VMEM],
        out_specs=VMEM,
        compiler_params=pltpu.CompilerParams(vmem_limit_bytes=LIMIT),
        name="loss_seed",
    )(meta, last, final_gain, here, there)


def rotary_table():
    lane = jnp.arange(128, dtype=jnp.int32)
    frequency = ROPE_BASE ** (-(lane % 32).astype(F32) * (2.0 / HEAD_DIM))
    angles = jnp.arange(LEN, dtype=F32)[:, None] * frequency[None, :]
    sign = jnp.where(lane % 64 < 32, -1.0, 1.0)
    return jnp.stack([jnp.cos(angles), jnp.sin(angles) * sign])


def per_device(entry, norm_gain, w_qkv, w_out, final_gain, lengths, positive):
    stage = lax.axis_index("section")
    stages = lax.axis_size("section")
    replica = lax.axis_index(DP)
    places = [lax.axis_index(name)[None] for name in DP]
    micro = lengths.shape[0]
    gain = norm_gain
    numbers = jnp.array([stages], jnp.int32)
    meta = jnp.concatenate(
        [stage[None], lengths, places[2], replica[None], numbers, places[0], places[1]]
    )
    (wq, wo), (meta, final_row, table) = gather_weights(
        places[2], w_qkv[0], w_out[0], (meta, final_gain[None, :], rotary_table())
    )
    ticks = micro + stages - 1
    half = stages // 2
    state, turned = (), ()
    inbox = entry
    for tick in range(ticks):
        before = turned if tick in (1, half + micro) else ()
        out, *state = forward_layer(
            tick, stages - 1, micro, meta, inbox, entry, gain, table, wq, wo, before, state
        )
        if tick == 0:
            turned = turn(True, meta, out, wq, wo, turned)
        if tick == half + micro - 1:
            turned = turn(False, meta, out, wq, wo, turned)
        if tick < ticks - 1:
            pairs = [(s, s + 1) for s in range(stages - 1) if 0 <= tick - s < micro]
            inbox = lax.ppermute(out, "section", pairs)
    *stash, last = state
    count = lax.axis_size(DP[:2])
    copies = embed(count, last, final_row, positive)
    here = lax.all_to_all(copies, DP[:2], split_axis=0, concat_axis=0, tiled=True)
    here = here.reshape(count * 8, WIDE)
    there = lax.ppermute(here, "dp_2", [(0, 1), (1, 0)])
    seed = loss_seed(meta, last, final_row, here, there)
    previous = ()
    for tick in range(ticks):
        previous = backward_layer(
            tick, stages - 1, micro, meta, inbox, seed, gain, table, *turned, stash, previous
        )
        if tick < ticks - 1:
            pairs = [
                (stages - 1 - s, stages - 2 - s)
                for s in range(stages - 1)
                if 0 <= tick - s < micro
            ]
            inbox = lax.ppermute(previous[0], "section", pairs)
    return previous[1][None]


def solution(mesh):
    finer = Mesh(
        mesh.devices.reshape(mesh.shape["section"], 4, 4, 2), ("section", "dp_0", "dp_1", "dp_2")
    )
    in_specs = (
        P(DP, None),
        P("section", None),
        P("section", DP, None),
        P("section", DP, None),
        P(),
        P(DP),
        P(DP),
    )
    return jax.shard_map(
        per_device,
        mesh=finer,
        in_specs=in_specs,
        out_specs=P("section", DP, None),
        check_vma=False,
    )
```
